32 devices in a mesh: groups: 2 (over y), tp: 4 (over x, core), dp: 4 (over z).
Axes of the slice: x: 2, y: 2, z: 4, core: 2. Of those that a mesh axis runs over, the one named last changes fastest.
Arguments:
- hidden: bfloat16 [128, 2560], P(('groups', 'dp'), 'tp'), parts along dimension 0, may hold values from -40 to 40
- in_gain: float32 [2560], replicated, may hold values from 0.1 to 1.9
- z_weight: bfloat16 [2560, 5120], P(None, 'tp'), may hold values from -0.125 to 0.125
- x_weight: bfloat16 [2560, 5120], P(None, 'tp'), may hold values from -0.125 to 0.125
- bc_weight: bfloat16 [2560, 256], P(None, 'tp'), may hold values from -0.125 to 0.125
- dt_weight: bfloat16 [2560, 80], P(None, 'tp'), may hold values from -0.125 to 0.125
- conv_x_weight: bfloat16 [4, 5120], P(None, 'tp'), may hold values from -3 to 3
- conv_x_bias: bfloat16 [5120], P('tp'), may hold values from -3 to 3
- conv_bc_weight: bfloat16 [4, 256], P(None, 'tp'), may hold values from -3 to 3
- conv_bc_bias: bfloat16 [256], P('tp'), may hold values from -3 to 3
- conv_x_state: bfloat16 [128, 3, 5120], P(('groups', 'dp'), None, 'tp'), parts along dimension 0, may hold values from -6 to 6
- conv_bc_state: bfloat16 [128, 3, 256], P(('groups', 'dp'), None, 'tp'), parts along dimension 0, may hold values from -6 to 6
- dt_bias: float32 [80], P('tp'), may hold values from -4 to -1
- log_rate: float32 [80], P('tp'), may hold values from 0 to 2.5
- skip_gain: float32 [80], P('tp'), may hold values from 0.5 to 2
- ssm_state: float32 [128, 80, 64, 128], P(('groups', 'dp'), 'tp'), parts along dimension 0, may hold values from -20 to 20
- norm_gain: float32 [5120], P('tp'), may hold values from 0.1 to 1.9
- out_weight: bfloat16 [5120, 2560], P('tp'), may hold values from -0.125 to 0.125
- pool_slot: int32 [8, 16], P(('groups', 'dp')), parts along dimension 0, may hold values from 0 to 15, as said below
- active: int32 [128], P(('groups', 'dp')), parts along dimension 0, may hold values 0 or 1
Outputs:
- layer_out: bfloat16 [128, 2560], P(('groups', 'dp'), 'tp'), parts along dimension 0
- conv_x_next: bfloat16 [128, 3, 5120], P(('groups', 'dp'), None, 'tp'), parts along dimension 0
- conv_bc_next: bfloat16 [128, 3, 256], P(('groups', 'dp'), None, 'tp'), parts along dimension 0
- ssm_next: float32 [128, 80, 64, 128], P(('groups', 'dp'), 'tp'), parts along dimension 0
The draws below stay inside these ranges and needn't reach their ends.
There are 2 independent parts, one for each index of `groups`. The reference program is written for one: setup_inputs(seed, part) draws one part's arguments, and reference() takes and returns one part's arrays. A program takes and returns all parts, laid end to end along the dimension named above; an argument that names none is the same for every part. Nothing has to cross between parts.
Inputs may be any that keep to these rules, and one draw needn't show every extreme that they name: `pool_slot`: each row is a permutation of 0 to 15.
All inputs are finite; a program needn't handle non-finite values. No bound on the sum of `active` on one device may be relied on, other than what follows from the above.
Results may differ from the reference program's by a relative error of at most 0.0085.
Values may be sent and summed in bfloat16 or wider, within the bound.
A program may use at most 128 MiB of HBM per device.

```python
import math
import jax
import jax.numpy as jnp
from jax import lax

D = 2560
HEADS = 80
HP = 64
NS = 128
KW = 4
SEQ_DEV = 16
INNER = 5120
BATCH = 64
N_DP = 4


def draw_hidden(key, part):
    base_key = jax.random.fold_in(key, 21)
    row_key = jax.random.fold_in(key, 22)
    col_key = jax.random.fold_in(key, 23)
    position = jnp.arange(D, dtype=jnp.float32) / (D - 1)
    jitter = jnp.exp(jax.random.uniform(col_key, (D,), jnp.float32, 0.0, math.log(3.3)))
    row_scale = jnp.exp(jax.random.uniform(row_key, (BATCH,), jnp.float32, math.log(0.3), math.log(3.0)))
    base_draw = jnp.clip(jax.random.normal(base_key, (BATCH, D), jnp.float32), -4.0, 4.0)
    col_scale = 3.0 ** position * jitter / 3.3
    return (base_draw * row_scale[:, None] * col_scale[None, :]).astype(jnp.bfloat16)


def draw_ssm_state(key, part):
    base_key = jax.random.fold_in(key, 11)
    head_key = jax.random.fold_in(key, 12)
    position = jnp.arange(HEADS, dtype=jnp.float32) / (HEADS - 1)
    base_draw = jnp.clip(jax.random.normal(base_key, (BATCH, HEADS, HP, NS), jnp.float32), -5.0, 5.0)
    head_trend = 3.0 ** position
    jitter = jnp.exp(jax.random.uniform(head_key, (HEADS,), jnp.float32, 0.0, math.log(3.0)))
    return 0.3 * base_draw * (head_trend * jitter)[None, :, None, None]


def permute_slots(slot_key):
    return jax.random.permutation(slot_key, SEQ_DEV)


def draw_pool_slot(key, part):
    slot_keys = jax.random.split(jax.random.fold_in(key, 31), N_DP)
    return jax.vmap(permute_slots)(slot_keys).astype(jnp.int32)


def place_ends(result, own_key, low, high):
    index_at = [jax.random.randint(jax.random.fold_in(own_key, axis), (), 0, length) for axis, length in enumerate(result.shape)]
    widest = result.shape.index(max(result.shape))
    beside = index_at[:widest] + [(index_at[widest] + 1) % result.shape[widest]] + index_at[widest + 1:]
    return result.at[tuple(index_at)].set(low).at[tuple(beside)].set(high)


def raised(values, own_key, source, target, blocks, factor):
    owner, partner = [(jnp.arange(values.shape[axis_at]) // (values.shape[axis_at] // blocks)).reshape([-1 if axis == axis_at else 1 for axis in range(values.ndim)]) for axis_at in (source, target)]
    chosen = jax.random.permutation(own_key, blocks)[partner]
    strong = (owner == chosen) | (owner == (partner + blocks // 2) % blocks)
    return jnp.where(strong, factor * values, values)


def level_of(stream_key, extent, cuts, least, largest):
    loudness = 1.0
    for axis_at, shards_of in cuts:
        steps = jax.random.uniform(jax.random.fold_in(jax.random.fold_in(stream_key, 6), axis_at), (shards_of,), jnp.float32, least / len(cuts), largest / len(cuts))
        loudness = loudness * jnp.repeat(jnp.exp(steps), extent[axis_at] // shards_of).reshape((-1,) + (1,) * (len(extent) - 1 - axis_at))
    return loudness


def normal_values(rng, dims, scale, bound, pieces=(), kind=jnp.bfloat16):
    entries = jax.random.normal(rng, dims, jnp.float32) * scale
    if len(pieces) > 0:
        entries = level_of(rng, dims, pieces, -0.22, 0.18) * entries
    return jnp.clip(entries, min=-bound, max=bound).astype(kind)


def gaussian_with(stream_key, shape, width, bound, cuts, heavy, kind=jnp.bfloat16):
    result = width * jax.random.normal(stream_key, shape, jnp.float32)
    if cuts:
        result = result * level_of(stream_key, shape, cuts, -0.22, 0.18)
    return jnp.clip(raised(result, jax.random.fold_in(stream_key, 3), *heavy), -bound, bound).astype(kind)


def setup_inputs(seed: int = 0, part: int = 0) -> dict:
    splits = jax.random.split(jax.random.key(seed), 21)
    part_splits = jax.random.split(jax.random.fold_in(splits[20], part), 21)
    hidden = draw_hidden(jax.random.fold_in(jax.random.fold_in(splits[20], part), 71), part)
    in_gain = jnp.clip(1.0 + 0.18 * jax.random.normal(splits[1], (D,), jnp.float32), 0.1, 1.9)
    z_weight = normal_values(splits[2], (D, INNER), D ** -0.5, 0.125, ((1, 4),))
    x_weight = normal_values(splits[3], (D, INNER), D ** -0.5, 0.125, ((1, 4),))
    bc_weight = normal_values(splits[4], (D, 2 * NS), D ** -0.5, 0.125, ((1, 4),))
    dt_weight = normal_values(splits[5], (D, HEADS), D ** -0.5, 0.125, ((1, 4),))
    conv_x_weight = normal_values(splits[6], (KW, INNER), KW ** -0.5, 3.0, ((1, 4),))
    conv_x_bias = normal_values(splits[7], (INNER,), 0.5, 3.0, ((0, 4),))
    conv_bc_weight = normal_values(splits[8], (KW, 2 * NS), KW ** -0.5, 3.0, ((1, 4),))
    conv_bc_bias = normal_values(splits[9], (2 * NS,), 0.5, 3.0, ((0, 4),))
    conv_x_state = normal_values(part_splits[10], (BATCH, KW - 1, INNER), 1.0, 6.0, ((0, 4), (2, 4)))
    conv_bc_state = normal_values(part_splits[11], (BATCH, KW - 1, 2 * NS), 1.0, 6.0, ((0, 4), (2, 4)))
    dt_bias = jnp.clip(-4.0 + 3.0 * jax.random.uniform(splits[12], (HEADS,), jnp.float32) ** level_of(splits[12], (HEADS,), ((0, 4),), -0.2, 0.2), -4.0, -1.0)
    log_rate = jnp.clip(2.5 * jax.random.uniform(splits[13], (HEADS,), jnp.float32) ** level_of(splits[13], (HEADS,), ((0, 4),), -0.2, 0.2), 0.0, 2.5)
    skip_gain = jnp.clip(0.5 + 1.5 * jax.random.uniform(splits[14], (HEADS,), jnp.float32) ** level_of(splits[14], (HEADS,), ((0, 4),), -0.2, 0.2), 0.5, 2.0)
    ssm_state = draw_ssm_state(jax.random.fold_in(jax.random.fold_in(splits[20], part), 71), part)
    norm_gain = jnp.clip(1.0 + 0.18 * jax.random.normal(splits[16], (INNER,), jnp.float32), 0.1, 1.9)
    out_weight = gaussian_with(splits[17], (INNER, D), INNER ** -0.5, 0.125, ((0, 4),), (0, 1, 4, 2.0))
    pool_slot = draw_pool_slot(jax.random.fold_in(jax.random.fold_in(splits[20], part), 71), part)
    active = place_ends((jax.random.randint(part_splits[19], (BATCH,), 0, 4) < 3).astype(jnp.int32), jax.random.fold_in(part_splits[19], 1), 0, 1)
    return dict(hidden=hidden, in_gain=in_gain, z_weight=z_weight, x_weight=x_weight, bc_weight=bc_weight, dt_weight=dt_weight, conv_x_weight=conv_x_weight, conv_x_bias=conv_x_bias, conv_bc_weight=conv_bc_weight, conv_bc_bias=conv_bc_bias, conv_x_state=conv_x_state, conv_bc_state=conv_bc_state, dt_bias=dt_bias, log_rate=log_rate, skip_gain=skip_gain, ssm_state=ssm_state, norm_gain=norm_gain, out_weight=out_weight, pool_slot=pool_slot, active=active)


def convolve(old_state, current, weight, conv_bias):
    window = jnp.concatenate([old_state.astype(jnp.float32), current.astype(jnp.float32)[:, None, :]], axis=1)
    conv_out = lax.optimization_barrier(jnp.sum(window * weight.astype(jnp.float32)[None], axis=1)) + conv_bias.astype(jnp.float32)
    return (jax.nn.silu(conv_out).astype(jnp.bfloat16), window[:, 1:, :].astype(jnp.bfloat16))

def reference(hidden, in_gain, z_weight, x_weight, bc_weight, dt_weight, conv_x_weight, conv_x_bias, conv_bc_weight, conv_bc_bias, conv_x_state, conv_bc_state, dt_bias, log_rate, skip_gain, ssm_state, norm_gain, out_weight, pool_slot, active):
    pool_row = (pool_slot + (jnp.arange(N_DP, dtype=jnp.int32) * SEQ_DEV)[:, None]).reshape(-1).astype(jnp.int32)
    is_live = active > 0
    hidden_f32 = hidden.astype(jnp.float32)
    inv_rms = lax.rsqrt(lax.optimization_barrier(jnp.mean(hidden_f32 * hidden_f32, axis=1, keepdims=True)) + 1e-05)
    normed = (hidden_f32 * inv_rms * in_gain).astype(jnp.bfloat16)
    z_proj = jnp.dot(normed, z_weight, preferred_element_type=jnp.float32).astype(jnp.bfloat16)
    x_proj = jnp.dot(normed, x_weight, preferred_element_type=jnp.float32).astype(jnp.bfloat16)
    bc_proj = jnp.dot(normed, bc_weight, preferred_element_type=jnp.float32).astype(jnp.bfloat16)
    dt_proj = jnp.dot(normed, dt_weight, preferred_element_type=jnp.float32).astype(jnp.bfloat16)
    x_old = conv_x_state[pool_row]
    bc_old = conv_bc_state[pool_row]
    x_conv, x_kept = convolve(x_old, x_proj, conv_x_weight, conv_x_bias)
    bc_conv, bc_kept = convolve(bc_old, bc_proj, conv_bc_weight, conv_bc_bias)
    conv_x_next = conv_x_state.at[pool_row].set(jnp.where(is_live[:, None, None], x_kept, x_old))
    conv_bc_next = conv_bc_state.at[pool_row].set(jnp.where(is_live[:, None, None], bc_kept, bc_old))
    b_rows = bc_conv[:, :NS].astype(jnp.float32)
    c_rows = bc_conv[:, NS:].astype(jnp.float32)
    dt_step = jax.nn.softplus(dt_proj.astype(jnp.float32) + dt_bias)
    decay_rate = jnp.exp(-dt_step * jnp.exp(log_rate))
    x_heads = x_conv.astype(jnp.float32).reshape(BATCH, HEADS, HP)
    old_state = ssm_state[pool_row]
    fresh_state = decay_rate[:, :, None, None] * old_state + (dt_step[:, :, None] * x_heads)[:, :, :, None] * b_rows[:, None, None, :]
    fresh_state = jnp.where(is_live[:, None, None, None], fresh_state, old_state)
    y_heads = jnp.einsum('bhpn,bn->bhp', fresh_state, c_rows, precision=lax.Precision.HIGHEST) + skip_gain[None, :, None] * x_heads
    gated_y = y_heads.reshape(BATCH, INNER) * jax.nn.silu(z_proj.astype(jnp.float32))
    inv_out = lax.rsqrt(lax.optimization_barrier(jnp.mean(gated_y * gated_y, axis=1)) + 1e-05)
    scaled = (gated_y * norm_gain).astype(jnp.bfloat16)
    branch_sum = jnp.dot(scaled, out_weight, preferred_element_type=jnp.float32)
    layer_out = jnp.where(is_live[:, None], (hidden_f32 + inv_out[:, None] * branch_sum).astype(jnp.bfloat16), hidden)
    ssm_next = ssm_state.at[pool_row].set(fresh_state)
    return (layer_out, conv_x_next, conv_bc_next, ssm_next)
```

```python
import functools

import jax
import jax.numpy as jnp
from jax import lax
from jax.experimental import pallas as pl
from jax.experimental.pallas import tpu as pltpu
from jax.sharding import PartitionSpec as P

F32 = jnp.float32
BF16 = jnp.bfloat16
VMEM = pl.BlockSpec(memory_space=pltpu.VMEM)
SMEM = pl.BlockSpec(memory_space=pltpu.SMEM)
ANY = pl.BlockSpec(memory_space=pl.ANY)
HBM = pl.BlockSpec(memory_space=pltpu.HBM)
NT = (((1,), (1,)), ((), ()))
TN = (((0,), (0,)), ((), ()))
STEPS = 4
ROWS = 256


def silu(v):
    return v / (1.0 + jnp.exp(-v))


def softplus(v):
    return jnp.maximum(v, 0.0) + jnp.log1p(jnp.exp(-jnp.abs(v)))


def slot_matrix(slot_row):
    rows = slot_row.shape[1]
    return slot_row == lax.broadcasted_iota(jnp.int32, (rows, rows), 0)


def greet(n):
    me = lax.axis_index("tp")
    barrier = pltpu.get_barrier_semaphore()
    for off in range(1, n):
        pl.semaphore_signal(
            barrier,
            inc=1,
            device_id={"tp": lax.rem(me + off, n)},
            device_id_type=pl.DeviceIdType.MESH,
        )
    pl.semaphore_wait(barrier, n - 1)


def push(src, dst, send, recv, off, n):
    copy = pltpu.make_async_remote_copy(
        src_ref=src,
        dst_ref=dst,
        send_sem=send.at[off],
        recv_sem=recv.at[off],
        device_id={"tp": lax.rem(lax.axis_index("tp") + off, n)},
        device_id_type=pl.DeviceIdType.MESH,
    )
    copy.start()
    return copy


def project_kernel(
    n,
    hidden, gain_h, zw, xw, bcw_h, dtw_h, bc_taps_h, bc_bias_h, bc_state_h, dt_bias_h, log_rate_h,
    slot_h, active_h, state_h,
    z_out, x_out, bcp_out, bc_out, dt_out, decay_out, state_out,
    hid_all, feed, zbuf, xbuf, bc_send, bc_all,
    gain, bcw, dtw, bc_taps, bc_bias, bc_state, dt_bias, log_rate, slot, active,
    zsem, xsem, hs, hr, bs, br, own_sem, small_sem, state_sem,
):
    me = lax.axis_index("tp")
    seqs, feats = hidden.shape
    own = pltpu.make_async_copy(hidden, hid_all.at[me], own_sem)
    own.start()
    smalls = []
    pairs = (
        (slot_h, slot), (active_h, active), (gain_h, gain), (bcw_h, bcw), (dtw_h, dtw),
        (bc_taps_h, bc_taps), (bc_bias_h, bc_bias), (bc_state_h, bc_state),
        (dt_bias_h, dt_bias), (log_rate_h, log_rate),
    )
    for k, (src, dst) in enumerate(pairs):
        copy = pltpu.make_async_copy(src, dst, small_sem.at[k])
        copy.start()
        smalls.append(copy)
    blocks = [lax.rem(me + n - off, n) for off in range(n)]
    loads = []
    for off, block in enumerate(blocks):
        rows = pl.ds(pl.multiple_of(block * feats, feats), feats)
        xc = pltpu.make_async_copy(xw.at[rows, :], xbuf.at[off], xsem.at[off])
        zc = pltpu.make_async_copy(zw.at[rows, :], zbuf.at[off], zsem.at[off])
        xc.start()
        zc.start()
        loads.append((xc, zc))
    state_copy = pltpu.make_async_copy(state_h, state_out, state_sem)
    state_copy.start()
    greet(n)
    own.wait()
    sends = [push(hid_all.at[me], hid_all.at[me], hs, hr, off, n) for off in range(1, n)]
    for copy in smalls:
        copy.wait()
    onehot = slot_matrix(slot[...])
    perm = onehot.astype(F32).astype(BF16)
    live = jnp.sum(jnp.where(onehot, active[...], 0), axis=1, keepdims=True) > 0
    gains = gain[...].reshape(1, -1)
    gains = [gains[:, j * feats : (j + 1) * feats] for j in range(n)]
    own_gain = gains[0]
    for j in range(1, n):
        own_gain = jnp.where(me == j, gains[j], own_gain)

    def fed(block, block_gain):
        return jnp.dot(
            perm, (block.astype(F32) * block_gain).astype(BF16), preferred_element_type=F32
        ).astype(BF16)

    part = fed(hid_all[me], own_gain)
    loads[0][0].wait()
    x = jnp.dot(part, xbuf[0], preferred_element_type=F32)
    loads[0][1].wait()
    z = jnp.dot(part, zbuf[0], preferred_element_type=F32)

    for copy in sends:
        copy.wait()
    squares = jnp.zeros((seqs, 1), F32)
    for j in range(n):
        block = hid_all[j]
        feed[j] = fed(block, gains[j])
        wide = block.astype(F32)
        squares += jnp.sum(wide * wide, axis=1, keepdims=True)
    inv = lax.rsqrt(squares / (n * feats) + 1e-05)
    inv = jnp.dot(
        onehot.astype(F32), jnp.broadcast_to(inv, (seqs, 128)),
        precision=lax.Precision.HIGHEST, preferred_element_type=F32,
    )[:, :1]
    whole = jnp.concatenate([feed[j] for j in range(n)], axis=1)
    bcp = lax.dot_general(whole, bcw[...], NT, preferred_element_type=F32)
    bcp = (bcp * inv).astype(BF16)
    bcp_out[...] = bcp
    acc = bcp.astype(F32) * bc_taps[3:4, :].astype(F32)
    for t in range(3):
        acc += bc_state[t].astype(F32) * bc_taps[t : t + 1, :].astype(F32)
    bc_send[...] = silu(acc + bc_bias[...].astype(F32).reshape(1, -1)).astype(BF16)
    bc_all[me] = bc_send[...]
    dtp = lax.dot_general(whole, dtw[...], NT, preferred_element_type=F32)
    sends = [push(bc_send, bc_all.at[me], bs, br, off, n) for off in range(1, n)]
    dt = softplus((dtp * inv).astype(BF16).astype(F32) + dt_bias[...].reshape(1, -1))
    dt_out[...] = dt
    decay_out[...] = jnp.where(live, jnp.exp(-dt * jnp.exp(log_rate[...].reshape(1, -1))), 1.0)

    for off in range(1, n):
        part = feed[blocks[off]]
        loads[off][0].wait()
        x += jnp.dot(part, xbuf[off], preferred_element_type=F32)
        loads[off][1].wait()
        z += jnp.dot(part, zbuf[off], preferred_element_type=F32)
    z_out[...] = (z * inv).astype(BF16)
    x_out[...] = (x * inv).astype(BF16)
    for copy in sends:
        copy.wait()
    bc_out[...] = jnp.concatenate([bc_all[j] for j in range(n)], axis=1)
    state_copy.wait()


def state_kernel(
    n, group,
    decay, decay_v, dt, z_proj, x_proj, bcp, bc, x_taps, x_bias, x_state, bc_state, skip, norm_gain,
    slot, active, state, out_w,
    x_next, bc_next, state_next, branch, sq,
    st, ow, ut, yb, c_rows, osem, wsem,
):
    seqs, heads, hp, ns = st.shape
    chans = heads * hp
    wcopy = pltpu.make_async_copy(out_w, ow, wsem)
    wcopy.start()

    onehot = slot_matrix(slot[...])
    live = jnp.sum(jnp.where(onehot, active[...], 0), axis=1, keepdims=True) > 0
    x_new = x_proj[...]
    acc = x_new.astype(F32) * x_taps[3:4, :].astype(F32)
    for t in range(3):
        acc += x_state[t].astype(F32) * x_taps[t : t + 1, :].astype(F32)
    xc = silu(acc + x_bias[...].astype(F32).reshape(1, -1)).astype(BF16).astype(F32)
    for old, new, nxt in ((x_state, x_new, x_next), (bc_state, bcp[...], bc_next)):
        nxt[0] = jnp.where(live, old[1], old[0])
        nxt[1] = jnp.where(live, old[2], old[1])
        nxt[2] = jnp.where(live, new, old[2])

    spread = (
        lax.broadcasted_iota(jnp.int32, (heads, chans), 1) // hp
        == lax.broadcasted_iota(jnp.int32, (heads, chans), 0)
    ).astype(F32)
    dt_wide = jnp.dot(dt[...], spread, precision=lax.Precision.HIGHEST, preferred_element_type=F32)
    skip_wide = jnp.dot(
        skip[...], spread, precision=lax.Precision.HIGHEST, preferred_element_type=F32
    )
    decay_wide = jnp.dot(
        decay_v[...], spread, precision=lax.Precision.HIGHEST, preferred_element_type=F32
    )
    u = jnp.where(live, dt_wide * xc, 0.0)
    high = u.astype(BF16).astype(F32)
    ut[...] = jnp.concatenate([high, u - high], axis=0).T.astype(BF16)
    b_rows = bc[:, :ns].astype(F32)
    b_twice = jnp.concatenate([b_rows, b_rows], axis=0)
    row_id = lax.broadcasted_iota(jnp.int32, (2 * seqs, ns), 0)
    c_rows[...] = bc[:, ns:].astype(F32)
    along = jnp.sum(b_rows * c_rows[...], axis=1, keepdims=True)

    def step(b, carry):
        b_one = jnp.where((row_id == b) | (row_id == b + seqs), b_twice, 0.0).astype(BF16)
        c_one = c_rows[pl.ds(b, 1), :].astype(BF16)
        for g in range(heads // group):
            lo = g * group * hp
            width = group * hp
            outer = jnp.dot(ut[lo : lo + width, :], b_one, preferred_element_type=F32)
            heads_here = pl.ds(g * group, group)
            old = state[b, heads_here].reshape(width, ns).astype(BF16)
            yb[pl.ds(b, 1), lo : lo + width] = lax.dot_general(
                c_one, old, NT, preferred_element_type=F32
            )
            for k in range(group):
                h = g * group + k
                st[b, h] = decay[b, h] * state[b, h] + outer[k * hp : (k + 1) * hp, :]
        pltpu.make_async_copy(st.at[b], state_next.at[b], osem.at[b]).start()
        return carry

    lax.fori_loop(0, seqs, step, 0, unroll=4)

    y = decay_wide * yb[...] + u * along + skip_wide * xc
    gated = y * silu(z_proj[...].astype(F32))
    perm = onehot.astype(F32)
    sq_slot = jnp.sum(gated * gated, axis=1, keepdims=True)
    sq_row = jnp.sum(perm * sq_slot, axis=0, keepdims=True)
    eye = lax.broadcasted_iota(jnp.int32, (seqs, seqs), 0) == lax.broadcasted_iota(
        jnp.int32, (seqs, seqs), 1
    )
    sq_col = jnp.sum(jnp.where(eye, sq_row, 0.0), axis=1, keepdims=True)
    sq[...] = jnp.broadcast_to(sq_col, sq.shape)
    scaled = (gated * norm_gain[...].reshape(1, -1)).astype(BF16)
    scaled = lax.dot_general(
        perm.astype(BF16), scaled, TN, preferred_element_type=F32
    ).astype(BF16)
    wcopy.wait()
    width = branch.shape[2]
    for j in range(n):
        branch[j] = jnp.dot(
            scaled, ow[:, j * width : (j + 1) * width], preferred_element_type=F32
        ).astype(BF16)

    def drain(b, carry):
        pltpu.make_async_copy(st.at[b], state_next.at[b], osem.at[b]).wait()
        return carry

    lax.fori_loop(0, seqs, drain, 0)


def reduce_kernel(n, inner, branch, sq, hidden, active, out, parts, sqs, ps, pr, qs, qr):
    me = lax.axis_index("tp")
    greet(n)
    copies = []
    for off in range(1, n):
        peer = lax.rem(me + off, n)
        copies.append(push(branch.at[peer], parts.at[off], ps, pr, off, n))
        copies.append(push(sq, sqs.at[off], qs, qr, off, n))
    rows = hidden.shape[0]
    eye = lax.broadcasted_iota(jnp.int32, (rows, rows), 0) == lax.broadcasted_iota(
        jnp.int32, (rows, rows), 1
    )
    live = jnp.sum(jnp.where(eye, active[...], 0), axis=1, keepdims=True) > 0
    old = hidden[...]
    total = branch[me].astype(F32)
    squares = sq[:, :1]
    for copy in copies:
        copy.wait()
    for off in range(1, n):
        total += parts[off].astype(F32)
        squares += sqs[off][:, :1]
    inv = lax.rsqrt(squares / inner + 1e-05)
    out[...] = jnp.where(live, (old.astype(F32) + inv * total).astype(BF16), old)


def flip(v, k):
    bit = 1
    while bit <= k:
        if k & bit:
            v = v + (1 - 2 * lax.rem(v // bit, 2)) * bit
        bit *= 2
    return v


def swap(src, dst, send, recv, k):
    return pltpu.make_async_remote_copy(
        src_ref=src,
        dst_ref=dst,
        send_sem=send.at[k],
        recv_sem=recv.at[k],
        device_id={"tp": flip(lax.axis_index("tp"), k)},
        device_id_type=pl.DeviceIdType.MESH,
    )


def front_kernel(
    n, steps,
    hidden, gain_h, zw, xw, bcw_h, dtw_h, ow_h, x_taps_h, x_bias_h, x_state_h,
    bc_taps_h, bc_bias_h, bc_state_h, dt_bias_h, log_rate_h, skip_h, norm_gain_h, slot_h, active_h, state_h,
    x_out, bcp_out, ut_out, b_out, dec_out, total_out, sq_out, state_out,
    own, hid, zbuf, xbuf, bcwbuf, dtwbuf, owbuf, bc_send, bc_all, yt, part_send, parts, sq_send, sqs,
    gain, x_taps, x_bias, x_state, bc_taps, bc_bias, bc_state, dt_bias, log_rate, skip, norm_gain, slot, active,
    own_sem, small_sem, xsem, zsem, bcsem, dtsem, ssem, wsem, hs, hr, bs, br, ps, pr, qs, qr,
):
    me = lax.axis_index("tp")
    seqs, feats = hidden.shape
    chans = x_out.shape[1]
    heads = dec_out.shape[0]
    ns = state_h.shape[3]
    hp = chans // heads
    far = list(range(2, n)) + list(range(1, min(n, 2)))
    blocks = [flip(me, k) for k in range(n)]
    spans = [pl.ds(pl.multiple_of(b * feats, feats), feats) for b in blocks]

    own_copy = pltpu.make_async_copy(hidden, own, own_sem)
    own_copy.start()
    pairs = (
        (slot_h, slot), (active_h, active), (gain_h, gain),
        (bc_taps_h, bc_taps), (bc_bias_h, bc_bias), (bc_state_h, bc_state),
        (dt_bias_h, dt_bias), (log_rate_h, log_rate), (skip_h, skip),
        (x_taps_h, x_taps), (x_bias_h, x_bias), (x_state_h, x_state), (norm_gain_h, norm_gain),
    )
    smalls = [pltpu.make_async_copy(s, d, small_sem.at[i]) for i, (s, d) in enumerate(pairs)]
    for copy in smalls:
        copy.start()
    xc = [pltpu.make_async_copy(xw.at[spans[k], :], xbuf.at[k], xsem.at[k]) for k in range(n)]
    zc = [pltpu.make_async_copy(zw.at[spans[k], :], zbuf.at[k], zsem.at[k]) for k in range(n)]
    bcc = [pltpu.make_async_copy(bcw_h.at[:, spans[k]], bcwbuf.at[k], bcsem.at[k]) for k in range(n)]
    dtc = [pltpu.make_async_copy(dtw_h.at[:, spans[k]], dtwbuf.at[k], dtsem.at[k]) for k in range(n)]
    owc = [pltpu.make_async_copy(ow_h.at[:, spans[k]], owbuf.at[k], wsem.at[k]) for k in range(n)]
    span = seqs // steps
    stc = [
        pltpu.make_async_copy(
            state_h.at[pl.ds(q * span, span)], state_out.at[pl.ds(q * span, span)], ssem.at[q]
        )
        for q in range(steps)
    ]
    order = [xc[0], zc[0]] + bcc + dtc
    for k in range(1, n):
        order += [xc[k], zc[k]]
    order += stc + [owc[k] for k in far] + [owc[0]]
    for copy in order:
        copy.start(priority=1)

    barrier = pltpu.get_barrier_semaphore()
    for k in range(1, n):
        pl.semaphore_signal(
            barrier, inc=1, device_id={"tp": blocks[k]}, device_id_type=pl.DeviceIdType.MESH
        )
    own_copy.wait()
    smalls[0].wait()
    onehot = slot_matrix(slot[...])
    perm = onehot.astype(F32).astype(BF16)
    hid[0] = jnp.dot(perm, own[...], preferred_element_type=F32).astype(BF16)
    pl.semaphore_wait(barrier, n - 1)
    hid_swaps = {k: swap(hid.at[0], hid.at[k], hs, hr, k) for k in far}
    for k in far:
        hid_swaps[k].start()

    for copy in smalls[1:]:
        copy.wait()
    live = jnp.sum(jnp.where(onehot, active[...], 0), axis=1, keepdims=True) > 0
    gains = gain[...].reshape(1, -1)
    gains = [gains[:, j * feats : (j + 1) * feats] for j in range(n)]

    def fed(k):
        block_gain = gains[0]
        for j in range(1, n):
            block_gain = jnp.where(blocks[k] == j, gains[j], block_gain)
        return (hid[k].astype(F32) * block_gain).astype(BF16)

    def squared(k):
        wide = hid[k].astype(F32)
        return jnp.sum(wide * wide, axis=1, keepdims=True)

    def narrow(k, part):
        bcc[k].wait()
        dtc[k].wait()
        return (
            lax.dot_general(part, bcwbuf[k], NT, preferred_element_type=F32),
            lax.dot_general(part, dtwbuf[k], NT, preferred_element_type=F32),
        )

    feed = fed(0)
    squares = squared(0)
    xc[0].wait()
    x = jnp.dot(feed, xbuf[0], preferred_element_type=F32)
    zc[0].wait()
    z = jnp.dot(feed, zbuf[0], preferred_element_type=F32)
    bcp, dtp = narrow(0, feed)
    feeds = {}
    for k in [1] + far[:-1]:
        hid_swaps[k].wait_recv()
        feeds[k] = fed(k)
        squares += squared(k)
        more = narrow(k, feeds[k])
        bcp += more[0]
        dtp += more[1]
        if k == 1:
            xc[1].wait()
            x += jnp.dot(feeds[1], xbuf[1], preferred_element_type=F32)
            zc[1].wait()
            z += jnp.dot(feeds[1], zbuf[1], preferred_element_type=F32)
    inv = lax.rsqrt(squares / (n * feats) + 1e-05)
    bcp = (bcp * inv).astype(BF16)
    bcp_out[...] = bcp
    acc = bcp.astype(F32) * bc_taps[3:4, :].astype(F32)
    for t in range(3):
        acc += bc_state[t].astype(F32) * bc_taps[t : t + 1, :].astype(F32)
    bc_send[...] = silu(acc + bc_bias[...].astype(F32).reshape(1, -1)).astype(BF16)
    bc_all[me] = bc_send[...]
    bc_swaps = {k: swap(bc_send, bc_all.at[me], bs, br, k) for k in far}
    for k in far:
        bc_swaps[k].start()

    for k in far[:-1]:
        xc[k].wait()
        x += jnp.dot(feeds[k], xbuf[k], preferred_element_type=F32)
        zc[k].wait()
        z += jnp.dot(feeds[k], zbuf[k], preferred_element_type=F32)
    dt = softplus((dtp * inv).astype(BF16).astype(F32) + dt_bias[...].reshape(1, -1))
    decay = jnp.where(live, jnp.exp(-dt * jnp.exp(log_rate[...].reshape(1, -1))), 1.0)
    for h in range(heads):
        dec_out[h] = jnp.broadcast_to(decay[:, h : h + 1], (seqs, ns))
    spread = (
        lax.broadcasted_iota(jnp.int32, (heads, chans), 1) // hp
        == lax.broadcasted_iota(jnp.int32, (heads, chans), 0)
    ).astype(F32).astype(BF16)
    per_head = jnp.concatenate(
        [dt, decay, jnp.broadcast_to(skip[...].reshape(1, -1), (8, heads))], axis=0
    )
    high = per_head.astype(BF16)
    rest = per_head - high.astype(F32)
    mid = rest.astype(BF16)
    low = (rest - mid.astype(F32)).astype(BF16)
    wide = sum(jnp.dot(v, spread, preferred_element_type=F32) for v in (high, mid, low))
    dt_wide, decay_wide, skip_wide = wide[:seqs], wide[seqs : 2 * seqs], wide[2 * seqs : 2 * seqs + 1]

    x_new = (x * inv).astype(BF16)
    x_out[...] = x_new
    acc = x_new.astype(F32) * x_taps[3:4, :].astype(F32)
    for t in range(3):
        acc += x_state[t].astype(F32) * x_taps[t : t + 1, :].astype(F32)
    conv = silu(acc + x_bias[...].astype(F32).reshape(1, -1)).astype(BF16).astype(F32)
    u = jnp.where(live, dt_wide * conv, 0.0)
    high = u.astype(BF16).astype(F32)
    ut_out[...] = jnp.concatenate([high, u - high], axis=0).T.astype(BF16)
    gate = silu((z * inv).astype(BF16).astype(F32))

    for k in far:
        bc_swaps[k].wait_recv()
    both = jnp.concatenate([bc_all[j] for j in range(n)], axis=1).astype(F32)
    b_rows = both[:, :ns]
    c_rows = both[:, ns:]
    b_out[...] = b_rows
    along = jnp.sum(b_rows * c_rows, axis=1, keepdims=True)
    row_id = lax.broadcasted_iota(jnp.int32, (seqs, ns), 0)
    tile = ROWS if chans % ROWS == 0 else chans
    for q in range(steps):
        stationary = jnp.concatenate(
            [jnp.where(row_id == q * span + i, c_rows, 0.0).astype(BF16) for i in range(span)], axis=1
        )
        stationary = jnp.concatenate(
            [stationary, jnp.zeros((128 - seqs, span * ns), BF16)], axis=0
        )
        stc[q].wait()
        for lo in range(0, chans, tile):
            moving = jnp.concatenate(
                [
                    state_out[q * span + i, lo // hp : (lo + tile) // hp].reshape(tile, ns).astype(BF16)
                    for i in range(span)
                ],
                axis=1,
            )
            got = lax.dot_general(moving, stationary, NT, preferred_element_type=F32)
            if q:
                yt[lo : lo + tile, :] += got
            else:
                yt[lo : lo + tile, :] = got
    old_y = yt[...].T[:seqs]
    y = decay_wide * old_y + u * along + skip_wide * conv
    gated = y * gate
    sq_own = jnp.broadcast_to(jnp.sum(gated * gated, axis=1, keepdims=True), sq_send.shape)
    sq_send[...] = sq_own
    scaled = (gated * norm_gain[...].reshape(1, -1)).astype(BF16)
    tails = []
    for i, k in enumerate(far):
        owc[k].wait()
        part_send[k] = jnp.dot(scaled, owbuf[k], preferred_element_type=F32).astype(BF16)
        if i == 0:
            for j in far:
                tails.append(swap(sq_send, sqs.at[j], qs, qr, j))
                tails[-1].start()
        tails.append(swap(part_send.at[k], parts.at[k], ps, pr, k))
        tails[-1].start()
    owc[0].wait()
    total = jnp.dot(scaled, owbuf[0], preferred_element_type=F32)
    for copies in (hid_swaps, bc_swaps):
        for k in far:
            copies[k].wait_send()
    for copy in tails:
        copy.wait()
    for k in far:
        total += parts[k].astype(F32)
        sq_own += sqs[k]
    total_out[...] = total
    sq_out[...] = sq_own


def back_kernel(
    inner,
    hidden, slot, active, total, sq, x_new, x_state, bcp, bc_state, ut, b_rows, dec, state,
    layer_h, x_next_h, bc_next_h, state_next,
    layer, x_next, bc_next, st, osem, lsem,
):
    seqs, heads, hp, ns = st.shape
    row_id = lax.broadcasted_iota(jnp.int32, (2 * seqs, ns), 0)
    b_twice = jnp.concatenate([b_rows[...], b_rows[...]], axis=0)
    pack = 128 // hp

    def write(p):
        both = pl.ds(2 * p, 2)
        return pltpu.make_async_copy(st.at[both], state_next.at[both], osem.at[p])

    def step(p, carry):
        stationary = jnp.concatenate(
            [
                jnp.where((row_id == 2 * p + i) | (row_id == 2 * p + i + seqs), b_twice, 0.0).astype(BF16)
                for i in range(2)
            ],
            axis=1,
        )
        for lo in range(0, heads, pack):
            outer = jnp.dot(ut[lo * hp : (lo + pack) * hp, :], stationary, preferred_element_type=F32)
            for i in range(2):
                for h in range(pack):
                    st[2 * p + i, lo + h] = (
                        dec[lo + h, pl.ds(2 * p + i, 1), :] * state[2 * p + i, lo + h]
                        + outer[h * hp : (h + 1) * hp, i * ns : (i + 1) * ns]
                    )
        write(p).start()
        return carry

    step(0, 0)
    onehot = slot_matrix(slot[...])
    live = jnp.sum(jnp.where(onehot, active[...], 0), axis=1, keepdims=True) > 0
    for old, new, nxt in ((x_state, x_new[...], x_next), (bc_state, bcp[...], bc_next)):
        nxt[0] = jnp.where(live, old[1], old[0])
        nxt[1] = jnp.where(live, old[2], old[1])
        nxt[2] = jnp.where(live, new, old[2])
    eye = lax.broadcasted_iota(jnp.int32, (seqs, seqs), 0) == lax.broadcasted_iota(
        jnp.int32, (seqs, seqs), 1
    )
    live = jnp.sum(jnp.where(eye, active[...], 0), axis=1, keepdims=True) > 0
    inv = lax.rsqrt(sq[:, :1] / inner + 1e-05)
    delta = lax.dot_general(
        onehot.astype(F32), inv * total[...], TN,
        precision=lax.Precision.HIGHEST, preferred_element_type=F32,
    )
    old = hidden[...]
    layer[...] = jnp.where(live, (old.astype(F32) + delta).astype(BF16), old)
    outs = [
        pltpu.make_async_copy(s, d, lsem.at[i])
        for i, (s, d) in enumerate(((layer, layer_h), (x_next, x_next_h), (bc_next, bc_next_h)))
    ]
    for copy in outs:
        copy.start()
    lax.fori_loop(1, seqs // 2, step, 0)
    for copy in outs:
        copy.wait()

    def drain(p, carry):
        write(p).wait()
        return carry

    lax.fori_loop(0, seqs // 2, drain, 0)


def shards(n, *args):
    hidden, z_weight, ssm_state = args[0], args[2], args[15]
    seqs, feats = hidden.shape
    chans = z_weight.shape[1]
    heads, hp, ns = ssm_state.shape[1:]
    aligned = feats % 128 == 0 and chans % 128 == 0 and ns == 128 and 128 % hp == 0
    if aligned and n > 1 and n & (n - 1) == 0 and seqs % 16 == 0 and seqs <= 128:
        return fast_shards(n, *args)
    return plain_shards(n, *args)


def fast_shards(
    n,
    hidden, in_gain, z_weight, x_weight, bc_weight, dt_weight,
    conv_x_weight, conv_x_bias, conv_bc_weight, conv_bc_bias, conv_x_state, conv_bc_state,
    dt_bias, log_rate, skip_gain, ssm_state, norm_gain, out_weight, pool_slot, active,
):
    seqs, feats = hidden.shape
    model, chans = z_weight.shape
    bc_own = bc_weight.shape[1]
    heads, hp, ns = ssm_state.shape[1:]
    steps = STEPS
    in_hbm = lambda v: pltpu.with_memory_space_constraint(v, pltpu.HBM)
    active = active.reshape(1, -1)
    x_old = jnp.transpose(conv_x_state, (1, 0, 2))
    bc_old = jnp.transpose(conv_bc_state, (1, 0, 2))
    dma = pltpu.SemaphoreType.DMA
    shape = jax.ShapeDtypeStruct
    like = lambda v: pltpu.VMEM(v.shape, v.dtype)
    x_new, bcp, ut, b_rows, dec, total, sq, held = pl.pallas_call(
        functools.partial(front_kernel, n, steps),
        out_shape=(
            shape((seqs, chans), BF16),
            shape((seqs, bc_own), BF16),
            shape((chans, 2 * seqs), BF16),
            shape((seqs, ns), F32),
            shape((heads, seqs, ns), F32),
            shape((seqs, feats), F32),
            shape((seqs, 128), F32),
            pltpu.VMEM(ssm_state.shape, F32),
        ),
        in_specs=[HBM] * 20,
        out_specs=(VMEM,) * 8,
        scratch_shapes=[
            like(hidden),
            pltpu.VMEM((n, seqs, feats), BF16),
            pltpu.VMEM((n, feats, chans), BF16),
            pltpu.VMEM((n, feats, chans), BF16),
            pltpu.VMEM((n, bc_own, feats), BF16),
            pltpu.VMEM((n, heads, feats), BF16),
            pltpu.VMEM((n, chans, feats), BF16),
            pltpu.VMEM((seqs, bc_own), BF16),
            pltpu.VMEM((n, seqs, bc_own), BF16),
            pltpu.VMEM((chans, 128), F32),
            pltpu.VMEM((n, seqs, feats), BF16),
            pltpu.VMEM((n, seqs, feats), BF16),
            pltpu.VMEM((seqs, 128), F32),
            pltpu.VMEM((n, seqs, 128), F32),
            like(in_gain), like(conv_x_weight), like(conv_x_bias), like(x_old),
            like(conv_bc_weight), like(conv_bc_bias), like(bc_old),
            like(dt_bias), like(log_rate), like(skip_gain), like(norm_gain), like(pool_slot), like(active),
            dma(()), dma((13,)), dma((n,)), dma((n,)), dma((n,)), dma((n,)), dma((steps,)), dma((n,)),
            dma((n,)), dma((n,)), dma((n,)), dma((n,)), dma((n,)), dma((n,)), dma((n,)), dma((n,)),
        ],
        compiler_params=pltpu.CompilerParams(
            collective_id=0, has_side_effects=True, vmem_limit_bytes=28 * 2**20
        ),
        name="front",
    )(*map(in_hbm, (
        hidden, in_gain, z_weight, x_weight, bc_weight.T, dt_weight.T, out_weight,
        conv_x_weight, conv_x_bias, x_old, conv_bc_weight, conv_bc_bias, bc_old,
        dt_bias, log_rate, skip_gain, norm_gain, pool_slot, active, ssm_state,
    )))
    layer_out, x_next, bc_next, state_next = pl.pallas_call(
        functools.partial(back_kernel, chans * n),
        out_shape=(
            shape(hidden.shape, BF16),
            shape(x_old.shape, BF16),
            shape(bc_old.shape, BF16),
            shape(ssm_state.shape, F32),
        ),
        in_specs=[VMEM] * 13,
        out_specs=(HBM,) * 4,
        scratch_shapes=[
            like(hidden), like(x_old), like(bc_old), like(ssm_state),
            dma((seqs // 2,)), dma((3,)),
        ],
        compiler_params=pltpu.CompilerParams(vmem_limit_bytes=16 * 2**20),
        name="back",
    )(
        hidden, pool_slot, active, total, sq, x_new, x_old, bcp, bc_old, ut, b_rows, dec, held,
    )
    return (
        layer_out,
        jnp.transpose(x_next, (1, 0, 2)),
        jnp.transpose(bc_next, (1, 0, 2)),
        state_next,
    )


def plain_shards(
    n,
    hidden, in_gain, z_weight, x_weight, bc_weight, dt_weight,
    conv_x_weight, conv_x_bias, conv_bc_weight, conv_bc_bias, conv_x_state, conv_bc_state,
    dt_bias, log_rate, skip_gain, ssm_state, norm_gain, out_weight, pool_slot, active,
):
    seqs, feats = hidden.shape
    model, chans = z_weight.shape
    bc_own = bc_weight.shape[1]
    heads, hp, ns = ssm_state.shape[1:]
    in_hbm = lambda v: pltpu.with_memory_space_constraint(v, pltpu.HBM)
    row = lambda v: v.reshape(1, -1)
    active = row(active)
    x_old = jnp.transpose(conv_x_state, (1, 0, 2))
    bc_old = jnp.transpose(conv_bc_state, (1, 0, 2))
    dma = pltpu.SemaphoreType.DMA
    shape = jax.ShapeDtypeStruct
    z, x, bcp, bc, dt, decay, held = pl.pallas_call(
        functools.partial(project_kernel, n),
        out_shape=(
            shape((seqs, chans), BF16),
            shape((seqs, chans), BF16),
            shape((seqs, bc_own), BF16),
            shape((seqs, bc_own * n), BF16),
            shape((seqs, heads), F32),
            shape((seqs, heads), F32),
            pltpu.VMEM(ssm_state.shape, F32),
        ),
        in_specs=[HBM] * 14,
        out_specs=(VMEM,) * 7,
        scratch_shapes=[
            pltpu.VMEM((n, seqs, feats), BF16),
            pltpu.VMEM((n, seqs, feats), BF16),
            pltpu.VMEM((n, feats, chans), BF16),
            pltpu.VMEM((n, feats, chans), BF16),
            pltpu.VMEM((seqs, bc_own), BF16),
            pltpu.VMEM((n, seqs, bc_own), BF16),
            pltpu.VMEM(in_gain.shape, F32),
            pltpu.VMEM((bc_own, model), BF16),
            pltpu.VMEM((heads, model), BF16),
            pltpu.VMEM(conv_bc_weight.shape, BF16),
            pltpu.VMEM(conv_bc_bias.shape, BF16),
            pltpu.VMEM(bc_old.shape, BF16),
            pltpu.VMEM(dt_bias.shape, F32),
            pltpu.VMEM(log_rate.shape, F32),
            pltpu.VMEM(pool_slot.shape, jnp.int32),
            pltpu.VMEM(active.shape, jnp.int32),
            dma((n,)), dma((n,)), dma((n,)), dma((n,)), dma((n,)), dma((n,)), dma(()), dma((10,)), dma(()),
        ],
        compiler_params=pltpu.CompilerParams(collective_id=0, has_side_effects=True, vmem_limit_bytes=20 * 2**20),
        name="project",
    )(*map(in_hbm, (
        hidden, in_gain, z_weight, x_weight, bc_weight.T, dt_weight.T,
        conv_bc_weight, conv_bc_bias, bc_old, dt_bias, log_rate, pool_slot, active, ssm_state,
    )))
    x_next, bc_next, state_next, branch, sq = pl.pallas_call(
        functools.partial(state_kernel, n, 4 if heads % 4 == 0 else heads),
        out_shape=(
            shape(x_old.shape, BF16),
            shape(bc_old.shape, BF16),
            shape(ssm_state.shape, F32),
            shape((n, seqs, feats), BF16),
            shape((seqs, 128), F32),
        ),
        in_specs=[SMEM] + [VMEM] * 15 + [HBM],
        out_specs=(VMEM, VMEM, HBM, VMEM, VMEM),
        scratch_shapes=[
            pltpu.VMEM(ssm_state.shape, F32),
            pltpu.VMEM(out_weight.shape, BF16),
            pltpu.VMEM((chans, 2 * seqs), BF16),
            pltpu.VMEM((seqs, chans), F32),
            pltpu.VMEM((seqs, ns), F32),
            dma((seqs,)), dma(()),
        ],
        compiler_params=pltpu.CompilerParams(vmem_limit_bytes=20 * 2**20),
        name="state",
    )(
        decay, decay, dt, z, x, bcp, bc, conv_x_weight, conv_x_bias, x_old, bc_old,
        row(skip_gain), norm_gain, pool_slot, active, held, in_hbm(out_weight),
    )
    layer_out = pl.pallas_call(
        functools.partial(reduce_kernel, n, chans * n),
        out_shape=shape((seqs, feats), BF16),
        in_specs=[VMEM] * 4,
        out_specs=VMEM,
        scratch_shapes=[
            pltpu.VMEM((n, seqs, feats), BF16),
            pltpu.VMEM((n, seqs, 128), F32),
            dma((n,)), dma((n,)), dma((n,)), dma((n,)),
        ],
        compiler_params=pltpu.CompilerParams(collective_id=1, has_side_effects=True, vmem_limit_bytes=2 * 2**20),
        name="reduce",
    )(branch, sq, hidden, active)
    return (
        layer_out,
        jnp.transpose(x_next, (1, 0, 2)),
        jnp.transpose(bc_next, (1, 0, 2)),
        state_next,
    )


def solution(mesh):
    rows = ("groups", "dp")
    placed = (
        P(rows, "tp"), P(), P(None, "tp"), P(None, "tp"), P(None, "tp"), P(None, "tp"),
        P(None, "tp"), P("tp"), P(None, "tp"), P("tp"),
        P(rows, None, "tp"), P(rows, None, "tp"),
        P("tp"), P("tp"), P("tp"), P(rows, "tp", None, None), P("tp"), P("tp", None),
        P(rows, None), P(rows),
    )
    return jax.shard_map(
        functools.partial(shards, mesh.shape["tp"]),
        mesh=mesh,
        in_specs=placed,
        out_specs=(
            P(rows, "tp"), P(rows, None, "tp"), P(rows, None, "tp"), P(rows, "tp", None, None),
        ),
        check_vma=False,
    )
```

```python
import functools

import jax
import jax.numpy as jnp
from jax import lax
from jax.experimental import pallas as pl
from jax.experimental.pallas import tpu as pltpu
from jax.sharding import PartitionSpec as P

F32 = jnp.float32
BF16 = jnp.bfloat16
VMEM = pl.BlockSpec(memory_space=pltpu.VMEM)
SMEM = pl.BlockSpec(memory_space=pltpu.SMEM)
ANY = pl.BlockSpec(memory_space=pl.ANY)
HBM = pl.BlockSpec(memory_space=pltpu.HBM)
NT = (((1,), (1,)), ((), ()))
TN = (((0,), (0,)), ((), ()))
STEPS = 4
ROWS = 256


def silu(v):
    return v / (1.0 + jnp.exp(-v))


def softplus(v):
    return jnp.maximum(v, 0.0) + jnp.log1p(jnp.exp(-jnp.abs(v)))


def slot_matrix(slot_row):
    rows = slot_row.shape[1]
    return slot_row == lax.broadcasted_iota(jnp.int32, (rows, rows), 0)


def greet(n):
    me = lax.axis_index("tp")
    barrier = pltpu.get_barrier_semaphore()
    for off in range(1, n):
        pl.semaphore_signal(
            barrier,
            inc=1,
            device_id={"tp": lax.rem(me + off, n)},
            device_id_type=pl.DeviceIdType.MESH,
        )
    pl.semaphore_wait(barrier, n - 1)


def push(src, dst, send, recv, off, n):
    copy = pltpu.make_async_remote_copy(
        src_ref=src,
        dst_ref=dst,
        send_sem=send.at[off],
        recv_sem=recv.at[off],
        device_id={"tp": lax.rem(lax.axis_index("tp") + off, n)},
        device_id_type=pl.DeviceIdType.MESH,
    )
    copy.start()
    return copy


def project_kernel(
    n,
    hidden, gain_h, zw, xw, bcw_h, dtw_h, bc_taps_h, bc_bias_h, bc_state_h, dt_bias_h, log_rate_h,
    slot_h, active_h, state_h,
    z_out, x_out, bcp_out, bc_out, dt_out, decay_out, state_out,
    hid_all, feed, zbuf, xbuf, bc_send, bc_all,
    gain, bcw, dtw, bc_taps, bc_bias, bc_state, dt_bias, log_rate, slot, active,
    zsem, xsem, hs, hr, bs, br, own_sem, small_sem, state_sem,
):
    me = lax.axis_index("tp")
    seqs, feats = hidden.shape
    own = pltpu.make_async_copy(hidden, hid_all.at[me], own_sem)
    own.start()
    smalls = []
    pairs = (
        (slot_h, slot), (active_h, active), (gain_h, gain), (bcw_h, bcw), (dtw_h, dtw),
        (bc_taps_h, bc_taps), (bc_bias_h, bc_bias), (bc_state_h, bc_state),
        (dt_bias_h, dt_bias), (log_rate_h, log_rate),
    )
    for k, (src, dst) in enumerate(pairs):
        copy = pltpu.make_async_copy(src, dst, small_sem.at[k])
        copy.start()
        smalls.append(copy)
    blocks = [lax.rem(me + n - off, n) for off in range(n)]
    loads = []
    for off, block in enumerate(blocks):
        rows = pl.ds(pl.multiple_of(block * feats, feats), feats)
        xc = pltpu.make_async_copy(xw.at[rows, :], xbuf.at[off], xsem.at[off])
        zc = pltpu.make_async_copy(zw.at[rows, :], zbuf.at[off], zsem.at[off])
        xc.start()
        zc.start()
        loads.append((xc, zc))
    state_copy = pltpu.make_async_copy(state_h, state_out, state_sem)
    state_copy.start()
    greet(n)
    own.wait()
    sends = [push(hid_all.at[me], hid_all.at[me], hs, hr, off, n) for off in range(1, n)]
    for copy in smalls:
        copy.wait()
    onehot = slot_matrix(slot[...])
    perm = onehot.astype(F32).astype(BF16)
    live = jnp.sum(jnp.where(onehot, active[...], 0), axis=1, keepdims=True) > 0
    gains = gain[...].reshape(1, -1)
    gains = [gains[:, j * feats : (j + 1) * feats] for j in range(n)]
    own_gain = gains[0]
    for j in range(1, n):
        own_gain = jnp.where(me == j, gains[j], own_gain)

    def fed(block, block_gain):
        return jnp.dot(
            perm, (block.astype(F32) * block_gain).astype(BF16), preferred_element_type=F32
        ).astype(BF16)

    part = fed(hid_all[me], own_gain)
    loads[0][0].wait()
    x = jnp.dot(part, xbuf[0], preferred_element_type=F32)
    loads[0][1].wait()
    z = jnp.dot(part, zbuf[0], preferred_element_type=F32)

    for copy in sends:
        copy.wait()
    squares = jnp.zeros((seqs, 1), F32)
    for j in range(n):
        block = hid_all[j]
        feed[j] = fed(block, gains[j])
        wide = block.astype(F32)
        squares += jnp.sum(wide * wide, axis=1, keepdims=True)
    inv = lax.rsqrt(squares / (n * feats) + 1e-05)
    inv = jnp.dot(
        onehot.astype(F32), jnp.broadcast_to(inv, (seqs, 128)),
        precision=lax.Precision.HIGHEST, preferred_element_type=F32,
    )[:, :1]
    whole = jnp.concatenate([feed[j] for j in range(n)], axis=1)
    bcp = lax.dot_general(whole, bcw[...], NT, preferred_element_type=F32)
    bcp = (bcp * inv).astype(BF16)
    bcp_out[...] = bcp
    acc = bcp.astype(F32) * bc_taps[3:4, :].astype(F32)
    for t in range(3):
        acc += bc_state[t].astype(F32) * bc_taps[t : t + 1, :].astype(F32)
    bc_send[...] = silu(acc + bc_bias[...].astype(F32).reshape(1, -1)).astype(BF16)
    bc_all[me] = bc_send[...]
    dtp = lax.dot_general(whole, dtw[...], NT, preferred_element_type=F32)
    sends = [push(bc_send, bc_all.at[me], bs, br, off, n) for off in range(1, n)]
    dt = softplus((dtp * inv).astype(BF16).astype(F32) + dt_bias[...].reshape(1, -1))
    dt_out[...] = dt
    decay_out[...] = jnp.where(live, jnp.exp(-dt * jnp.exp(log_rate[...].reshape(1, -1))), 1.0)

    for off in range(1, n):
        part = feed[blocks[off]]
        loads[off][0].wait()
        x += jnp.dot(part, xbuf[off], preferred_element_type=F32)
        loads[off][1].wait()
        z += jnp.dot(part, zbuf[off], preferred_element_type=F32)
    z_out[...] = (z * inv).astype(BF16)
    x_out[...] = (x * inv).astype(BF16)
    for copy in sends:
        copy.wait()
    bc_out[...] = jnp.concatenate([bc_all[j] for j in range(n)], axis=1)
    state_copy.wait()


def state_kernel(
    n, group,
    decay, decay_v, dt, z_proj, x_proj, bcp, bc, x_taps, x_bias, x_state, bc_state, skip, norm_gain,
    slot, active, state, out_w,
    x_next, bc_next, state_next, branch, sq,
    st, ow, ut, yb, c_rows, osem, wsem,
):
    seqs, heads, hp, ns = st.shape
    chans = heads * hp
    wcopy = pltpu.make_async_copy(out_w, ow, wsem)
    wcopy.start()

    onehot = slot_matrix(slot[...])
    live = jnp.sum(jnp.where(onehot, active[...], 0), axis=1, keepdims=True) > 0
    x_new = x_proj[...]
    acc = x_new.astype(F32) * x_taps[3:4, :].astype(F32)
    for t in range(3):
        acc += x_state[t].astype(F32) * x_taps[t : t + 1, :].astype(F32)
    xc = silu(acc + x_bias[...].astype(F32).reshape(1, -1)).astype(BF16).astype(F32)
    for old, new, nxt in ((x_state, x_new, x_next), (bc_state, bcp[...], bc_next)):
        nxt[0] = jnp.where(live, old[1], old[0])
        nxt[1] = jnp.where(live, old[2], old[1])
        nxt[2] = jnp.where(live, new, old[2])

    spread = (
        lax.broadcasted_iota(jnp.int32, (heads, chans), 1) // hp
        == lax.broadcasted_iota(jnp.int32, (heads, chans), 0)
    ).astype(F32)
    dt_wide = jnp.dot(dt[...], spread, precision=lax.Precision.HIGHEST, preferred_element_type=F32)
    skip_wide = jnp.dot(
        skip[...], spread, precision=lax.Precision.HIGHEST, preferred_element_type=F32
    )
    decay_wide = jnp.dot(
        decay_v[...], spread, precision=lax.Precision.HIGHEST, preferred_element_type=F32
    )
    u = jnp.where(live, dt_wide * xc, 0.0)
    high = u.astype(BF16).astype(F32)
    ut[...] = jnp.concatenate([high, u - high], axis=0).T.astype(BF16)
    b_rows = bc[:, :ns].astype(F32)
    b_twice = jnp.concatenate([b_rows, b_rows], axis=0)
    row_id = lax.broadcasted_iota(jnp.int32, (2 * seqs, ns), 0)
    c_rows[...] = bc[:, ns:].astype(F32)
    along = jnp.sum(b_rows * c_rows[...], axis=1, keepdims=True)

    def step(b, carry):
        b_one = jnp.where((row_id == b) | (row_id == b + seqs), b_twice, 0.0).astype(BF16)
        c_one = c_rows[pl.ds(b, 1), :].astype(BF16)
        for g in range(heads // group):
            lo = g * group * hp
            width = group * hp
            outer = jnp.dot(ut[lo : lo + width, :], b_one, preferred_element_type=F32)
            heads_here = pl.ds(g * group, group)
            old = state[b, heads_here].reshape(width, ns).astype(BF16)
            yb[pl.ds(b, 1), lo : lo + width] = lax.dot_general(
                c_one, old, NT, preferred_element_type=F32
            )
            for k in range(group):
                h = g * group + k
                st[b, h] = decay[b, h] * state[b, h] + outer[k * hp : (k + 1) * hp, :]
        pltpu.make_async_copy(st.at[b], state_next.at[b], osem.at[b]).start()
        return carry

    lax.fori_loop(0, seqs, step, 0, unroll=4)

    y = decay_wide * yb[...] + u * along + skip_wide * xc
    gated = y * silu(z_proj[...].astype(F32))
    perm = onehot.astype(F32)
    sq_slot = jnp.sum(gated * gated, axis=1, keepdims=True)
    sq_row = jnp.sum(perm * sq_slot, axis=0, keepdims=True)
    eye = lax.broadcasted_iota(jnp.int32, (seqs, seqs), 0) == lax.broadcasted_iota(
        jnp.int32, (seqs, seqs), 1
    )
    sq_col = jnp.sum(jnp.where(eye, sq_row, 0.0), axis=1, keepdims=True)
    sq[...] = jnp.broadcast_to(sq_col, sq.shape)
    scaled = (gated * norm_gain[...].reshape(1, -1)).astype(BF16)
    scaled = lax.dot_general(
        perm.astype(BF16), scaled, TN, preferred_element_type=F32
    ).astype(BF16)
    wcopy.wait()
    width = branch.shape[2]
    for j in range(n):
        branch[j] = jnp.dot(
            scaled, ow[:, j * width : (j + 1) * width], preferred_element_type=F32
        ).astype(BF16)

    def drain(b, carry):
        pltpu.make_async_copy(st.at[b], state_next.at[b], osem.at[b]).wait()
        return carry

    lax.fori_loop(0, seqs, drain, 0)


def reduce_kernel(n, inner, branch, sq, hidden, active, out, parts, sqs, ps, pr, qs, qr):
    me = lax.axis_index("tp")
    greet(n)
    copies = []
    for off in range(1, n):
        peer = lax.rem(me + off, n)
        copies.append(push(branch.at[peer], parts.at[off], ps, pr, off, n))
        copies.append(push(sq, sqs.at[off], qs, qr, off, n))
    rows = hidden.shape[0]
    eye = lax.broadcasted_iota(jnp.int32, (rows, rows), 0) == lax.broadcasted_iota(
        jnp.int32, (rows, rows), 1
    )
    live = jnp.sum(jnp.where(eye, active[...], 0), axis=1, keepdims=True) > 0
    old = hidden[...]
    total = branch[me].astype(F32)
    squares = sq[:, :1]
    for copy in copies:
        copy.wait()
    for off in range(1, n):
        total += parts[off].astype(F32)
        squares += sqs[off][:, :1]
    inv = lax.rsqrt(squares / inner + 1e-05)
    out[...] = jnp.where(live, (old.astype(F32) + inv * total).astype(BF16), old)


def flip(v, k):
    bit = 1
    while bit <= k:
        if k & bit:
            v = v + (1 - 2 * lax.rem(v // bit, 2)) * bit
        bit *= 2
    return v


def swap(src, dst, send, recv, k):
    return pltpu.make_async_remote_copy(
        src_ref=src,
        dst_ref=dst,
        send_sem=send.at[k],
        recv_sem=recv.at[k],
        device_id={"tp": flip(lax.axis_index("tp"), k)},
        device_id_type=pl.DeviceIdType.MESH,
    )


def front_kernel(
    n, steps,
    hidden, gain_h, zw, xw, bcw_h, dtw_h, ow_h, x_taps_h, x_bias_h, x_state_h,
    bc_taps_h, bc_bias_h, bc_state_h, dt_bias_h, log_rate_h, skip_h, norm_gain_h, slot_h, active_h, state_h,
    x_out, bcp_out, ut_out, b_out, dec_out, mine_out, sq_send, parts, sqs, state_out,
    own, hid, zbuf, xbuf, bcw, dtw, owbuf, bc_send, bc_all, yt, part_send,
    gain, x_taps, x_bias, x_state, bc_taps, bc_bias, bc_state, dt_bias, log_rate, skip, norm_gain, slot, active,
    own_sem, small_sem, xsem, zsem, ssem, wsem, hs, hr, bs, br, ps, pr, qs, qr,
):
    me = lax.axis_index("tp")
    seqs, feats = hidden.shape
    chans = x_out.shape[1]
    heads = dec_out.shape[0]
    ns = state_h.shape[3]
    hp = chans // heads
    far = list(range(2, n)) + list(range(1, min(n, 2)))
    blocks = [flip(me, k) for k in range(n)]
    spans = [pl.ds(pl.multiple_of(b * feats, feats), feats) for b in blocks]

    own_copy = pltpu.make_async_copy(hidden, own, own_sem)
    own_copy.start()
    pairs = (
        (slot_h, slot), (active_h, active), (gain_h, gain),
        (bc_taps_h, bc_taps), (bc_bias_h, bc_bias), (bc_state_h, bc_state),
        (dt_bias_h, dt_bias), (log_rate_h, log_rate), (skip_h, skip), (bcw_h, bcw), (dtw_h, dtw),
        (x_taps_h, x_taps), (x_bias_h, x_bias), (x_state_h, x_state), (norm_gain_h, norm_gain),
    )
    smalls = [pltpu.make_async_copy(s, d, small_sem.at[i]) for i, (s, d) in enumerate(pairs)]
    for copy in smalls:
        copy.start()
    xc = [pltpu.make_async_copy(xw.at[spans[k], :], xbuf.at[k], xsem.at[k]) for k in range(n)]
    zc = [pltpu.make_async_copy(zw.at[spans[k], :], zbuf.at[k], zsem.at[k]) for k in range(n)]
    owc = [pltpu.make_async_copy(ow_h.at[:, spans[k]], owbuf.at[k], wsem.at[k]) for k in range(n)]
    span = seqs // steps
    stc = [
        pltpu.make_async_copy(
            state_h.at[pl.ds(q * span, span)], state_out.at[pl.ds(q * span, span)], ssem.at[q]
        )
        for q in range(steps)
    ]

    def stream(copies):
        for copy in copies:
            copy.start(priority=1)

    for k in range(n):
        stream([xc[k], zc[k]])

    barrier = pltpu.get_barrier_semaphore()
    for k in range(1, n):
        pl.semaphore_signal(
            barrier, inc=1, device_id={"tp": blocks[k]}, device_id_type=pl.DeviceIdType.MESH
        )
    own_copy.wait()
    smalls[0].wait()
    onehot = slot_matrix(slot[...])
    perm = onehot.astype(F32).astype(BF16)
    hid[0] = jnp.dot(perm, own[...], preferred_element_type=F32).astype(BF16)
    pl.semaphore_wait(barrier, n - 1)
    hid_swaps = {k: swap(hid.at[0], hid.at[k], hs, hr, k) for k in far}
    for k in far:
        hid_swaps[k].start()

    for copy in smalls[1:]:
        copy.wait()
    live = jnp.sum(jnp.where(onehot, active[...], 0), axis=1, keepdims=True) > 0
    gains = gain[...].reshape(1, -1)
    gains = [gains[:, j * feats : (j + 1) * feats] for j in range(n)]

    def fed(k):
        block_gain = gains[0]
        for j in range(1, n):
            block_gain = jnp.where(blocks[k] == j, gains[j], block_gain)
        return (hid[k].astype(F32) * block_gain).astype(BF16)

    def squared(k):
        wide = hid[k].astype(F32)
        return jnp.sum(wide * wide, axis=1, keepdims=True)

    def narrow(k, part):
        return (
            lax.dot_general(part, bcw[:, spans[k]], NT, preferred_element_type=F32),
            lax.dot_general(part, dtw[:, spans[k]], NT, preferred_element_type=F32),
        )

    feed = fed(0)
    squares = squared(0)
    xc[0].wait()
    x = jnp.dot(feed, xbuf[0], preferred_element_type=F32)
    zc[0].wait()
    z = jnp.dot(feed, zbuf[0], preferred_element_type=F32)
    bcp, dtp = narrow(0, feed)
    feeds = {}
    for k in [1] + far[:-1]:
        hid_swaps[k].wait_recv()
        feeds[k] = fed(k)
        squares += squared(k)
        more = narrow(k, feeds[k])
        bcp += more[0]
        dtp += more[1]
        if k == 1:
            xc[1].wait()
            x += jnp.dot(feeds[1], xbuf[1], preferred_element_type=F32)
            stream(stc[: steps // 2])
            zc[1].wait()
            z += jnp.dot(feeds[1], zbuf[1], preferred_element_type=F32)
    inv = lax.rsqrt(squares / (n * feats) + 1e-05)
    bcp = (bcp * inv).astype(BF16)
    bcp_out[...] = bcp
    acc = bcp.astype(F32) * bc_taps[3:4, :].astype(F32)
    for t in range(3):
        acc += bc_state[t].astype(F32) * bc_taps[t : t + 1, :].astype(F32)
    bc_send[...] = silu(acc + bc_bias[...].astype(F32).reshape(1, -1)).astype(BF16)
    bc_all[me] = bc_send[...]
    bc_swaps = {k: swap(bc_send, bc_all.at[me], bs, br, k) for k in far}
    for k in far:
        bc_swaps[k].start()
    stream(stc[steps // 2 :])

    for k in far[:-1]:
        xc[k].wait()
        x += jnp.dot(feeds[k], xbuf[k], preferred_element_type=F32)
        zc[k].wait()
        z += jnp.dot(feeds[k], zbuf[k], preferred_element_type=F32)
    stream([owc[k] for k in far[:2]])
    dt = softplus((dtp * inv).astype(BF16).astype(F32) + dt_bias[...].reshape(1, -1))
    decay = jnp.where(live, jnp.exp(-dt * jnp.exp(log_rate[...].reshape(1, -1))), 1.0)
    for h in range(heads):
        dec_out[h] = jnp.broadcast_to(decay[:, h : h + 1], (seqs, ns))
    spread = (
        lax.broadcasted_iota(jnp.int32, (heads, chans), 1) // hp
        == lax.broadcasted_iota(jnp.int32, (heads, chans), 0)
    ).astype(F32).astype(BF16)
    per_head = jnp.concatenate(
        [dt, decay, jnp.broadcast_to(skip[...].reshape(1, -1), (8, heads))], axis=0
    )
    high = per_head.astype(BF16)
    rest = per_head - high.astype(F32)
    mid = rest.astype(BF16)
    low = (rest - mid.astype(F32)).astype(BF16)
    wide = sum(jnp.dot(v, spread, preferred_element_type=F32) for v in (high, mid, low))
    dt_wide, decay_wide, skip_wide = wide[:seqs], wide[seqs : 2 * seqs], wide[2 * seqs : 2 * seqs + 1]

    x_new = (x * inv).astype(BF16)
    x_out[...] = x_new
    acc = x_new.astype(F32) * x_taps[3:4, :].astype(F32)
    for t in range(3):
        acc += x_state[t].astype(F32) * x_taps[t : t + 1, :].astype(F32)
    conv = silu(acc + x_bias[...].astype(F32).reshape(1, -1)).astype(BF16).astype(F32)
    u = jnp.where(live, dt_wide * conv, 0.0)
    high = u.astype(BF16).astype(F32)
    ut_out[...] = jnp.concatenate([high, u - high], axis=0).T.astype(BF16)
    gate = silu((z * inv).astype(BF16).astype(F32))

    for k in far:
        bc_swaps[k].wait_recv()
    stream([owc[k] for k in far[2:] + [0]])
    both = jnp.concatenate([bc_all[j] for j in range(n)], axis=1).astype(F32)
    b_rows = both[:, :ns]
    c_rows = both[:, ns:]
    b_out[...] = b_rows
    along = jnp.sum(b_rows * c_rows, axis=1, keepdims=True)
    row_id = lax.broadcasted_iota(jnp.int32, (seqs, ns), 0)
    tile = ROWS if chans % ROWS == 0 else chans
    for q in range(steps):
        stationary = jnp.concatenate(
            [jnp.where(row_id == q * span + i, c_rows, 0.0).astype(BF16) for i in range(span)], axis=1
        )
        stationary = jnp.concatenate(
            [stationary, jnp.zeros((128 - seqs, span * ns), BF16)], axis=0
        )
        stc[q].wait()
        for lo in range(0, chans, tile):
            moving = jnp.concatenate(
                [
                    state_out[q * span + i, lo // hp : (lo + tile) // hp].reshape(tile, ns).astype(BF16)
                    for i in range(span)
                ],
                axis=1,
            )
            got = lax.dot_general(moving, stationary, NT, preferred_element_type=F32)
            if q:
                yt[lo : lo + tile, :] += got
            else:
                yt[lo : lo + tile, :] = got
    old_y = yt[...].T[:seqs]
    y = decay_wide * old_y + u * along + skip_wide * conv
    gated = y * gate
    sq_send[...] = jnp.broadcast_to(jnp.sum(gated * gated, axis=1, keepdims=True), sq_send.shape)
    scaled = (gated * norm_gain[...].reshape(1, -1)).astype(BF16)
    tails = []
    for i, k in enumerate(far):
        owc[k].wait()
        part_send[k] = jnp.dot(scaled, owbuf[k], preferred_element_type=F32).astype(BF16)
        if i == 0:
            for j in far:
                tails.append(swap(sq_send, sqs.at[j - 1], qs, qr, j))
                tails[-1].start()
        tails.append(swap(part_send.at[k], parts.at[k - 1], ps, pr, k))
        tails[-1].start()
    owc[0].wait()
    mine_out[...] = jnp.dot(scaled, owbuf[0], preferred_element_type=F32)
    for copies in (hid_swaps, bc_swaps):
        for k in far:
            copies[k].wait_send()
    for copy in tails:
        copy.wait()


def back_kernel(
    inner,
    hidden, slot, active, mine, sq, parts, sqs, x_new, x_state, bcp, bc_state, ut, b_rows, dec, state,
    layer_h, x_next_h, bc_next_h, state_next,
    layer, x_next, bc_next, st, osem, lsem,
):
    seqs, heads, hp, ns = st.shape
    row_id = lax.broadcasted_iota(jnp.int32, (2 * seqs, ns), 0)
    b_twice = jnp.concatenate([b_rows[...], b_rows[...]], axis=0)
    pack = 128 // hp

    def write(p):
        both = pl.ds(2 * p, 2)
        return pltpu.make_async_copy(st.at[both], state_next.at[both], osem.at[p])

    def step(p, carry):
        stationary = jnp.concatenate(
            [
                jnp.where((row_id == 2 * p + i) | (row_id == 2 * p + i + seqs), b_twice, 0.0).astype(BF16)
                for i in range(2)
            ],
            axis=1,
        )
        for lo in range(0, heads, pack):
            outer = jnp.dot(ut[lo * hp : (lo + pack) * hp, :], stationary, preferred_element_type=F32)
            for i in range(2):
                for h in range(pack):
                    st[2 * p + i, lo + h] = (
                        dec[lo + h, pl.ds(2 * p + i, 1), :] * state[2 * p + i, lo + h]
                        + outer[h * hp : (h + 1) * hp, i * ns : (i + 1) * ns]
                    )
        write(p).start()
        return carry

    step(0, 0)
    onehot = slot_matrix(slot[...])
    live = jnp.sum(jnp.where(onehot, active[...], 0), axis=1, keepdims=True) > 0
    for old, new, nxt in ((x_state, x_new[...], x_next), (bc_state, bcp[...], bc_next)):
        nxt[0] = jnp.where(live, old[1], old[0])
        nxt[1] = jnp.where(live, old[2], old[1])
        nxt[2] = jnp.where(live, new, old[2])
    eye = lax.broadcasted_iota(jnp.int32, (seqs, seqs), 0) == lax.broadcasted_iota(
        jnp.int32, (seqs, seqs), 1
    )
    live = jnp.sum(jnp.where(eye, active[...], 0), axis=1, keepdims=True) > 0
    total = mine[...]
    squares = sq[:, :1]
    for k in range(parts.shape[0]):
        total += parts[k].astype(F32)
        squares += sqs[k][:, :1]
    inv = lax.rsqrt(squares / inner + 1e-05)
    delta = lax.dot_general(
        onehot.astype(F32), inv * total, TN,
        precision=lax.Precision.HIGHEST, preferred_element_type=F32,
    )
    old = hidden[...]
    layer[...] = jnp.where(live, (old.astype(F32) + delta).astype(BF16), old)
    outs = [
        pltpu.make_async_copy(s, d, lsem.at[i])
        for i, (s, d) in enumerate(((layer, layer_h), (x_next, x_next_h), (bc_next, bc_next_h)))
    ]
    for copy in outs:
        copy.start()
    lax.fori_loop(1, seqs // 2, step, 0)
    for copy in outs:
        copy.wait()

    def drain(p, carry):
        write(p).wait()
        return carry

    lax.fori_loop(0, seqs // 2, drain, 0)


def shards(n, *args):
    hidden, z_weight, ssm_state = args[0], args[2], args[15]
    seqs, feats = hidden.shape
    chans = z_weight.shape[1]
    heads, hp, ns = ssm_state.shape[1:]
    aligned = feats % 128 == 0 and chans % 128 == 0 and ns == 128 and 128 % hp == 0
    if aligned and n > 1 and n & (n - 1) == 0 and seqs % 16 == 0 and seqs <= 128:
        return fast_shards(n, *args)
    return plain_shards(n, *args)


def fast_shards(
    n,
    hidden, in_gain, z_weight, x_weight, bc_weight, dt_weight,
    conv_x_weight, conv_x_bias, conv_bc_weight, conv_bc_bias, conv_x_state, conv_bc_state,
    dt_bias, log_rate, skip_gain, ssm_state, norm_gain, out_weight, pool_slot, active,
):
    seqs, feats = hidden.shape
    model, chans = z_weight.shape
    bc_own = bc_weight.shape[1]
    heads, hp, ns = ssm_state.shape[1:]
    steps = STEPS
    in_hbm = lambda v: pltpu.with_memory_space_constraint(v, pltpu.HBM)
    active = active.reshape(1, -1)
    x_old = jnp.transpose(conv_x_state, (1, 0, 2))
    bc_old = jnp.transpose(conv_bc_state, (1, 0, 2))
    dma = pltpu.SemaphoreType.DMA
    shape = jax.ShapeDtypeStruct
    like = lambda v: pltpu.VMEM(v.shape, v.dtype)
    x_new, bcp, ut, b_rows, dec, mine, sq, parts, sqs, held = pl.pallas_call(
        functools.partial(front_kernel, n, steps),
        out_shape=(
            pltpu.VMEM((seqs, chans), BF16),
            pltpu.VMEM((seqs, bc_own), BF16),
            pltpu.VMEM((chans, 2 * seqs), BF16),
            pltpu.VMEM((seqs, ns), F32),
            pltpu.VMEM((heads, seqs, ns), F32),
            pltpu.VMEM((seqs, feats), F32),
            pltpu.VMEM((seqs, 128), F32),
            pltpu.VMEM((n - 1, seqs, feats), BF16),
            pltpu.VMEM((n - 1, seqs, 128), F32),
            pltpu.VMEM(ssm_state.shape, F32),
        ),
        in_specs=[HBM] * 20,
        out_specs=(VMEM,) * 10,
        scratch_shapes=[
            like(hidden),
            pltpu.VMEM((n, seqs, feats), BF16),
            pltpu.VMEM((n, feats, chans), BF16),
            pltpu.VMEM((n, feats, chans), BF16),
            pltpu.VMEM((bc_own, model), BF16),
            pltpu.VMEM((heads, model), BF16),
            pltpu.VMEM((n, chans, feats), BF16),
            pltpu.VMEM((seqs, bc_own), BF16),
            pltpu.VMEM((n, seqs, bc_own), BF16),
            pltpu.VMEM((chans, 128), F32),
            pltpu.VMEM((n, seqs, feats), BF16),
            like(in_gain), like(conv_x_weight), like(conv_x_bias), like(x_old),
            like(conv_bc_weight), like(conv_bc_bias), like(bc_old),
            like(dt_bias), like(log_rate), like(skip_gain), like(norm_gain), like(pool_slot), like(active),
            dma(()), dma((15,)), dma((n,)), dma((n,)), dma((steps,)), dma((n,)),
            dma((n,)), dma((n,)), dma((n,)), dma((n,)), dma((n,)), dma((n,)), dma((n,)), dma((n,)),
        ],
        compiler_params=pltpu.CompilerParams(
            collective_id=0, has_side_effects=True, vmem_limit_bytes=28 * 2**20
        ),
        name="front",
    )(*map(in_hbm, (
        hidden, in_gain, z_weight, x_weight, bc_weight.T, dt_weight.T, out_weight,
        conv_x_weight, conv_x_bias, x_old, conv_bc_weight, conv_bc_bias, bc_old,
        dt_bias, log_rate, skip_gain, norm_gain, pool_slot, active, ssm_state,
    )))
    layer_out, x_next, bc_next, state_next = pl.pallas_call(
        functools.partial(back_kernel, chans * n),
        out_shape=(
            shape(hidden.shape, BF16),
            shape(x_old.shape, BF16),
            shape(bc_old.shape, BF16),
            shape(ssm_state.shape, F32),
        ),
        in_specs=[VMEM] * 15,
        out_specs=(HBM,) * 4,
        scratch_shapes=[
            like(hidden), like(x_old), like(bc_old), like(ssm_state),
            dma((seqs // 2,)), dma((3,)),
        ],
        compiler_params=pltpu.CompilerParams(vmem_limit_bytes=16 * 2**20),
        name="back",
    )(
        hidden, pool_slot, active, mine, sq, parts, sqs, x_new, x_old, bcp, bc_old, ut, b_rows, dec, held,
    )
    return (
        layer_out,
        jnp.transpose(x_next, (1, 0, 2)),
        jnp.transpose(bc_next, (1, 0, 2)),
        state_next,
    )


def plain_shards(
    n,
    hidden, in_gain, z_weight, x_weight, bc_weight, dt_weight,
    conv_x_weight, conv_x_bias, conv_bc_weight, conv_bc_bias, conv_x_state, conv_bc_state,
    dt_bias, log_rate, skip_gain, ssm_state, norm_gain, out_weight, pool_slot, active,
):
    seqs, feats = hidden.shape
    model, chans = z_weight.shape
    bc_own = bc_weight.shape[1]
    heads, hp, ns = ssm_state.shape[1:]
    in_hbm = lambda v: pltpu.with_memory_space_constraint(v, pltpu.HBM)
    row = lambda v: v.reshape(1, -1)
    active = row(active)
    x_old = jnp.transpose(conv_x_state, (1, 0, 2))
    bc_old = jnp.transpose(conv_bc_state, (1, 0, 2))
    dma = pltpu.SemaphoreType.DMA
    shape = jax.ShapeDtypeStruct
    z, x, bcp, bc, dt, decay, held = pl.pallas_call(
        functools.partial(project_kernel, n),
        out_shape=(
            shape((seqs, chans), BF16),
            shape((seqs, chans), BF16),
            shape((seqs, bc_own), BF16),
            shape((seqs, bc_own * n), BF16),
            shape((seqs, heads), F32),
            shape((seqs, heads), F32),
            pltpu.VMEM(ssm_state.shape, F32),
        ),
        in_specs=[HBM] * 14,
        out_specs=(VMEM,) * 7,
        scratch_shapes=[
            pltpu.VMEM((n, seqs, feats), BF16),
            pltpu.VMEM((n, seqs, feats), BF16),
            pltpu.VMEM((n, feats, chans), BF16),
            pltpu.VMEM((n, feats, chans), BF16),
            pltpu.VMEM((seqs, bc_own), BF16),
            pltpu.VMEM((n, seqs, bc_own), BF16),
            pltpu.VMEM(in_gain.shape, F32),
            pltpu.VMEM((bc_own, model), BF16),
            pltpu.VMEM((heads, model), BF16),
            pltpu.VMEM(conv_bc_weight.shape, BF16),
            pltpu.VMEM(conv_bc_bias.shape, BF16),
            pltpu.VMEM(bc_old.shape, BF16),
            pltpu.VMEM(dt_bias.shape, F32),
            pltpu.VMEM(log_rate.shape, F32),
            pltpu.VMEM(pool_slot.shape, jnp.int32),
            pltpu.VMEM(active.shape, jnp.int32),
            dma((n,)), dma((n,)), dma((n,)), dma((n,)), dma((n,)), dma((n,)), dma(()), dma((10,)), dma(()),
        ],
        compiler_params=pltpu.CompilerParams(collective_id=0, has_side_effects=True, vmem_limit_bytes=20 * 2**20),
        name="project",
    )(*map(in_hbm, (
        hidden, in_gain, z_weight, x_weight, bc_weight.T, dt_weight.T,
        conv_bc_weight, conv_bc_bias, bc_old, dt_bias, log_rate, pool_slot, active, ssm_state,
    )))
    x_next, bc_next, state_next, branch, sq = pl.pallas_call(
        functools.partial(state_kernel, n, 4 if heads % 4 == 0 else heads),
        out_shape=(
            shape(x_old.shape, BF16),
            shape(bc_old.shape, BF16),
            shape(ssm_state.shape, F32),
            shape((n, seqs, feats), BF16),
            shape((seqs, 128), F32),
        ),
        in_specs=[SMEM] + [VMEM] * 15 + [HBM],
        out_specs=(VMEM, VMEM, HBM, VMEM, VMEM),
        scratch_shapes=[
            pltpu.VMEM(ssm_state.shape, F32),
            pltpu.VMEM(out_weight.shape, BF16),
            pltpu.VMEM((chans, 2 * seqs), BF16),
            pltpu.VMEM((seqs, chans), F32),
            pltpu.VMEM((seqs, ns), F32),
            dma((seqs,)), dma(()),
        ],
        compiler_params=pltpu.CompilerParams(vmem_limit_bytes=20 * 2**20),
        name="state",
    )(
        decay, decay, dt, z, x, bcp, bc, conv_x_weight, conv_x_bias, x_old, bc_old,
        row(skip_gain), norm_gain, pool_slot, active, held, in_hbm(out_weight),
    )
    layer_out = pl.pallas_call(
        functools.partial(reduce_kernel, n, chans * n),
        out_shape=shape((seqs, feats), BF16),
        in_specs=[VMEM] * 4,
        out_specs=VMEM,
        scratch_shapes=[
            pltpu.VMEM((n, seqs, feats), BF16),
            pltpu.VMEM((n, seqs, 128), F32),
            dma((n,)), dma((n,)), dma((n,)), dma((n,)),
        ],
        compiler_params=pltpu.CompilerParams(collective_id=1, has_side_effects=True, vmem_limit_bytes=2 * 2**20),
        name="reduce",
    )(branch, sq, hidden, active)
    return (
        layer_out,
        jnp.transpose(x_next, (1, 0, 2)),
        jnp.transpose(bc_next, (1, 0, 2)),
        state_next,
    )


def solution(mesh):
    rows = ("groups", "dp")
    placed = (
        P(rows, "tp"), P(), P(None, "tp"), P(None, "tp"), P(None, "tp"), P(None, "tp"),
        P(None, "tp"), P("tp"), P(None, "tp"), P("tp"),
        P(rows, None, "tp"), P(rows, None, "tp"),
        P("tp"), P("tp"), P("tp"), P(rows, "tp", None, None), P("tp"), P("tp", None),
        P(rows, None), P(rows),
    )
    return jax.shard_map(
        functools.partial(shards, mesh.shape["tp"]),
        mesh=mesh,
        in_specs=placed,
        out_specs=(
            P(rows, "tp"), P(rows, None, "tp"), P(rows, None, "tp"), P(rows, "tp", None, None),
        ),
        check_vma=False,
    )
```

```python
import functools

import jax
import jax.numpy as jnp
from jax import lax
from jax.experimental import pallas as pl
from jax.experimental.pallas import tpu as pltpu
from jax.sharding import PartitionSpec as P

F32 = jnp.float32
BF16 = jnp.bfloat16
VMEM = pl.BlockSpec(memory_space=pltpu.VMEM)
SMEM = pl.BlockSpec(memory_space=pltpu.SMEM)
ANY = pl.BlockSpec(memory_space=pl.ANY)
HBM = pl.BlockSpec(memory_space=pltpu.HBM)
NT = (((1,), (1,)), ((), ()))
TN = (((0,), (0,)), ((), ()))
STEPS = 4
ROWS = 256
READY = 4


def silu(v):
    return v / (1.0 + jnp.exp(-v))


def softplus(v):
    return jnp.maximum(v, 0.0) + jnp.log1p(jnp.exp(-jnp.abs(v)))


def slot_matrix(slot_row):
    rows = slot_row.shape[1]
    return slot_row == lax.broadcasted_iota(jnp.int32, (rows, rows), 0)


def greet(n):
    me = lax.axis_index("tp")
    barrier = pltpu.get_barrier_semaphore()
    for off in range(1, n):
        pl.semaphore_signal(
            barrier,
            inc=1,
            device_id={"tp": lax.rem(me + off, n)},
            device_id_type=pl.DeviceIdType.MESH,
        )
    pl.semaphore_wait(barrier, n - 1)


def push(src, dst, send, recv, off, n):
    copy = pltpu.make_async_remote_copy(
        src_ref=src,
        dst_ref=dst,
        send_sem=send.at[off],
        recv_sem=recv.at[off],
        device_id={"tp": lax.rem(lax.axis_index("tp") + off, n)},
        device_id_type=pl.DeviceIdType.MESH,
    )
    copy.start()
    return copy


def project_kernel(
    n,
    hidden, gain_h, zw, xw, bcw_h, dtw_h, bc_taps_h, bc_bias_h, bc_state_h, dt_bias_h, log_rate_h,
    slot_h, active_h, state_h,
    z_out, x_out, bcp_out, bc_out, dt_out, decay_out, state_out,
    hid_all, feed, zbuf, xbuf, bc_send, bc_all,
    gain, bcw, dtw, bc_taps, bc_bias, bc_state, dt_bias, log_rate, slot, active,
    zsem, xsem, hs, hr, bs, br, own_sem, small_sem, state_sem,
):
    me = lax.axis_index("tp")
    seqs, feats = hidden.shape
    own = pltpu.make_async_copy(hidden, hid_all.at[me], own_sem)
    own.start()
    smalls = []
    pairs = (
        (slot_h, slot), (active_h, active), (gain_h, gain), (bcw_h, bcw), (dtw_h, dtw),
        (bc_taps_h, bc_taps), (bc_bias_h, bc_bias), (bc_state_h, bc_state),
        (dt_bias_h, dt_bias), (log_rate_h, log_rate),
    )
    for k, (src, dst) in enumerate(pairs):
        copy = pltpu.make_async_copy(src, dst, small_sem.at[k])
        copy.start()
        smalls.append(copy)
    blocks = [lax.rem(me + n - off, n) for off in range(n)]
    loads = []
    for off, block in enumerate(blocks):
        rows = pl.ds(pl.multiple_of(block * feats, feats), feats)
        xc = pltpu.make_async_copy(xw.at[rows, :], xbuf.at[off], xsem.at[off])
        zc = pltpu.make_async_copy(zw.at[rows, :], zbuf.at[off], zsem.at[off])
        xc.start()
        zc.start()
        loads.append((xc, zc))
    state_copy = pltpu.make_async_copy(state_h, state_out, state_sem)
    state_copy.start()
    greet(n)
    own.wait()
    sends = [push(hid_all.at[me], hid_all.at[me], hs, hr, off, n) for off in range(1, n)]
    for copy in smalls:
        copy.wait()
    onehot = slot_matrix(slot[...])
    perm = onehot.astype(F32).astype(BF16)
    live = jnp.sum(jnp.where(onehot, active[...], 0), axis=1, keepdims=True) > 0
    gains = gain[...].reshape(1, -1)
    gains = [gains[:, j * feats : (j + 1) * feats] for j in range(n)]
    own_gain = gains[0]
    for j in range(1, n):
        own_gain = jnp.where(me == j, gains[j], own_gain)

    def fed(block, block_gain):
        return jnp.dot(
            perm, (block.astype(F32) * block_gain).astype(BF16), preferred_element_type=F32
        ).astype(BF16)

    part = fed(hid_all[me], own_gain)
    loads[0][0].wait()
    x = jnp.dot(part, xbuf[0], preferred_element_type=F32)
    loads[0][1].wait()
    z = jnp.dot(part, zbuf[0], preferred_element_type=F32)

    for copy in sends:
        copy.wait()
    squares = jnp.zeros((seqs, 1), F32)
    for j in range(n):
        block = hid_all[j]
        feed[j] = fed(block, gains[j])
        wide = block.astype(F32)
        squares += jnp.sum(wide * wide, axis=1, keepdims=True)
    inv = lax.rsqrt(squares / (n * feats) + 1e-05)
    inv = jnp.dot(
        onehot.astype(F32), jnp.broadcast_to(inv, (seqs, 128)),
        precision=lax.Precision.HIGHEST, preferred_element_type=F32,
    )[:, :1]
    whole = jnp.concatenate([feed[j] for j in range(n)], axis=1)
    bcp = lax.dot_general(whole, bcw[...], NT, preferred_element_type=F32)
    bcp = (bcp * inv).astype(BF16)
    bcp_out[...] = bcp
    acc = bcp.astype(F32) * bc_taps[3:4, :].astype(F32)
    for t in range(3):
        acc += bc_state[t].astype(F32) * bc_taps[t : t + 1, :].astype(F32)
    bc_send[...] = silu(acc + bc_bias[...].astype(F32).reshape(1, -1)).astype(BF16)
    bc_all[me] = bc_send[...]
    dtp = lax.dot_general(whole, dtw[...], NT, preferred_element_type=F32)
    sends = [push(bc_send, bc_all.at[me], bs, br, off, n) for off in range(1, n)]
    dt = softplus((dtp * inv).astype(BF16).astype(F32) + dt_bias[...].reshape(1, -1))
    dt_out[...] = dt
    decay_out[...] = jnp.where(live, jnp.exp(-dt * jnp.exp(log_rate[...].reshape(1, -1))), 1.0)

    for off in range(1, n):
        part = feed[blocks[off]]
        loads[off][0].wait()
        x += jnp.dot(part, xbuf[off], preferred_element_type=F32)
        loads[off][1].wait()
        z += jnp.dot(part, zbuf[off], preferred_element_type=F32)
    z_out[...] = (z * inv).astype(BF16)
    x_out[...] = (x * inv).astype(BF16)
    for copy in sends:
        copy.wait()
    bc_out[...] = jnp.concatenate([bc_all[j] for j in range(n)], axis=1)
    state_copy.wait()


def state_kernel(
    n, group,
    decay, decay_v, dt, z_proj, x_proj, bcp, bc, x_taps, x_bias, x_state, bc_state, skip, norm_gain,
    slot, active, state, out_w,
    x_next, bc_next, state_next, branch, sq,
    st, ow, ut, yb, c_rows, osem, wsem,
):
    seqs, heads, hp, ns = st.shape
    chans = heads * hp
    wcopy = pltpu.make_async_copy(out_w, ow, wsem)
    wcopy.start()

    onehot = slot_matrix(slot[...])
    live = jnp.sum(jnp.where(onehot, active[...], 0), axis=1, keepdims=True) > 0
    x_new = x_proj[...]
    acc = x_new.astype(F32) * x_taps[3:4, :].astype(F32)
    for t in range(3):
        acc += x_state[t].astype(F32) * x_taps[t : t + 1, :].astype(F32)
    xc = silu(acc + x_bias[...].astype(F32).reshape(1, -1)).astype(BF16).astype(F32)
    for old, new, nxt in ((x_state, x_new, x_next), (bc_state, bcp[...], bc_next)):
        nxt[0] = jnp.where(live, old[1], old[0])
        nxt[1] = jnp.where(live, old[2], old[1])
        nxt[2] = jnp.where(live, new, old[2])

    spread = (
        lax.broadcasted_iota(jnp.int32, (heads, chans), 1) // hp
        == lax.broadcasted_iota(jnp.int32, (heads, chans), 0)
    ).astype(F32)
    dt_wide = jnp.dot(dt[...], spread, precision=lax.Precision.HIGHEST, preferred_element_type=F32)
    skip_wide = jnp.dot(
        skip[...], spread, precision=lax.Precision.HIGHEST, preferred_element_type=F32
    )
    decay_wide = jnp.dot(
        decay_v[...], spread, precision=lax.Precision.HIGHEST, preferred_element_type=F32
    )
    u = jnp.where(live, dt_wide * xc, 0.0)
    high = u.astype(BF16).astype(F32)
    ut[...] = jnp.concatenate([high, u - high], axis=0).T.astype(BF16)
    b_rows = bc[:, :ns].astype(F32)
    b_twice = jnp.concatenate([b_rows, b_rows], axis=0)
    row_id = lax.broadcasted_iota(jnp.int32, (2 * seqs, ns), 0)
    c_rows[...] = bc[:, ns:].astype(F32)
    along = jnp.sum(b_rows * c_rows[...], axis=1, keepdims=True)

    def step(b, carry):
        b_one = jnp.where((row_id == b) | (row_id == b + seqs), b_twice, 0.0).astype(BF16)
        c_one = c_rows[pl.ds(b, 1), :].astype(BF16)
        for g in range(heads // group):
            lo = g * group * hp
            width = group * hp
            outer = jnp.dot(ut[lo : lo + width, :], b_one, preferred_element_type=F32)
            heads_here = pl.ds(g * group, group)
            old = state[b, heads_here].reshape(width, ns).astype(BF16)
            yb[pl.ds(b, 1), lo : lo + width] = lax.dot_general(
                c_one, old, NT, preferred_element_type=F32
            )
            for k in range(group):
                h = g * group + k
                st[b, h] = decay[b, h] * state[b, h] + outer[k * hp : (k + 1) * hp, :]
        pltpu.make_async_copy(st.at[b], state_next.at[b], osem.at[b]).start()
        return carry

    lax.fori_loop(0, seqs, step, 0, unroll=4)

    y = decay_wide * yb[...] + u * along + skip_wide * xc
    gated = y * silu(z_proj[...].astype(F32))
    perm = onehot.astype(F32)
    sq_slot = jnp.sum(gated * gated, axis=1, keepdims=True)
    sq_row = jnp.sum(perm * sq_slot, axis=0, keepdims=True)
    eye = lax.broadcasted_iota(jnp.int32, (seqs, seqs), 0) == lax.broadcasted_iota(
        jnp.int32, (seqs, seqs), 1
    )
    sq_col = jnp.sum(jnp.where(eye, sq_row, 0.0), axis=1, keepdims=True)
    sq[...] = jnp.broadcast_to(sq_col, sq.shape)
    scaled = (gated * norm_gain[...].reshape(1, -1)).astype(BF16)
    scaled = lax.dot_general(
        perm.astype(BF16), scaled, TN, preferred_element_type=F32
    ).astype(BF16)
    wcopy.wait()
    width = branch.shape[2]
    for j in range(n):
        branch[j] = jnp.dot(
            scaled, ow[:, j * width : (j + 1) * width], preferred_element_type=F32
        ).astype(BF16)

    def drain(b, carry):
        pltpu.make_async_copy(st.at[b], state_next.at[b], osem.at[b]).wait()
        return carry

    lax.fori_loop(0, seqs, drain, 0)


def reduce_kernel(n, inner, branch, sq, hidden, active, out, parts, sqs, ps, pr, qs, qr):
    me = lax.axis_index("tp")
    greet(n)
    copies = []
    for off in range(1, n):
        peer = lax.rem(me + off, n)
        copies.append(push(branch.at[peer], parts.at[off], ps, pr, off, n))
        copies.append(push(sq, sqs.at[off], qs, qr, off, n))
    rows = hidden.shape[0]
    eye = lax.broadcasted_iota(jnp.int32, (rows, rows), 0) == lax.broadcasted_iota(
        jnp.int32, (rows, rows), 1
    )
    live = jnp.sum(jnp.where(eye, active[...], 0), axis=1, keepdims=True) > 0
    old = hidden[...]
    total = branch[me].astype(F32)
    squares = sq[:, :1]
    for copy in copies:
        copy.wait()
    for off in range(1, n):
        total += parts[off].astype(F32)
        squares += sqs[off][:, :1]
    inv = lax.rsqrt(squares / inner + 1e-05)
    out[...] = jnp.where(live, (old.astype(F32) + inv * total).astype(BF16), old)


def flip(v, k):
    bit = 1
    while bit <= k:
        if k & bit:
            v = v + (1 - 2 * lax.rem(v // bit, 2)) * bit
        bit *= 2
    return v


def swap(src, dst, send, recv, k):
    return pltpu.make_async_remote_copy(
        src_ref=src,
        dst_ref=dst,
        send_sem=send.at[k],
        recv_sem=recv.at[k - 1],
        device_id={"tp": flip(lax.axis_index("tp"), k)},
        device_id_type=pl.DeviceIdType.MESH,
    )


def front_kernel(n, steps, ready, *refs):
    dma = pltpu.SemaphoreType.DMA
    pl.run_scoped(
        functools.partial(front_body, n, steps, ready, *refs),
        dma(()), dma((15,)), dma((n,)), dma((n,)), dma((steps,)), dma((n,)), dma((n,)), dma((n,)), dma((n,)),
    )


def front_body(
    n, steps, ready,
    hidden, gain_h, zw, xw, bcw_h, dtw_h, ow_h, x_taps_h, x_bias_h, x_state_h,
    bc_taps_h, bc_bias_h, bc_state_h, dt_bias_h, log_rate_h, skip_h, norm_gain_h, slot_h, active_h, state_h,
    x_out, bcp_out, ut_out, b_out, dec_out, mine_out, parts, state_out,
    own, hid, zbuf, xbuf, bcw, dtw, owbuf, bc_send, bc_all, yt, part_send,
    gain, x_taps, x_bias, x_state, bc_taps, bc_bias, bc_state, dt_bias, log_rate, skip, norm_gain, slot, active,
    hr, br, pr,
    own_sem, small_sem, xsem, zsem, ssem, wsem, hs, bs, ps,
):
    me = lax.axis_index("tp")
    seqs, feats = hidden.shape
    chans = x_out.shape[1]
    heads = dec_out.shape[0]
    ns = state_h.shape[3]
    hp = chans // heads
    far = list(range(2, n)) + list(range(1, min(n, 2)))
    blocks = [flip(me, k) for k in range(n)]
    spans = [pl.ds(pl.multiple_of(b * feats, feats), feats) for b in blocks]

    own_copy = pltpu.make_async_copy(hidden, own, own_sem)
    own_copy.start()
    pairs = (
        (slot_h, slot), (active_h, active), (gain_h, gain),
        (bc_taps_h, bc_taps), (bc_bias_h, bc_bias), (bc_state_h, bc_state),
        (dt_bias_h, dt_bias), (log_rate_h, log_rate), (skip_h, skip),
        (x_taps_h, x_taps), (x_bias_h, x_bias), (x_state_h, x_state), (norm_gain_h, norm_gain),
        (bcw_h, bcw), (dtw_h, dtw),
    )
    smalls = [pltpu.make_async_copy(s, d, small_sem.at[i]) for i, (s, d) in enumerate(pairs)]
    for copy in smalls[:-2]:
        copy.start()
    xc = [pltpu.make_async_copy(xw.at[spans[k], :], xbuf.at[k], xsem.at[k]) for k in range(n)]
    zc = [pltpu.make_async_copy(zw.at[spans[k], :], zbuf.at[k], zsem.at[k]) for k in range(n)]
    owc = [pltpu.make_async_copy(ow_h.at[:, spans[k]], owbuf.at[k], wsem.at[k]) for k in range(n)]
    span = seqs // steps
    stc = [
        pltpu.make_async_copy(
            state_h.at[pl.ds(q * span, span)], state_out.at[pl.ds(q * span, span)], ssem.at[q]
        )
        for q in range(steps)
    ]

    def stream(copies):
        for copy in copies:
            copy.start(priority=1)

    for k in range(n):
        stream([xc[k], zc[k]])

    barrier = pltpu.get_barrier_semaphore()
    for k in range(1, n):
        pl.semaphore_signal(
            barrier, inc=1, device_id={"tp": blocks[k]}, device_id_type=pl.DeviceIdType.MESH
        )
    own_copy.wait()
    smalls[0].wait()
    for copy in smalls[-2:]:
        copy.start()
    onehot = slot_matrix(slot[...])
    perm = onehot.astype(F32).astype(BF16)
    hid[0] = jnp.dot(perm, own[...], preferred_element_type=F32).astype(BF16)
    pl.semaphore_wait(barrier, n - 1)
    hid_swaps = {k: swap(hid.at[0], hid.at[k], hs, hr, k) for k in far}
    for k in far:
        hid_swaps[k].start()

    for copy in smalls[1:-2]:
        copy.wait()
    live = jnp.sum(jnp.where(onehot, active[...], 0), axis=1, keepdims=True) > 0
    gains = gain[...].reshape(1, -1)
    gains = [gains[:, j * feats : (j + 1) * feats] for j in range(n)]

    def fed(k):
        block_gain = gains[0]
        for j in range(1, n):
            block_gain = jnp.where(blocks[k] == j, gains[j], block_gain)
        return (hid[k].astype(F32) * block_gain).astype(BF16)

    def squared(k):
        wide = hid[k].astype(F32)
        return jnp.sum(wide * wide, axis=1, keepdims=True)

    def narrow(k, part):
        return (
            lax.dot_general(part, bcw[:, spans[k]], NT, preferred_element_type=F32),
            lax.dot_general(part, dtw[:, spans[k]], NT, preferred_element_type=F32),
        )

    feed = fed(0)
    squares = squared(0)
    xc[0].wait()
    x = jnp.dot(feed, xbuf[0], preferred_element_type=F32)
    zc[0].wait()
    z = jnp.dot(feed, zbuf[0], preferred_element_type=F32)
    for copy in smalls[-2:]:
        copy.wait()
    bcp, dtp = narrow(0, feed)
    feeds = {}
    for k in [1] + far[:-1]:
        hid_swaps[k].wait_recv()
        feeds[k] = fed(k)
        squares += squared(k)
        more = narrow(k, feeds[k])
        bcp += more[0]
        dtp += more[1]
        if k == 1:
            xc[1].wait()
            x += jnp.dot(feeds[1], xbuf[1], preferred_element_type=F32)
            stream(stc[: steps // 2])
            zc[1].wait()
            z += jnp.dot(feeds[1], zbuf[1], preferred_element_type=F32)
    inv = lax.rsqrt(squares / (n * feats) + 1e-05)
    bcp = (bcp * inv).astype(BF16)
    bcp_out[...] = bcp
    acc = bcp.astype(F32) * bc_taps[3:4, :].astype(F32)
    for t in range(3):
        acc += bc_state[t].astype(F32) * bc_taps[t : t + 1, :].astype(F32)
    bc_send[...] = silu(acc + bc_bias[...].astype(F32).reshape(1, -1)).astype(BF16)
    bc_all[me] = bc_send[...]
    bc_swaps = {k: swap(bc_send, bc_all.at[me], bs, br, k) for k in far}
    for k in far:
        bc_swaps[k].start()
    stream(stc[steps // 2 :])

    for k in far[:-1]:
        xc[k].wait()
        x += jnp.dot(feeds[k], xbuf[k], preferred_element_type=F32)
        zc[k].wait()
        z += jnp.dot(feeds[k], zbuf[k], preferred_element_type=F32)
    stream([owc[k] for k in far[:2]])
    dt = softplus((dtp * inv).astype(BF16).astype(F32) + dt_bias[...].reshape(1, -1))
    decay = jnp.where(live, jnp.exp(-dt * jnp.exp(log_rate[...].reshape(1, -1))), 1.0)
    for h in range(heads):
        dec_out[h] = jnp.broadcast_to(decay[:, h : h + 1], (seqs, ns))
    spread = (
        lax.broadcasted_iota(jnp.int32, (heads, chans), 1) // hp
        == lax.broadcasted_iota(jnp.int32, (heads, chans), 0)
    ).astype(F32).astype(BF16)
    per_head = jnp.concatenate(
        [dt, decay, jnp.broadcast_to(skip[...].reshape(1, -1), (8, heads))], axis=0
    )
    high = per_head.astype(BF16)
    rest = per_head - high.astype(F32)
    mid = rest.astype(BF16)
    low = (rest - mid.astype(F32)).astype(BF16)
    wide = sum(jnp.dot(v, spread, preferred_element_type=F32) for v in (high, mid, low))
    dt_wide, decay_wide, skip_wide = wide[:seqs], wide[seqs : 2 * seqs], wide[2 * seqs : 2 * seqs + 1]

    x_new = (x * inv).astype(BF16)
    x_out[...] = x_new
    acc = x_new.astype(F32) * x_taps[3:4, :].astype(F32)
    for t in range(3):
        acc += x_state[t].astype(F32) * x_taps[t : t + 1, :].astype(F32)
    conv = silu(acc + x_bias[...].astype(F32).reshape(1, -1)).astype(BF16).astype(F32)
    u = jnp.where(live, dt_wide * conv, 0.0)
    high = u.astype(BF16).astype(F32)
    ut_out[...] = jnp.concatenate([high, u - high], axis=0).T.astype(BF16)
    gate = silu((z * inv).astype(BF16).astype(F32))

    for k in far:
        bc_swaps[k].wait_recv()
    stream([owc[k] for k in far[2:] + [0]])
    both = jnp.concatenate([bc_all[j] for j in range(n)], axis=1).astype(F32)
    b_rows = both[:, :ns]
    c_rows = both[:, ns:]
    b_out[...] = b_rows
    along = jnp.sum(b_rows * c_rows, axis=1, keepdims=True)
    row_id = lax.broadcasted_iota(jnp.int32, (seqs, ns), 0)
    tile = ROWS if chans % ROWS == 0 else chans
    old_y = []
    for q in range(steps):
        stationary = jnp.concatenate(
            [jnp.where(row_id == q * span + i, c_rows, 0.0).astype(BF16) for i in range(span)], axis=1
        )
        stationary = jnp.concatenate(
            [stationary, jnp.zeros((128 - seqs, span * ns), BF16)], axis=0
        )
        stc[q].wait()
        for lo in range(0, chans, tile):
            moving = jnp.concatenate(
                [
                    state_out[q * span + i, lo // hp : (lo + tile) // hp].reshape(tile, ns).astype(BF16)
                    for i in range(span)
                ],
                axis=1,
            )
            got = lax.dot_general(moving, stationary, NT, preferred_element_type=F32)
            if q == 0:
                yt[lo : lo + tile, :] = got
            elif q < steps - 1:
                yt[lo : lo + tile, :] += got
            else:
                old_y.append((yt[lo : lo + tile, :] + got).T[:seqs])
    old_y = jnp.concatenate(old_y, axis=1)
    y = decay_wide * old_y + u * along + skip_wide * conv
    gated = y * gate
    sq = jnp.sum(gated * gated, axis=1, keepdims=True)
    high = sq.astype(BF16).astype(F32)
    mid = (sq - high).astype(BF16).astype(F32)
    lane = lax.broadcasted_iota(jnp.int32, (seqs, 128), 1)
    rest = jnp.where(lane == 1, mid, sq - high - mid)
    coded = jnp.where(lane == 0, high, jnp.where(lane < 3, rest, 0.0))
    for k in far:
        part_send[k, :, feats:] = coded.astype(BF16)
    mine_out[:, feats:] = coded
    scaled = (gated * norm_gain[...].reshape(1, -1)).astype(BF16)
    tails = []
    for k in far:
        owc[k].wait()
        part_send[k, :, :feats] = jnp.dot(scaled, owbuf[k], preferred_element_type=F32).astype(BF16)
        tails.append(swap(part_send.at[k], parts.at[k - 1], ps, pr, k))
        tails[-1].start()
    owc[0].wait()
    mine_out[:, :feats] = jnp.dot(scaled, owbuf[0], preferred_element_type=F32)
    for p in range(ready):
        update(p, dec_out, ut_out, b_out, state_out, state_out)
    for copies in (hid_swaps, bc_swaps):
        for k in far:
            copies[k].wait_send()
    for copy in tails:
        copy.wait()


def update(p, dec, ut, b_rows, state, out):
    seqs, heads, hp, ns = state.shape
    row_id = lax.broadcasted_iota(jnp.int32, (2 * seqs, ns), 0)
    b_twice = jnp.concatenate([b_rows[...], b_rows[...]], axis=0)
    stationary = jnp.concatenate(
        [
            jnp.where((row_id == 2 * p + i) | (row_id == 2 * p + i + seqs), b_twice, 0.0).astype(BF16)
            for i in range(2)
        ],
        axis=1,
    )
    pack = 128 // hp
    for lo in range(0, heads, pack):
        outer = jnp.dot(ut[lo * hp : (lo + pack) * hp, :], stationary, preferred_element_type=F32)
        for i in range(2):
            for h in range(pack):
                out[2 * p + i, lo + h] = (
                    dec[lo + h, pl.ds(2 * p + i, 1), :] * state[2 * p + i, lo + h]
                    + outer[h * hp : (h + 1) * hp, i * ns : (i + 1) * ns]
                )


def back_kernel(
    inner, ready,
    hidden, slot, active, mine, parts, x_new, x_state, bcp, bc_state, ut, b_rows, dec, state,
    layer_h, x_next_h, bc_next_h, state_next,
    layer, x_next, bc_next, st, osem, lsem,
):
    seqs = state.shape[0]

    def write(source, p):
        both = pl.ds(2 * p, 2)
        return pltpu.make_async_copy(source.at[both], state_next.at[both], osem.at[p])

    for p in range(ready):
        write(state, p).start(priority=1)

    def step(p, carry):
        update(p, dec, ut, b_rows, state, st)
        write(st, p).start(priority=1)
        return carry

    lax.fori_loop(ready, seqs // 2, step, 0)
    onehot = slot_matrix(slot[...])
    live = jnp.sum(jnp.where(onehot, active[...], 0), axis=1, keepdims=True) > 0
    for old, new, nxt in ((x_state, x_new[...], x_next), (bc_state, bcp[...], bc_next)):
        nxt[0] = jnp.where(live, old[1], old[0])
        nxt[1] = jnp.where(live, old[2], old[1])
        nxt[2] = jnp.where(live, new, old[2])
    eye = lax.broadcasted_iota(jnp.int32, (seqs, seqs), 0) == lax.broadcasted_iota(
        jnp.int32, (seqs, seqs), 1
    )
    live = jnp.sum(jnp.where(eye, active[...], 0), axis=1, keepdims=True) > 0
    total = mine[...]
    for k in range(parts.shape[0]):
        total += parts[k].astype(F32)
    feats = hidden.shape[1]
    inv = lax.rsqrt(jnp.sum(total[:, feats:], axis=1, keepdims=True) / inner + 1e-05)
    total = total[:, :feats]
    delta = lax.dot_general(
        onehot.astype(F32), inv * total, TN,
        precision=lax.Precision.HIGHEST, preferred_element_type=F32,
    )
    old = hidden[...]
    layer[...] = jnp.where(live, (old.astype(F32) + delta).astype(BF16), old)
    outs = [
        pltpu.make_async_copy(s, d, lsem.at[i])
        for i, (s, d) in enumerate(((layer, layer_h), (x_next, x_next_h), (bc_next, bc_next_h)))
    ]
    for copy in outs:
        copy.start()

    def drain(p, carry):
        write(st, p).wait()
        return carry

    lax.fori_loop(0, seqs // 2, drain, 0)
    for copy in outs:
        copy.wait()


def shards(n, *args):
    hidden, z_weight, ssm_state = args[0], args[2], args[15]
    seqs, feats = hidden.shape
    chans = z_weight.shape[1]
    heads, hp, ns = ssm_state.shape[1:]
    aligned = feats % 128 == 0 and chans % 128 == 0 and ns == 128 and 128 % hp == 0
    if aligned and n > 1 and n & (n - 1) == 0 and seqs % 16 == 0 and seqs <= 128:
        return fast_shards(n, *args)
    return plain_shards(n, *args)


def fast_shards(
    n,
    hidden, in_gain, z_weight, x_weight, bc_weight, dt_weight,
    conv_x_weight, conv_x_bias, conv_bc_weight, conv_bc_bias, conv_x_state, conv_bc_state,
    dt_bias, log_rate, skip_gain, ssm_state, norm_gain, out_weight, pool_slot, active,
):
    seqs, feats = hidden.shape
    model, chans = z_weight.shape
    bc_own = bc_weight.shape[1]
    heads, hp, ns = ssm_state.shape[1:]
    steps = STEPS
    ready = READY
    in_hbm = lambda v: pltpu.with_memory_space_constraint(v, pltpu.HBM)
    active = active.reshape(1, -1)
    x_old = jnp.transpose(conv_x_state, (1, 0, 2))
    bc_old = jnp.transpose(conv_bc_state, (1, 0, 2))
    dma = pltpu.SemaphoreType.DMA
    shape = jax.ShapeDtypeStruct
    like = lambda v: pltpu.VMEM(v.shape, v.dtype)
    x_new, bcp, ut, b_rows, dec, mine, parts, held = pl.pallas_call(
        functools.partial(front_kernel, n, steps, ready),
        out_shape=(
            pltpu.VMEM((seqs, chans), BF16),
            pltpu.VMEM((seqs, bc_own), BF16),
            pltpu.VMEM((chans, 2 * seqs), BF16),
            pltpu.VMEM((seqs, ns), F32),
            pltpu.VMEM((heads, seqs, ns), F32),
            pltpu.VMEM((seqs, feats + 128), F32),
            pltpu.VMEM((n - 1, seqs, feats + 128), BF16),
            pltpu.VMEM(ssm_state.shape, F32),
        ),
        in_specs=[HBM] * 20,
        out_specs=(VMEM,) * 8,
        scratch_shapes=[
            like(hidden),
            pltpu.VMEM((n, seqs, feats), BF16),
            pltpu.VMEM((n, feats, chans), BF16),
            pltpu.VMEM((n, feats, chans), BF16),
            pltpu.VMEM((bc_own, model), BF16),
            pltpu.VMEM((heads, model), BF16),
            pltpu.VMEM((n, chans, feats), BF16),
            pltpu.VMEM((seqs, bc_own), BF16),
            pltpu.VMEM((n, seqs, bc_own), BF16),
            pltpu.VMEM((chans, 128), F32),
            pltpu.VMEM((n, seqs, feats + 128), BF16),
            like(in_gain), like(conv_x_weight), like(conv_x_bias), like(x_old),
            like(conv_bc_weight), like(conv_bc_bias), like(bc_old),
            like(dt_bias), like(log_rate), like(skip_gain), like(norm_gain), like(pool_slot), like(active),
            dma((n - 1,)), dma((n - 1,)), dma((n - 1,)),
        ],
        compiler_params=pltpu.CompilerParams(
            collective_id=0, has_side_effects=True, vmem_limit_bytes=28 * 2**20
        ),
        name="front",
    )(*map(in_hbm, (
        hidden, in_gain, z_weight, x_weight, bc_weight.T, dt_weight.T, out_weight,
        conv_x_weight, conv_x_bias, x_old, conv_bc_weight, conv_bc_bias, bc_old,
        dt_bias, log_rate, skip_gain, norm_gain, pool_slot, active, ssm_state,
    )))
    layer_out, x_next, bc_next, state_next = pl.pallas_call(
        functools.partial(back_kernel, chans * n, ready),
        out_shape=(
            shape(hidden.shape, BF16),
            shape(x_old.shape, BF16),
            shape(bc_old.shape, BF16),
            shape(ssm_state.shape, F32),
        ),
        in_specs=[VMEM] * 13,
        out_specs=(HBM,) * 4,
        scratch_shapes=[
            like(hidden), like(x_old), like(bc_old), like(ssm_state),
            dma((seqs // 2,)), dma((3,)),
        ],
        compiler_params=pltpu.CompilerParams(vmem_limit_bytes=16 * 2**20),
        name="back",
    )(
        hidden, pool_slot, active, mine, parts, x_new, x_old, bcp, bc_old, ut, b_rows, dec, held,
    )
    return (
        layer_out,
        jnp.transpose(x_next, (1, 0, 2)),
        jnp.transpose(bc_next, (1, 0, 2)),
        state_next,
    )


def plain_shards(
    n,
    hidden, in_gain, z_weight, x_weight, bc_weight, dt_weight,
    conv_x_weight, conv_x_bias, conv_bc_weight, conv_bc_bias, conv_x_state, conv_bc_state,
    dt_bias, log_rate, skip_gain, ssm_state, norm_gain, out_weight, pool_slot, active,
):
    seqs, feats = hidden.shape
    model, chans = z_weight.shape
    bc_own = bc_weight.shape[1]
    heads, hp, ns = ssm_state.shape[1:]
    in_hbm = lambda v: pltpu.with_memory_space_constraint(v, pltpu.HBM)
    row = lambda v: v.reshape(1, -1)
    active = row(active)
    x_old = jnp.transpose(conv_x_state, (1, 0, 2))
    bc_old = jnp.transpose(conv_bc_state, (1, 0, 2))
    dma = pltpu.SemaphoreType.DMA
    shape = jax.ShapeDtypeStruct
    z, x, bcp, bc, dt, decay, held = pl.pallas_call(
        functools.partial(project_kernel, n),
        out_shape=(
            shape((seqs, chans), BF16),
            shape((seqs, chans), BF16),
            shape((seqs, bc_own), BF16),
            shape((seqs, bc_own * n), BF16),
            shape((seqs, heads), F32),
            shape((seqs, heads), F32),
            pltpu.VMEM(ssm_state.shape, F32),
        ),
        in_specs=[HBM] * 14,
        out_specs=(VMEM,) * 7,
        scratch_shapes=[
            pltpu.VMEM((n, seqs, feats), BF16),
            pltpu.VMEM((n, seqs, feats), BF16),
            pltpu.VMEM((n, feats, chans), BF16),
            pltpu.VMEM((n, feats, chans), BF16),
            pltpu.VMEM((seqs, bc_own), BF16),
            pltpu.VMEM((n, seqs, bc_own), BF16),
            pltpu.VMEM(in_gain.shape, F32),
            pltpu.VMEM((bc_own, model), BF16),
            pltpu.VMEM((heads, model), BF16),
            pltpu.VMEM(conv_bc_weight.shape, BF16),
            pltpu.VMEM(conv_bc_bias.shape, BF16),
            pltpu.VMEM(bc_old.shape, BF16),
            pltpu.VMEM(dt_bias.shape, F32),
            pltpu.VMEM(log_rate.shape, F32),
            pltpu.VMEM(pool_slot.shape, jnp.int32),
            pltpu.VMEM(active.shape, jnp.int32),
            dma((n,)), dma((n,)), dma((n,)), dma((n,)), dma((n,)), dma((n,)), dma(()), dma((10,)), dma(()),
        ],
        compiler_params=pltpu.CompilerParams(collective_id=0, has_side_effects=True, vmem_limit_bytes=20 * 2**20),
        name="project",
    )(*map(in_hbm, (
        hidden, in_gain, z_weight, x_weight, bc_weight.T, dt_weight.T,
        conv_bc_weight, conv_bc_bias, bc_old, dt_bias, log_rate, pool_slot, active, ssm_state,
    )))
    x_next, bc_next, state_next, branch, sq = pl.pallas_call(
        functools.partial(state_kernel, n, 4 if heads % 4 == 0 else heads),
        out_shape=(
            shape(x_old.shape, BF16),
            shape(bc_old.shape, BF16),
            shape(ssm_state.shape, F32),
            shape((n, seqs, feats), BF16),
            shape((seqs, 128), F32),
        ),
        in_specs=[SMEM] + [VMEM] * 15 + [HBM],
        out_specs=(VMEM, VMEM, HBM, VMEM, VMEM),
        scratch_shapes=[
            pltpu.VMEM(ssm_state.shape, F32),
            pltpu.VMEM(out_weight.shape, BF16),
            pltpu.VMEM((chans, 2 * seqs), BF16),
            pltpu.VMEM((seqs, chans), F32),
            pltpu.VMEM((seqs, ns), F32),
            dma((seqs,)), dma(()),
        ],
        compiler_params=pltpu.CompilerParams(vmem_limit_bytes=20 * 2**20),
        name="state",
    )(
        decay, decay, dt, z, x, bcp, bc, conv_x_weight, conv_x_bias, x_old, bc_old,
        row(skip_gain), norm_gain, pool_slot, active, held, in_hbm(out_weight),
    )
    layer_out = pl.pallas_call(
        functools.partial(reduce_kernel, n, chans * n),
        out_shape=shape((seqs, feats), BF16),
        in_specs=[VMEM] * 4,
        out_specs=VMEM,
        scratch_shapes=[
            pltpu.VMEM((n, seqs, feats), BF16),
            pltpu.VMEM((n, seqs, 128), F32),
            dma((n,)), dma((n,)), dma((n,)), dma((n,)),
        ],
        compiler_params=pltpu.CompilerParams(collective_id=1, has_side_effects=True, vmem_limit_bytes=2 * 2**20),
        name="reduce",
    )(branch, sq, hidden, active)
    return (
        layer_out,
        jnp.transpose(x_next, (1, 0, 2)),
        jnp.transpose(bc_next, (1, 0, 2)),
        state_next,
    )


def solution(mesh):
    rows = ("groups", "dp")
    placed = (
        P(rows, "tp"), P(), P(None, "tp"), P(None, "tp"), P(None, "tp"), P(None, "tp"),
        P(None, "tp"), P("tp"), P(None, "tp"), P("tp"),
        P(rows, None, "tp"), P(rows, None, "tp"),
        P("tp"), P("tp"), P("tp"), P(rows, "tp", None, None), P("tp"), P("tp", None),
        P(rows, None), P(rows),
    )
    return jax.shard_map(
        functools.partial(shards, mesh.shape["tp"]),
        mesh=mesh,
        in_specs=placed,
        out_specs=(
            P(rows, "tp"), P(rows, None, "tp"), P(rows, None, "tp"), P(rows, "tp", None, None),
        ),
        check_vma=False,
    )
```

```python
import functools

import jax
import jax.numpy as jnp
from jax import lax
from jax.experimental import pallas as pl
from jax.experimental.pallas import tpu as pltpu
from jax.sharding import PartitionSpec as P

F32 = jnp.float32
BF16 = jnp.bfloat16
VMEM = pl.BlockSpec(memory_space=pltpu.VMEM)
SMEM = pl.BlockSpec(memory_space=pltpu.SMEM)
ANY = pl.BlockSpec(memory_space=pl.ANY)
HBM = pl.BlockSpec(memory_space=pltpu.HBM)
NT = (((1,), (1,)), ((), ()))
TN = (((0,), (0,)), ((), ()))
STEPS = 8
ROWS = 128
READY = 4
GROUPS = ((0, 1, 2, 3), (4, 5), (6,), (7,))


def silu(v):
    return v / (1.0 + jnp.exp(-v))


def softplus(v):
    return jnp.maximum(v, 0.0) + jnp.log1p(jnp.exp(-jnp.abs(v)))


def slot_matrix(slot_row):
    rows = slot_row.shape[1]
    return slot_row == lax.broadcasted_iota(jnp.int32, (rows, rows), 0)


def greet(n):
    me = lax.axis_index("tp")
    barrier = pltpu.get_barrier_semaphore()
    for off in range(1, n):
        pl.semaphore_signal(
            barrier,
            inc=1,
            device_id={"tp": lax.rem(me + off, n)},
            device_id_type=pl.DeviceIdType.MESH,
        )
    pl.semaphore_wait(barrier, n - 1)


def push(src, dst, send, recv, off, n):
    copy = pltpu.make_async_remote_copy(
        src_ref=src,
        dst_ref=dst,
        send_sem=send.at[off],
        recv_sem=recv.at[off],
        device_id={"tp": lax.rem(lax.axis_index("tp") + off, n)},
        device_id_type=pl.DeviceIdType.MESH,
    )
    copy.start()
    return copy


def project_kernel(
    n,
    hidden, gain_h, zw, xw, bcw_h, dtw_h, bc_taps_h, bc_bias_h, bc_state_h, dt_bias_h, log_rate_h,
    slot_h, active_h, state_h,
    z_out, x_out, bcp_out, bc_out, dt_out, decay_out, state_out,
    hid_all, feed, zbuf, xbuf, bc_send, bc_all,
    gain, bcw, dtw, bc_taps, bc_bias, bc_state, dt_bias, log_rate, slot, active,
    zsem, xsem, hs, hr, bs, br, own_sem, small_sem, state_sem,
):
    me = lax.axis_index("tp")
    seqs, feats = hidden.shape
    own = pltpu.make_async_copy(hidden, hid_all.at[me], own_sem)
    own.start()
    smalls = []
    pairs = (
        (slot_h, slot), (active_h, active), (gain_h, gain), (bcw_h, bcw), (dtw_h, dtw),
        (bc_taps_h, bc_taps), (bc_bias_h, bc_bias), (bc_state_h, bc_state),
        (dt_bias_h, dt_bias), (log_rate_h, log_rate),
    )
    for k, (src, dst) in enumerate(pairs):
        copy = pltpu.make_async_copy(src, dst, small_sem.at[k])
        copy.start()
        smalls.append(copy)
    blocks = [lax.rem(me + n - off, n) for off in range(n)]
    loads = []
    for off, block in enumerate(blocks):
        rows = pl.ds(pl.multiple_of(block * feats, feats), feats)
        xc = pltpu.make_async_copy(xw.at[rows, :], xbuf.at[off], xsem.at[off])
        zc = pltpu.make_async_copy(zw.at[rows, :], zbuf.at[off], zsem.at[off])
        xc.start()
        zc.start()
        loads.append((xc, zc))
    state_copy = pltpu.make_async_copy(state_h, state_out, state_sem)
    state_copy.start()
    greet(n)
    own.wait()
    sends = [push(hid_all.at[me], hid_all.at[me], hs, hr, off, n) for off in range(1, n)]
    for copy in smalls:
        copy.wait()
    onehot = slot_matrix(slot[...])
    perm = onehot.astype(F32).astype(BF16)
    live = jnp.sum(jnp.where(onehot, active[...], 0), axis=1, keepdims=True) > 0
    gains = gain[...].reshape(1, -1)
    gains = [gains[:, j * feats : (j + 1) * feats] for j in range(n)]
    own_gain = gains[0]
    for j in range(1, n):
        own_gain = jnp.where(me == j, gains[j], own_gain)

    def fed(block, block_gain):
        return jnp.dot(
            perm, (block.astype(F32) * block_gain).astype(BF16), preferred_element_type=F32
        ).astype(BF16)

    part = fed(hid_all[me], own_gain)
    loads[0][0].wait()
    x = jnp.dot(part, xbuf[0], preferred_element_type=F32)
    loads[0][1].wait()
    z = jnp.dot(part, zbuf[0], preferred_element_type=F32)

    for copy in sends:
        copy.wait()
    squares = jnp.zeros((seqs, 1), F32)
    for j in range(n):
        block = hid_all[j]
        feed[j] = fed(block, gains[j])
        wide = block.astype(F32)
        squares += jnp.sum(wide * wide, axis=1, keepdims=True)
    inv = lax.rsqrt(squares / (n * feats) + 1e-05)
    inv = jnp.dot(
        onehot.astype(F32), jnp.broadcast_to(inv, (seqs, 128)),
        precision=lax.Precision.HIGHEST, preferred_element_type=F32,
    )[:, :1]
    whole = jnp.concatenate([feed[j] for j in range(n)], axis=1)
    bcp = lax.dot_general(whole, bcw[...], NT, preferred_element_type=F32)
    bcp = (bcp * inv).astype(BF16)
    bcp_out[...] = bcp
    acc = bcp.astype(F32) * bc_taps[3:4, :].astype(F32)
    for t in range(3):
        acc += bc_state[t].astype(F32) * bc_taps[t : t + 1, :].astype(F32)
    bc_send[...] = silu(acc + bc_bias[...].astype(F32).reshape(1, -1)).astype(BF16)
    bc_all[me] = bc_send[...]
    dtp = lax.dot_general(whole, dtw[...], NT, preferred_element_type=F32)
    sends = [push(bc_send, bc_all.at[me], bs, br, off, n) for off in range(1, n)]
    dt = softplus((dtp * inv).astype(BF16).astype(F32) + dt_bias[...].reshape(1, -1))
    dt_out[...] = dt
    decay_out[...] = jnp.where(live, jnp.exp(-dt * jnp.exp(log_rate[...].reshape(1, -1))), 1.0)

    for off in range(1, n):
        part = feed[blocks[off]]
        loads[off][0].wait()
        x += jnp.dot(part, xbuf[off], preferred_element_type=F32)
        loads[off][1].wait()
        z += jnp.dot(part, zbuf[off], preferred_element_type=F32)
    z_out[...] = (z * inv).astype(BF16)
    x_out[...] = (x * inv).astype(BF16)
    for copy in sends:
        copy.wait()
    bc_out[...] = jnp.concatenate([bc_all[j] for j in range(n)], axis=1)
    state_copy.wait()


def state_kernel(
    n, group,
    decay, decay_v, dt, z_proj, x_proj, bcp, bc, x_taps, x_bias, x_state, bc_state, skip, norm_gain,
    slot, active, state, out_w,
    x_next, bc_next, state_next, branch, sq,
    st, ow, ut, yb, c_rows, osem, wsem,
):
    seqs, heads, hp, ns = st.shape
    chans = heads * hp
    wcopy = pltpu.make_async_copy(out_w, ow, wsem)
    wcopy.start()

    onehot = slot_matrix(slot[...])
    live = jnp.sum(jnp.where(onehot, active[...], 0), axis=1, keepdims=True) > 0
    x_new = x_proj[...]
    acc = x_new.astype(F32) * x_taps[3:4, :].astype(F32)
    for t in range(3):
        acc += x_state[t].astype(F32) * x_taps[t : t + 1, :].astype(F32)
    xc = silu(acc + x_bias[...].astype(F32).reshape(1, -1)).astype(BF16).astype(F32)
    for old, new, nxt in ((x_state, x_new, x_next), (bc_state, bcp[...], bc_next)):
        nxt[0] = jnp.where(live, old[1], old[0])
        nxt[1] = jnp.where(live, old[2], old[1])
        nxt[2] = jnp.where(live, new, old[2])

    spread = (
        lax.broadcasted_iota(jnp.int32, (heads, chans), 1) // hp
        == lax.broadcasted_iota(jnp.int32, (heads, chans), 0)
    ).astype(F32)
    dt_wide = jnp.dot(dt[...], spread, precision=lax.Precision.HIGHEST, preferred_element_type=F32)
    skip_wide = jnp.dot(
        skip[...], spread, precision=lax.Precision.HIGHEST, preferred_element_type=F32
    )
    decay_wide = jnp.dot(
        decay_v[...], spread, precision=lax.Precision.HIGHEST, preferred_element_type=F32
    )
    u = jnp.where(live, dt_wide * xc, 0.0)
    high = u.astype(BF16).astype(F32)
    ut[...] = jnp.concatenate([high, u - high], axis=0).T.astype(BF16)
    b_rows = bc[:, :ns].astype(F32)
    b_twice = jnp.concatenate([b_rows, b_rows], axis=0)
    row_id = lax.broadcasted_iota(jnp.int32, (2 * seqs, ns), 0)
    c_rows[...] = bc[:, ns:].astype(F32)
    along = jnp.sum(b_rows * c_rows[...], axis=1, keepdims=True)

    def step(b, carry):
        b_one = jnp.where((row_id == b) | (row_id == b + seqs), b_twice, 0.0).astype(BF16)
        c_one = c_rows[pl.ds(b, 1), :].astype(BF16)
        for g in range(heads // group):
            lo = g * group * hp
            width = group * hp
            outer = jnp.dot(ut[lo : lo + width, :], b_one, preferred_element_type=F32)
            heads_here = pl.ds(g * group, group)
            old = state[b, heads_here].reshape(width, ns).astype(BF16)
            yb[pl.ds(b, 1), lo : lo + width] = lax.dot_general(
                c_one, old, NT, preferred_element_type=F32
            )
            for k in range(group):
                h = g * group + k
                st[b, h] = decay[b, h] * state[b, h] + outer[k * hp : (k + 1) * hp, :]
        pltpu.make_async_copy(st.at[b], state_next.at[b], osem.at[b]).start()
        return carry

    lax.fori_loop(0, seqs, step, 0, unroll=4)

    y = decay_wide * yb[...] + u * along + skip_wide * xc
    gated = y * silu(z_proj[...].astype(F32))
    perm = onehot.astype(F32)
    sq_slot = jnp.sum(gated * gated, axis=1, keepdims=True)
    sq_row = jnp.sum(perm * sq_slot, axis=0, keepdims=True)
    eye = lax.broadcasted_iota(jnp.int32, (seqs, seqs), 0) == lax.broadcasted_iota(
        jnp.int32, (seqs, seqs), 1
    )
    sq_col = jnp.sum(jnp.where(eye, sq_row, 0.0), axis=1, keepdims=True)
    sq[...] = jnp.broadcast_to(sq_col, sq.shape)
    scaled = (gated * norm_gain[...].reshape(1, -1)).astype(BF16)
    scaled = lax.dot_general(
        perm.astype(BF16), scaled, TN, preferred_element_type=F32
    ).astype(BF16)
    wcopy.wait()
    width = branch.shape[2]
    for j in range(n):
        branch[j] = jnp.dot(
            scaled, ow[:, j * width : (j + 1) * width], preferred_element_type=F32
        ).astype(BF16)

    def drain(b, carry):
        pltpu.make_async_copy(st.at[b], state_next.at[b], osem.at[b]).wait()
        return carry

    lax.fori_loop(0, seqs, drain, 0)


def reduce_kernel(n, inner, branch, sq, hidden, active, out, parts, sqs, ps, pr, qs, qr):
    me = lax.axis_index("tp")
    greet(n)
    copies = []
    for off in range(1, n):
        peer = lax.rem(me + off, n)
        copies.append(push(branch.at[peer], parts.at[off], ps, pr, off, n))
        copies.append(push(sq, sqs.at[off], qs, qr, off, n))
    rows = hidden.shape[0]
    eye = lax.broadcasted_iota(jnp.int32, (rows, rows), 0) == lax.broadcasted_iota(
        jnp.int32, (rows, rows), 1
    )
    live = jnp.sum(jnp.where(eye, active[...], 0), axis=1, keepdims=True) > 0
    old = hidden[...]
    total = branch[me].astype(F32)
    squares = sq[:, :1]
    for copy in copies:
        copy.wait()
    for off in range(1, n):
        total += parts[off].astype(F32)
        squares += sqs[off][:, :1]
    inv = lax.rsqrt(squares / inner + 1e-05)
    out[...] = jnp.where(live, (old.astype(F32) + inv * total).astype(BF16), old)


def flip(v, k):
    bit = 1
    while bit <= k:
        if k & bit:
            v = v + (1 - 2 * lax.rem(v // bit, 2)) * bit
        bit *= 2
    return v


def swap(src, dst, send, recv, k):
    return pltpu.make_async_remote_copy(
        src_ref=src,
        dst_ref=dst,
        send_sem=send.at[k],
        recv_sem=recv.at[k - 1],
        device_id={"tp": flip(lax.axis_index("tp"), k)},
        device_id_type=pl.DeviceIdType.MESH,
    )


def front_kernel(n, steps, ready, *refs):
    dma = pltpu.SemaphoreType.DMA
    pl.run_scoped(
        functools.partial(front_body, n, steps, ready, *refs),
        dma(()), dma((15,)), dma((n,)), dma((n,)), dma((steps,)), dma((n,)), dma((n,)), dma((n,)), dma((n,)), dma((n,)),
    )


def front_body(
    n, steps, ready,
    hidden, gain_h, zw, xw, bcw_h, dtw_h, ow_h, x_taps_h, x_bias_h, x_state_h,
    bc_taps_h, bc_bias_h, bc_state_h, dt_bias_h, log_rate_h, skip_h, norm_gain_h, slot_h, active_h, state_h,
    x_out, bcp_out, ut_out, b_out, dec_out, mine_out, sq_out, parts, sqs, state_out,
    own, hid, zbuf, xbuf, bcw, dtw, owbuf, bc_send, bc_all, yt, part_send,
    gain, x_taps, x_bias, x_state, bc_taps, bc_bias, bc_state, dt_bias, log_rate, skip, norm_gain, slot, active,
    hr, br, pr, qr,
    own_sem, small_sem, xsem, zsem, ssem, wsem, hs, bs, ps, qs,
):
    me = lax.axis_index("tp")
    seqs, feats = hidden.shape
    chans = x_out.shape[1]
    heads = dec_out.shape[0]
    ns = state_h.shape[3]
    hp = chans // heads
    far = list(range(2, n)) + list(range(1, min(n, 2)))
    blocks = [flip(me, k) for k in range(n)]
    spans = [pl.ds(pl.multiple_of(b * feats, feats), feats) for b in blocks]

    own_copy = pltpu.make_async_copy(hidden, own, own_sem)
    own_copy.start()
    pairs = (
        (slot_h, slot), (active_h, active), (gain_h, gain),
        (bc_taps_h, bc_taps), (bc_bias_h, bc_bias), (bc_state_h, bc_state),
        (dt_bias_h, dt_bias), (log_rate_h, log_rate), (skip_h, skip),
        (x_taps_h, x_taps), (x_bias_h, x_bias), (x_state_h, x_state), (norm_gain_h, norm_gain),
        (bcw_h, bcw), (dtw_h, dtw),
    )
    smalls = [pltpu.make_async_copy(s, d, small_sem.at[i]) for i, (s, d) in enumerate(pairs)]
    for copy in smalls[:-2]:
        copy.start()
    xc = [pltpu.make_async_copy(xw.at[spans[k], :], xbuf.at[k], xsem.at[k]) for k in range(n)]
    zc = [pltpu.make_async_copy(zw.at[spans[k], :], zbuf.at[k], zsem.at[k]) for k in range(n)]
    owc = [pltpu.make_async_copy(ow_h.at[:, spans[k]], owbuf.at[k], wsem.at[k]) for k in range(n)]
    span = seqs // steps
    stc = [
        pltpu.make_async_copy(
            state_h.at[pl.ds(q * span, span)], state_out.at[pl.ds(q * span, span)], ssem.at[q]
        )
        for q in range(steps)
    ]

    def stream(copies):
        for copy in copies:
            copy.start(priority=1)

    for k in range(n):
        stream([xc[k], zc[k]])

    barrier = pltpu.get_barrier_semaphore()
    for k in range(1, n):
        pl.semaphore_signal(
            barrier, inc=1, device_id={"tp": blocks[k]}, device_id_type=pl.DeviceIdType.MESH
        )
    own_copy.wait()
    smalls[0].wait()
    for copy in smalls[-2:]:
        copy.start()
    onehot = slot_matrix(slot[...])
    perm = onehot.astype(F32).astype(BF16)
    hid[0] = jnp.dot(perm, own[...], preferred_element_type=F32).astype(BF16)
    pl.semaphore_wait(barrier, n - 1)
    hid_swaps = {k: swap(hid.at[0], hid.at[k], hs, hr, k) for k in far}
    for k in far:
        hid_swaps[k].start()

    for copy in smalls[1:-2]:
        copy.wait()
    live = jnp.sum(jnp.where(onehot, active[...], 0), axis=1, keepdims=True) > 0
    gains = gain[...].reshape(1, -1)
    gains = [gains[:, j * feats : (j + 1) * feats] for j in range(n)]

    def fed(k):
        block_gain = gains[0]
        for j in range(1, n):
            block_gain = jnp.where(blocks[k] == j, gains[j], block_gain)
        return (hid[k].astype(F32) * block_gain).astype(BF16)

    def squared(k):
        wide = hid[k].astype(F32)
        return jnp.sum(wide * wide, axis=1, keepdims=True)

    def narrow(k, part):
        return (
            lax.dot_general(part, bcw[:, spans[k]], NT, preferred_element_type=F32),
            lax.dot_general(part, dtw[:, spans[k]], NT, preferred_element_type=F32),
        )

    feed = fed(0)
    squares = squared(0)
    xc[0].wait()
    x = jnp.dot(feed, xbuf[0], preferred_element_type=F32)
    zc[0].wait()
    z = jnp.dot(feed, zbuf[0], preferred_element_type=F32)
    for copy in smalls[-2:]:
        copy.wait()
    bcp, dtp = narrow(0, feed)
    feeds = {}
    for k in [1] + far[:-1]:
        hid_swaps[k].wait_recv()
        feeds[k] = fed(k)
        squares += squared(k)
        more = narrow(k, feeds[k])
        bcp += more[0]
        dtp += more[1]
        if k == 1:
            xc[1].wait()
            x += jnp.dot(feeds[1], xbuf[1], preferred_element_type=F32)
            stream(stc)
            zc[1].wait()
            z += jnp.dot(feeds[1], zbuf[1], preferred_element_type=F32)
    inv = lax.rsqrt(squares / (n * feats) + 1e-05)
    bcp = (bcp * inv).astype(BF16)
    bcp_out[...] = bcp
    acc = bcp.astype(F32) * bc_taps[3:4, :].astype(F32)
    for t in range(3):
        acc += bc_state[t].astype(F32) * bc_taps[t : t + 1, :].astype(F32)
    bc_send[...] = silu(acc + bc_bias[...].astype(F32).reshape(1, -1)).astype(BF16)
    bc_all[me] = bc_send[...]
    bc_swaps = {k: swap(bc_send, bc_all.at[me], bs, br, k) for k in far}
    for k in far:
        bc_swaps[k].start()

    for k in far[:-1]:
        xc[k].wait()
        x += jnp.dot(feeds[k], xbuf[k], preferred_element_type=F32)
        zc[k].wait()
        z += jnp.dot(feeds[k], zbuf[k], preferred_element_type=F32)
    stream([owc[k] for k in far[:-1]])
    dt = softplus((dtp * inv).astype(BF16).astype(F32) + dt_bias[...].reshape(1, -1))
    decay = jnp.where(live, jnp.exp(-dt * jnp.exp(log_rate[...].reshape(1, -1))), 1.0)
    for h in range(heads):
        dec_out[h] = jnp.broadcast_to(decay[:, h : h + 1], (seqs, ns))
    spread = (
        lax.broadcasted_iota(jnp.int32, (heads, chans), 1) // hp
        == lax.broadcasted_iota(jnp.int32, (heads, chans), 0)
    ).astype(F32).astype(BF16)
    per_head = jnp.concatenate(
        [dt, decay, jnp.broadcast_to(skip[...].reshape(1, -1), (8, heads))], axis=0
    )
    high = per_head.astype(BF16)
    rest = per_head - high.astype(F32)
    mid = rest.astype(BF16)
    low = (rest - mid.astype(F32)).astype(BF16)
    wide = sum(jnp.dot(v, spread, preferred_element_type=F32) for v in (high, mid, low))
    dt_wide, decay_wide, skip_wide = wide[:seqs], wide[seqs : 2 * seqs], wide[2 * seqs : 2 * seqs + 1]

    x_new = (x * inv).astype(BF16)
    x_out[...] = x_new
    acc = x_new.astype(F32) * x_taps[3:4, :].astype(F32)
    for t in range(3):
        acc += x_state[t].astype(F32) * x_taps[t : t + 1, :].astype(F32)
    conv = silu(acc + x_bias[...].astype(F32).reshape(1, -1)).astype(BF16).astype(F32)
    u = jnp.where(live, dt_wide * conv, 0.0)
    high = u.astype(BF16).astype(F32)
    ut_out[...] = jnp.concatenate([high, u - high], axis=0).T.astype(BF16)
    gate = silu((z * inv).astype(BF16).astype(F32))

    for k in far:
        bc_swaps[k].wait_recv()
    stream([owc[far[-1]], owc[0]])
    both = jnp.concatenate([bc_all[j] for j in range(n)], axis=1).astype(F32)
    b_rows = both[:, :ns]
    c_rows = both[:, ns:]
    b_out[...] = b_rows
    along = jnp.sum(b_rows * c_rows, axis=1, keepdims=True)
    row_id = lax.broadcasted_iota(jnp.int32, (seqs, ns), 0)
    tile = ROWS if chans % ROWS == 0 else chans
    old_y = []
    for g, group in enumerate(GROUPS):
        rows = [q * span + i for q in group for i in range(span)]
        stationary = jnp.concatenate(
            [jnp.where(row_id == b, c_rows, 0.0).astype(BF16) for b in rows], axis=1
        )
        stationary = jnp.concatenate(
            [stationary, jnp.zeros((128 - seqs, len(rows) * ns), BF16)], axis=0
        )
        for q in group:
            stc[q].wait()
        for lo in range(0, chans, tile):
            moving = jnp.concatenate(
                [state_out[b, lo // hp : (lo + tile) // hp].reshape(tile, ns).astype(BF16) for b in rows],
                axis=1,
            )
            got = lax.dot_general(moving, stationary, NT, preferred_element_type=F32)
            if g == len(GROUPS) - 1:
                old_y.append((yt[lo : lo + tile, :] + got).T[:seqs])
            elif g:
                yt[lo : lo + tile, :] += got
            else:
                yt[lo : lo + tile, :] = got
    old_y = jnp.concatenate(old_y, axis=1)
    y = decay_wide * old_y + u * along + skip_wide * conv
    gated = y * gate
    scaled = (gated * norm_gain[...].reshape(1, -1)).astype(BF16)
    tails = []
    started = False
    for group in [[k] for k in far[:-1]] + [[far[-1], 0]]:
        for k in group:
            owc[k].wait()
        columns = jnp.concatenate([owbuf[k] for k in group], axis=1)
        got = jnp.dot(scaled, columns, preferred_element_type=F32)
        for i, k in enumerate(group):
            piece = got[:, i * feats : (i + 1) * feats]
            if k == 0:
                mine_out[...] = piece
            else:
                part_send[k] = piece.astype(BF16)
                tails.append(swap(part_send.at[k], parts.at[k - 1], ps, pr, k))
                tails[-1].start()
        if not started:
            started = True
            sq_out[...] = jnp.broadcast_to(jnp.sum(gated * gated, axis=1, keepdims=True), sq_out.shape)
            for k in far:
                tails.append(swap(sq_out, sqs.at[k - 1], qs, qr, k))
                tails[-1].start()
    for p in range(ready):
        update(p, dec_out, ut_out, b_out, state_out, state_out)
    for copies in (hid_swaps, bc_swaps):
        for k in far:
            copies[k].wait_send()
    for copy in tails:
        copy.wait()


def update(p, dec, ut, b_rows, state, out):
    seqs, heads, hp, ns = state.shape
    row_id = lax.broadcasted_iota(jnp.int32, (2 * seqs, ns), 0)
    b_twice = jnp.concatenate([b_rows[...], b_rows[...]], axis=0)
    stationary = jnp.concatenate(
        [
            jnp.where((row_id == 2 * p + i) | (row_id == 2 * p + i + seqs), b_twice, 0.0).astype(BF16)
            for i in range(2)
        ],
        axis=1,
    )
    pack = 128 // hp
    for lo in range(0, heads, pack):
        outer = jnp.dot(ut[lo * hp : (lo + pack) * hp, :], stationary, preferred_element_type=F32)
        for i in range(2):
            for h in range(pack):
                out[2 * p + i, lo + h] = (
                    dec[lo + h, pl.ds(2 * p + i, 1), :] * state[2 * p + i, lo + h]
                    + outer[h * hp : (h + 1) * hp, i * ns : (i + 1) * ns]
                )


def back_kernel(
    inner, ready,
    hidden, slot, active, mine, sq, parts, sqs, x_new, x_state, bcp, bc_state, ut, b_rows, dec, state,
    layer_h, x_next_h, bc_next_h, state_next,
    layer, x_next, bc_next, st, osem, lsem,
):
    seqs = state.shape[0]

    def write(source, p):
        both = pl.ds(2 * p, 2)
        return pltpu.make_async_copy(source.at[both], state_next.at[both], osem.at[p])

    for p in range(ready):
        write(state, p).start(priority=1)

    def step(p, carry):
        update(p, dec, ut, b_rows, state, st)
        write(st, p).start(priority=1)
        return carry

    lax.fori_loop(ready, seqs // 2, step, 0)
    onehot = slot_matrix(slot[...])
    live = jnp.sum(jnp.where(onehot, active[...], 0), axis=1, keepdims=True) > 0
    for old, new, nxt in ((x_state, x_new[...], x_next), (bc_state, bcp[...], bc_next)):
        nxt[0] = jnp.where(live, old[1], old[0])
        nxt[1] = jnp.where(live, old[2], old[1])
        nxt[2] = jnp.where(live, new, old[2])
    eye = lax.broadcasted_iota(jnp.int32, (seqs, seqs), 0) == lax.broadcasted_iota(
        jnp.int32, (seqs, seqs), 1
    )
    live = jnp.sum(jnp.where(eye, active[...], 0), axis=1, keepdims=True) > 0
    total = mine[...]
    squares = sq[:, :1]
    for k in range(parts.shape[0]):
        total += parts[k].astype(F32)
        squares += sqs[k][:, :1]
    inv = lax.rsqrt(squares / inner + 1e-05)
    delta = lax.dot_general(
        onehot.astype(F32), inv * total, TN,
        precision=lax.Precision.HIGHEST, preferred_element_type=F32,
    )
    old = hidden[...]
    layer[...] = jnp.where(live, (old.astype(F32) + delta).astype(BF16), old)
    outs = [
        pltpu.make_async_copy(s, d, lsem.at[i])
        for i, (s, d) in enumerate(((layer, layer_h), (x_next, x_next_h), (bc_next, bc_next_h)))
    ]
    for copy in outs:
        copy.start()

    def drain(p, carry):
        write(st, p).wait()
        return carry

    lax.fori_loop(0, seqs // 2, drain, 0)
    for copy in outs:
        copy.wait()


def shards(n, *args):
    hidden, z_weight, ssm_state = args[0], args[2], args[15]
    seqs, feats = hidden.shape
    chans = z_weight.shape[1]
    heads, hp, ns = ssm_state.shape[1:]
    aligned = feats % 128 == 0 and chans % 128 == 0 and ns == 128 and 128 % hp == 0
    if aligned and n > 1 and n & (n - 1) == 0 and seqs % 16 == 0 and seqs <= 128:
        return fast_shards(n, *args)
    return plain_shards(n, *args)


def fast_shards(
    n,
    hidden, in_gain, z_weight, x_weight, bc_weight, dt_weight,
    conv_x_weight, conv_x_bias, conv_bc_weight, conv_bc_bias, conv_x_state, conv_bc_state,
    dt_bias, log_rate, skip_gain, ssm_state, norm_gain, out_weight, pool_slot, active,
):
    seqs, feats = hidden.shape
    model, chans = z_weight.shape
    bc_own = bc_weight.shape[1]
    heads, hp, ns = ssm_state.shape[1:]
    steps = STEPS
    ready = READY
    in_hbm = lambda v: pltpu.with_memory_space_constraint(v, pltpu.HBM)
    active = active.reshape(1, -1)
    x_old = jnp.transpose(conv_x_state, (1, 0, 2))
    bc_old = jnp.transpose(conv_bc_state, (1, 0, 2))
    dma = pltpu.SemaphoreType.DMA
    shape = jax.ShapeDtypeStruct
    like = lambda v: pltpu.VMEM(v.shape, v.dtype)
    x_new, bcp, ut, b_rows, dec, mine, sq, parts, sqs, held = pl.pallas_call(
        functools.partial(front_kernel, n, steps, ready),
        out_shape=(
            pltpu.VMEM((seqs, chans), BF16),
            pltpu.VMEM((seqs, bc_own), BF16),
            pltpu.VMEM((chans, 2 * seqs), BF16),
            pltpu.VMEM((seqs, ns), F32),
            pltpu.VMEM((heads, seqs, ns), F32),
            pltpu.VMEM((seqs, feats), F32),
            pltpu.VMEM((seqs, 128), F32),
            pltpu.VMEM((n - 1, seqs, feats), BF16),
            pltpu.VMEM((n - 1, seqs, 128), F32),
            pltpu.VMEM(ssm_state.shape, F32),
        ),
        in_specs=[HBM] * 20,
        out_specs=(VMEM,) * 10,
        scratch_shapes=[
            like(hidden),
            pltpu.VMEM((n, seqs, feats), BF16),
            pltpu.VMEM((n, feats, chans), BF16),
            pltpu.VMEM((n, feats, chans), BF16),
            pltpu.VMEM((bc_own, model), BF16),
            pltpu.VMEM((heads, model), BF16),
            pltpu.VMEM((n, chans, feats), BF16),
            pltpu.VMEM((seqs, bc_own), BF16),
            pltpu.VMEM((n, seqs, bc_own), BF16),
            pltpu.VMEM((chans, 128), F32),
            pltpu.VMEM((n, seqs, feats), BF16),
            like(in_gain), like(conv_x_weight), like(conv_x_bias), like(x_old),
            like(conv_bc_weight), like(conv_bc_bias), like(bc_old),
            like(dt_bias), like(log_rate), like(skip_gain), like(norm_gain), like(pool_slot), like(active),
            dma((n - 1,)), dma((n - 1,)), dma((n - 1,)), dma((n - 1,)),
        ],
        compiler_params=pltpu.CompilerParams(
            collective_id=0, has_side_effects=True, vmem_limit_bytes=28 * 2**20
        ),
        name="front",
    )(*map(in_hbm, (
        hidden, in_gain, z_weight, x_weight, bc_weight.T, dt_weight.T, out_weight,
        conv_x_weight, conv_x_bias, x_old, conv_bc_weight, conv_bc_bias, bc_old,
        dt_bias, log_rate, skip_gain, norm_gain, pool_slot, active, ssm_state,
    )))
    layer_out, x_next, bc_next, state_next = pl.pallas_call(
        functools.partial(back_kernel, chans * n, ready),
        out_shape=(
            shape(hidden.shape, BF16),
            shape(x_old.shape, BF16),
            shape(bc_old.shape, BF16),
            shape(ssm_state.shape, F32),
        ),
        in_specs=[VMEM] * 15,
        out_specs=(HBM,) * 4,
        scratch_shapes=[
            like(hidden), like(x_old), like(bc_old), like(ssm_state),
            dma((seqs // 2,)), dma((3,)),
        ],
        compiler_params=pltpu.CompilerParams(vmem_limit_bytes=16 * 2**20),
        name="back",
    )(
        hidden, pool_slot, active, mine, sq, parts, sqs, x_new, x_old, bcp, bc_old, ut, b_rows, dec, held,
    )
    return (
        layer_out,
        jnp.transpose(x_next, (1, 0, 2)),
        jnp.transpose(bc_next, (1, 0, 2)),
        state_next,
    )


def plain_shards(
    n,
    hidden, in_gain, z_weight, x_weight, bc_weight, dt_weight,
    conv_x_weight, conv_x_bias, conv_bc_weight, conv_bc_bias, conv_x_state, conv_bc_state,
    dt_bias, log_rate, skip_gain, ssm_state, norm_gain, out_weight, pool_slot, active,
):
    seqs, feats = hidden.shape
    model, chans = z_weight.shape
    bc_own = bc_weight.shape[1]
    heads, hp, ns = ssm_state.shape[1:]
    in_hbm = lambda v: pltpu.with_memory_space_constraint(v, pltpu.HBM)
    row = lambda v: v.reshape(1, -1)
    active = row(active)
    x_old = jnp.transpose(conv_x_state, (1, 0, 2))
    bc_old = jnp.transpose(conv_bc_state, (1, 0, 2))
    dma = pltpu.SemaphoreType.DMA
    shape = jax.ShapeDtypeStruct
    z, x, bcp, bc, dt, decay, held = pl.pallas_call(
        functools.partial(project_kernel, n),
        out_shape=(
            shape((seqs, chans), BF16),
            shape((seqs, chans), BF16),
            shape((seqs, bc_own), BF16),
            shape((seqs, bc_own * n), BF16),
            shape((seqs, heads), F32),
            shape((seqs, heads), F32),
            pltpu.VMEM(ssm_state.shape, F32),
        ),
        in_specs=[HBM] * 14,
        out_specs=(VMEM,) * 7,
        scratch_shapes=[
            pltpu.VMEM((n, seqs, feats), BF16),
            pltpu.VMEM((n, seqs, feats), BF16),
            pltpu.VMEM((n, feats, chans), BF16),
            pltpu.VMEM((n, feats, chans), BF16),
            pltpu.VMEM((seqs, bc_own), BF16),
            pltpu.VMEM((n, seqs, bc_own), BF16),
            pltpu.VMEM(in_gain.shape, F32),
            pltpu.VMEM((bc_own, model), BF16),
            pltpu.VMEM((heads, model), BF16),
            pltpu.VMEM(conv_bc_weight.shape, BF16),
            pltpu.VMEM(conv_bc_bias.shape, BF16),
            pltpu.VMEM(bc_old.shape, BF16),
            pltpu.VMEM(dt_bias.shape, F32),
            pltpu.VMEM(log_rate.shape, F32),
            pltpu.VMEM(pool_slot.shape, jnp.int32),
            pltpu.VMEM(active.shape, jnp.int32),
            dma((n,)), dma((n,)), dma((n,)), dma((n,)), dma((n,)), dma((n,)), dma(()), dma((10,)), dma(()),
        ],
        compiler_params=pltpu.CompilerParams(collective_id=0, has_side_effects=True, vmem_limit_bytes=20 * 2**20),
        name="project",
    )(*map(in_hbm, (
        hidden, in_gain, z_weight, x_weight, bc_weight.T, dt_weight.T,
        conv_bc_weight, conv_bc_bias, bc_old, dt_bias, log_rate, pool_slot, active, ssm_state,
    )))
    x_next, bc_next, state_next, branch, sq = pl.pallas_call(
        functools.partial(state_kernel, n, 4 if heads % 4 == 0 else heads),
        out_shape=(
            shape(x_old.shape, BF16),
            shape(bc_old.shape, BF16),
            shape(ssm_state.shape, F32),
            shape((n, seqs, feats), BF16),
            shape((seqs, 128), F32),
        ),
        in_specs=[SMEM] + [VMEM] * 15 + [HBM],
        out_specs=(VMEM, VMEM, HBM, VMEM, VMEM),
        scratch_shapes=[
            pltpu.VMEM(ssm_state.shape, F32),
            pltpu.VMEM(out_weight.shape, BF16),
            pltpu.VMEM((chans, 2 * seqs), BF16),
            pltpu.VMEM((seqs, chans), F32),
            pltpu.VMEM((seqs, ns), F32),
            dma((seqs,)), dma(()),
        ],
        compiler_params=pltpu.CompilerParams(vmem_limit_bytes=20 * 2**20),
        name="state",
    )(
        decay, decay, dt, z, x, bcp, bc, conv_x_weight, conv_x_bias, x_old, bc_old,
        row(skip_gain), norm_gain, pool_slot, active, held, in_hbm(out_weight),
    )
    layer_out = pl.pallas_call(
        functools.partial(reduce_kernel, n, chans * n),
        out_shape=shape((seqs, feats), BF16),
        in_specs=[VMEM] * 4,
        out_specs=VMEM,
        scratch_shapes=[
            pltpu.VMEM((n, seqs, feats), BF16),
            pltpu.VMEM((n, seqs, 128), F32),
            dma((n,)), dma((n,)), dma((n,)), dma((n,)),
        ],
        compiler_params=pltpu.CompilerParams(collective_id=1, has_side_effects=True, vmem_limit_bytes=2 * 2**20),
        name="reduce",
    )(branch, sq, hidden, active)
    return (
        layer_out,
        jnp.transpose(x_next, (1, 0, 2)),
        jnp.transpose(bc_next, (1, 0, 2)),
        state_next,
    )


def solution(mesh):
    rows = ("groups", "dp")
    placed = (
        P(rows, "tp"), P(), P(None, "tp"), P(None, "tp"), P(None, "tp"), P(None, "tp"),
        P(None, "tp"), P("tp"), P(None, "tp"), P("tp"),
        P(rows, None, "tp"), P(rows, None, "tp"),
        P("tp"), P("tp"), P("tp"), P(rows, "tp", None, None), P("tp"), P("tp", None),
        P(rows, None), P(rows),
    )
    return jax.shard_map(
        functools.partial(shards, mesh.shape["tp"]),
        mesh=mesh,
        in_specs=placed,
        out_specs=(
            P(rows, "tp"), P(rows, None, "tp"), P(rows, None, "tp"), P(rows, "tp", None, None),
        ),
        check_vma=False,
    )
```

```python
import functools

import jax
import jax.numpy as jnp
from jax import lax
from jax.experimental import pallas as pl
from jax.experimental.pallas import tpu as pltpu
from jax.sharding import PartitionSpec as P

F32 = jnp.float32
BF16 = jnp.bfloat16
VMEM = pl.BlockSpec(memory_space=pltpu.VMEM)
SMEM = pl.BlockSpec(memory_space=pltpu.SMEM)
ANY = pl.BlockSpec(memory_space=pl.ANY)
HBM = pl.BlockSpec(memory_space=pltpu.HBM)
NT = (((1,), (1,)), ((), ()))
TN = (((0,), (0,)), ((), ()))
STEPS = 8
ROWS = 128
READY = 4
GROUPS = ((0, 1, 2, 3), (4, 5), (6,), (7,))


def silu(v):
    return v / (1.0 + jnp.exp(-v))


def softplus(v):
    return jnp.maximum(v, 0.0) + jnp.log1p(jnp.exp(-jnp.abs(v)))


def slot_matrix(slot_row):
    rows = slot_row.shape[1]
    return slot_row == lax.broadcasted_iota(jnp.int32, (rows, rows), 0)


def greet(n):
    me = lax.axis_index("tp")
    barrier = pltpu.get_barrier_semaphore()
    for off in range(1, n):
        pl.semaphore_signal(
            barrier,
            inc=1,
            device_id={"tp": lax.rem(me + off, n)},
            device_id_type=pl.DeviceIdType.MESH,
        )
    pl.semaphore_wait(barrier, n - 1)


def push(src, dst, send, recv, off, n):
    copy = pltpu.make_async_remote_copy(
        src_ref=src,
        dst_ref=dst,
        send_sem=send.at[off],
        recv_sem=recv.at[off],
        device_id={"tp": lax.rem(lax.axis_index("tp") + off, n)},
        device_id_type=pl.DeviceIdType.MESH,
    )
    copy.start()
    return copy


def project_kernel(
    n,
    hidden, gain_h, zw, xw, bcw_h, dtw_h, bc_taps_h, bc_bias_h, bc_state_h, dt_bias_h, log_rate_h,
    slot_h, active_h, state_h,
    z_out, x_out, bcp_out, bc_out, dt_out, decay_out, state_out,
    hid_all, feed, zbuf, xbuf, bc_send, bc_all,
    gain, bcw, dtw, bc_taps, bc_bias, bc_state, dt_bias, log_rate, slot, active,
    zsem, xsem, hs, hr, bs, br, own_sem, small_sem, state_sem,
):
    me = lax.axis_index("tp")
    seqs, feats = hidden.shape
    own = pltpu.make_async_copy(hidden, hid_all.at[me], own_sem)
    own.start()
    smalls = []
    pairs = (
        (slot_h, slot), (active_h, active), (gain_h, gain), (bcw_h, bcw), (dtw_h, dtw),
        (bc_taps_h, bc_taps), (bc_bias_h, bc_bias), (bc_state_h, bc_state),
        (dt_bias_h, dt_bias), (log_rate_h, log_rate),
    )
    for k, (src, dst) in enumerate(pairs):
        copy = pltpu.make_async_copy(src, dst, small_sem.at[k])
        copy.start()
        smalls.append(copy)
    blocks = [lax.rem(me + n - off, n) for off in range(n)]
    loads = []
    for off, block in enumerate(blocks):
        rows = pl.ds(pl.multiple_of(block * feats, feats), feats)
        xc = pltpu.make_async_copy(xw.at[rows, :], xbuf.at[off], xsem.at[off])
        zc = pltpu.make_async_copy(zw.at[rows, :], zbuf.at[off], zsem.at[off])
        xc.start()
        zc.start()
        loads.append((xc, zc))
    state_copy = pltpu.make_async_copy(state_h, state_out, state_sem)
    state_copy.start()
    greet(n)
    own.wait()
    sends = [push(hid_all.at[me], hid_all.at[me], hs, hr, off, n) for off in range(1, n)]
    for copy in smalls:
        copy.wait()
    onehot = slot_matrix(slot[...])
    perm = onehot.astype(F32).astype(BF16)
    live = jnp.sum(jnp.where(onehot, active[...], 0), axis=1, keepdims=True) > 0
    gains = gain[...].reshape(1, -1)
    gains = [gains[:, j * feats : (j + 1) * feats] for j in range(n)]
    own_gain = gains[0]
    for j in range(1, n):
        own_gain = jnp.where(me == j, gains[j], own_gain)

    def fed(block, block_gain):
        return jnp.dot(
            perm, (block.astype(F32) * block_gain).astype(BF16), preferred_element_type=F32
        ).astype(BF16)

    part = fed(hid_all[me], own_gain)
    loads[0][0].wait()
    x = jnp.dot(part, xbuf[0], preferred_element_type=F32)
    loads[0][1].wait()
    z = jnp.dot(part, zbuf[0], preferred_element_type=F32)

    for copy in sends:
        copy.wait()
    squares = jnp.zeros((seqs, 1), F32)
    for j in range(n):
        block = hid_all[j]
        feed[j] = fed(block, gains[j])
        wide = block.astype(F32)
        squares += jnp.sum(wide * wide, axis=1, keepdims=True)
    inv = lax.rsqrt(squares / (n * feats) + 1e-05)
    inv = jnp.dot(
        onehot.astype(F32), jnp.broadcast_to(inv, (seqs, 128)),
        precision=lax.Precision.HIGHEST, preferred_element_type=F32,
    )[:, :1]
    whole = jnp.concatenate([feed[j] for j in range(n)], axis=1)
    bcp = lax.dot_general(whole, bcw[...], NT, preferred_element_type=F32)
    bcp = (bcp * inv).astype(BF16)
    bcp_out[...] = bcp
    acc = bcp.astype(F32) * bc_taps[3:4, :].astype(F32)
    for t in range(3):
        acc += bc_state[t].astype(F32) * bc_taps[t : t + 1, :].astype(F32)
    bc_send[...] = silu(acc + bc_bias[...].astype(F32).reshape(1, -1)).astype(BF16)
    bc_all[me] = bc_send[...]
    dtp = lax.dot_general(whole, dtw[...], NT, preferred_element_type=F32)
    sends = [push(bc_send, bc_all.at[me], bs, br, off, n) for off in range(1, n)]
    dt = softplus((dtp * inv).astype(BF16).astype(F32) + dt_bias[...].reshape(1, -1))
    dt_out[...] = dt
    decay_out[...] = jnp.where(live, jnp.exp(-dt * jnp.exp(log_rate[...].reshape(1, -1))), 1.0)

    for off in range(1, n):
        part = feed[blocks[off]]
        loads[off][0].wait()
        x += jnp.dot(part, xbuf[off], preferred_element_type=F32)
        loads[off][1].wait()
        z += jnp.dot(part, zbuf[off], preferred_element_type=F32)
    z_out[...] = (z * inv).astype(BF16)
    x_out[...] = (x * inv).astype(BF16)
    for copy in sends:
        copy.wait()
    bc_out[...] = jnp.concatenate([bc_all[j] for j in range(n)], axis=1)
    state_copy.wait()


def state_kernel(
    n, group,
    decay, decay_v, dt, z_proj, x_proj, bcp, bc, x_taps, x_bias, x_state, bc_state, skip, norm_gain,
    slot, active, state, out_w,
    x_next, bc_next, state_next, branch, sq,
    st, ow, ut, yb, c_rows, osem, wsem,
):
    seqs, heads, hp, ns = st.shape
    chans = heads * hp
    wcopy = pltpu.make_async_copy(out_w, ow, wsem)
    wcopy.start()

    onehot = slot_matrix(slot[...])
    live = jnp.sum(jnp.where(onehot, active[...], 0), axis=1, keepdims=True) > 0
    x_new = x_proj[...]
    acc = x_new.astype(F32) * x_taps[3:4, :].astype(F32)
    for t in range(3):
        acc += x_state[t].astype(F32) * x_taps[t : t + 1, :].astype(F32)
    xc = silu(acc + x_bias[...].astype(F32).reshape(1, -1)).astype(BF16).astype(F32)
    for old, new, nxt in ((x_state, x_new, x_next), (bc_state, bcp[...], bc_next)):
        nxt[0] = jnp.where(live, old[1], old[0])
        nxt[1] = jnp.where(live, old[2], old[1])
        nxt[2] = jnp.where(live, new, old[2])

    spread = (
        lax.broadcasted_iota(jnp.int32, (heads, chans), 1) // hp
        == lax.broadcasted_iota(jnp.int32, (heads, chans), 0)
    ).astype(F32)
    dt_wide = jnp.dot(dt[...], spread, precision=lax.Precision.HIGHEST, preferred_element_type=F32)
    skip_wide = jnp.dot(
        skip[...], spread, precision=lax.Precision.HIGHEST, preferred_element_type=F32
    )
    decay_wide = jnp.dot(
        decay_v[...], spread, precision=lax.Precision.HIGHEST, preferred_element_type=F32
    )
    u = jnp.where(live, dt_wide * xc, 0.0)
    high = u.astype(BF16).astype(F32)
    ut[...] = jnp.concatenate([high, u - high], axis=0).T.astype(BF16)
    b_rows = bc[:, :ns].astype(F32)
    b_twice = jnp.concatenate([b_rows, b_rows], axis=0)
    row_id = lax.broadcasted_iota(jnp.int32, (2 * seqs, ns), 0)
    c_rows[...] = bc[:, ns:].astype(F32)
    along = jnp.sum(b_rows * c_rows[...], axis=1, keepdims=True)

    def step(b, carry):
        b_one = jnp.where((row_id == b) | (row_id == b + seqs), b_twice, 0.0).astype(BF16)
        c_one = c_rows[pl.ds(b, 1), :].astype(BF16)
        for g in range(heads // group):
            lo = g * group * hp
            width = group * hp
            outer = jnp.dot(ut[lo : lo + width, :], b_one, preferred_element_type=F32)
            heads_here = pl.ds(g * group, group)
            old = state[b, heads_here].reshape(width, ns).astype(BF16)
            yb[pl.ds(b, 1), lo : lo + width] = lax.dot_general(
                c_one, old, NT, preferred_element_type=F32
            )
            for k in range(group):
                h = g * group + k
                st[b, h] = decay[b, h] * state[b, h] + outer[k * hp : (k + 1) * hp, :]
        pltpu.make_async_copy(st.at[b], state_next.at[b], osem.at[b]).start()
        return carry

    lax.fori_loop(0, seqs, step, 0, unroll=4)

    y = decay_wide * yb[...] + u * along + skip_wide * xc
    gated = y * silu(z_proj[...].astype(F32))
    perm = onehot.astype(F32)
    sq_slot = jnp.sum(gated * gated, axis=1, keepdims=True)
    sq_row = jnp.sum(perm * sq_slot, axis=0, keepdims=True)
    eye = lax.broadcasted_iota(jnp.int32, (seqs, seqs), 0) == lax.broadcasted_iota(
        jnp.int32, (seqs, seqs), 1
    )
    sq_col = jnp.sum(jnp.where(eye, sq_row, 0.0), axis=1, keepdims=True)
    sq[...] = jnp.broadcast_to(sq_col, sq.shape)
    scaled = (gated * norm_gain[...].reshape(1, -1)).astype(BF16)
    scaled = lax.dot_general(
        perm.astype(BF16), scaled, TN, preferred_element_type=F32
    ).astype(BF16)
    wcopy.wait()
    width = branch.shape[2]
    for j in range(n):
        branch[j] = jnp.dot(
            scaled, ow[:, j * width : (j + 1) * width], preferred_element_type=F32
        ).astype(BF16)

    def drain(b, carry):
        pltpu.make_async_copy(st.at[b], state_next.at[b], osem.at[b]).wait()
        return carry

    lax.fori_loop(0, seqs, drain, 0)


def reduce_kernel(n, inner, branch, sq, hidden, active, out, parts, sqs, ps, pr, qs, qr):
    me = lax.axis_index("tp")
    greet(n)
    copies = []
    for off in range(1, n):
        peer = lax.rem(me + off, n)
        copies.append(push(branch.at[peer], parts.at[off], ps, pr, off, n))
        copies.append(push(sq, sqs.at[off], qs, qr, off, n))
    rows = hidden.shape[0]
    eye = lax.broadcasted_iota(jnp.int32, (rows, rows), 0) == lax.broadcasted_iota(
        jnp.int32, (rows, rows), 1
    )
    live = jnp.sum(jnp.where(eye, active[...], 0), axis=1, keepdims=True) > 0
    old = hidden[...]
    total = branch[me].astype(F32)
    squares = sq[:, :1]
    for copy in copies:
        copy.wait()
    for off in range(1, n):
        total += parts[off].astype(F32)
        squares += sqs[off][:, :1]
    inv = lax.rsqrt(squares / inner + 1e-05)
    out[...] = jnp.where(live, (old.astype(F32) + inv * total).astype(BF16), old)


def flip(v, k):
    bit = 1
    while bit <= k:
        if k & bit:
            v = v + (1 - 2 * lax.rem(v // bit, 2)) * bit
        bit *= 2
    return v


def swap(src, dst, send, recv, k):
    return pltpu.make_async_remote_copy(
        src_ref=src,
        dst_ref=dst,
        send_sem=send.at[k],
        recv_sem=recv.at[k - 1],
        device_id={"tp": flip(lax.axis_index("tp"), k)},
        device_id_type=pl.DeviceIdType.MESH,
    )


def front_kernel(n, steps, ready, *refs):
    dma = pltpu.SemaphoreType.DMA
    pl.run_scoped(
        functools.partial(front_body, n, steps, ready, *refs),
        dma(()), dma((15,)), dma((n,)), dma((n,)), dma((steps,)), dma((n,)), dma((n,)), dma((n,)), dma((n,)), dma((n,)),
    )


def front_body(
    n, steps, ready,
    hidden, gain_h, zw, xw, bcw_h, dtw_h, ow_h, x_taps_h, x_bias_h, x_state_h,
    bc_taps_h, bc_bias_h, bc_state_h, dt_bias_h, log_rate_h, skip_h, norm_gain_h, slot_h, active_h, state_h,
    x_out, bcp_out, ut_out, b_out, dec_out, mine_out, sq_out, parts, sqs, state_out,
    own, x_state, bc_state, slot, active,
    hid, zbuf, xbuf, bcw, dtw, owbuf, bc_send, bc_all, yt, part_send,
    gain, x_taps, x_bias, bc_taps, bc_bias, dt_bias, log_rate, skip, norm_gain,
    hr, br, pr, qr,
    own_sem, small_sem, xsem, zsem, ssem, wsem, hs, bs, ps, qs,
):
    me = lax.axis_index("tp")
    seqs, feats = hidden.shape
    chans = x_out.shape[1]
    heads = dec_out.shape[0]
    ns = state_h.shape[3]
    hp = chans // heads
    far = list(range(2, n)) + list(range(1, min(n, 2)))
    blocks = [flip(me, k) for k in range(n)]
    spans = [pl.ds(pl.multiple_of(b * feats, feats), feats) for b in blocks]

    own_copy = pltpu.make_async_copy(hidden, own, own_sem)
    own_copy.start()
    pairs = (
        (slot_h, slot), (active_h, active), (gain_h, gain),
        (bc_taps_h, bc_taps), (bc_bias_h, bc_bias), (bc_state_h, bc_state),
        (dt_bias_h, dt_bias), (log_rate_h, log_rate), (skip_h, skip),
        (x_taps_h, x_taps), (x_bias_h, x_bias), (x_state_h, x_state), (norm_gain_h, norm_gain),
        (bcw_h, bcw), (dtw_h, dtw),
    )
    smalls = [pltpu.make_async_copy(s, d, small_sem.at[i]) for i, (s, d) in enumerate(pairs)]
    for copy in smalls[:-2]:
        copy.start()
    xc = [pltpu.make_async_copy(xw.at[spans[k], :], xbuf.at[k], xsem.at[k]) for k in range(n)]
    zc = [pltpu.make_async_copy(zw.at[spans[k], :], zbuf.at[k], zsem.at[k]) for k in range(n)]
    owc = [pltpu.make_async_copy(ow_h.at[:, spans[k]], owbuf.at[k], wsem.at[k]) for k in range(n)]
    span = seqs // steps
    stc = [
        pltpu.make_async_copy(
            state_h.at[pl.ds(q * span, span)], state_out.at[pl.ds(q * span, span)], ssem.at[q]
        )
        for q in range(steps)
    ]

    def stream(copies):
        for copy in copies:
            copy.start(priority=1)

    for k in range(n):
        stream([xc[k], zc[k]])

    barrier = pltpu.get_barrier_semaphore()
    for k in range(1, n):
        pl.semaphore_signal(
            barrier, inc=1, device_id={"tp": blocks[k]}, device_id_type=pl.DeviceIdType.MESH
        )
    own_copy.wait()
    smalls[0].wait()
    for copy in smalls[-2:]:
        copy.start()
    onehot = slot_matrix(slot[...])
    perm = onehot.astype(F32).astype(BF16)
    hid[0] = jnp.dot(perm, own[...], preferred_element_type=F32).astype(BF16)
    pl.semaphore_wait(barrier, n - 1)
    hid_swaps = {k: swap(hid.at[0], hid.at[k], hs, hr, k) for k in far}
    for k in far:
        hid_swaps[k].start()

    for copy in smalls[1:-2]:
        copy.wait()
    live = jnp.sum(jnp.where(onehot, active[...], 0), axis=1, keepdims=True) > 0
    gains = gain[...].reshape(1, -1)
    gains = [gains[:, j * feats : (j + 1) * feats] for j in range(n)]

    def fed(k):
        block_gain = gains[0]
        for j in range(1, n):
            block_gain = jnp.where(blocks[k] == j, gains[j], block_gain)
        return (hid[k].astype(F32) * block_gain).astype(BF16)

    def squared(k):
        wide = hid[k].astype(F32)
        return jnp.sum(wide * wide, axis=1, keepdims=True)

    def narrow(k, part):
        return (
            lax.dot_general(part, bcw[:, spans[k]], NT, preferred_element_type=F32),
            lax.dot_general(part, dtw[:, spans[k]], NT, preferred_element_type=F32),
        )

    feed = fed(0)
    squares = squared(0)
    xc[0].wait()
    x = jnp.dot(feed, xbuf[0], preferred_element_type=F32)
    zc[0].wait()
    z = jnp.dot(feed, zbuf[0], preferred_element_type=F32)
    for copy in smalls[-2:]:
        copy.wait()
    bcp, dtp = narrow(0, feed)
    feeds = {}
    for k in [1] + far[:-1]:
        hid_swaps[k].wait_recv()
        feeds[k] = fed(k)
        squares += squared(k)
        more = narrow(k, feeds[k])
        bcp += more[0]
        dtp += more[1]
        if k == 1:
            xc[1].wait()
            x += jnp.dot(feeds[1], xbuf[1], preferred_element_type=F32)
            stream(stc)
            zc[1].wait()
            z += jnp.dot(feeds[1], zbuf[1], preferred_element_type=F32)
    inv = lax.rsqrt(squares / (n * feats) + 1e-05)
    bcp = (bcp * inv).astype(BF16)
    bcp_out[...] = bcp
    acc = bcp.astype(F32) * bc_taps[3:4, :].astype(F32)
    for t in range(3):
        acc += bc_state[t].astype(F32) * bc_taps[t : t + 1, :].astype(F32)
    bc_send[...] = silu(acc + bc_bias[...].astype(F32).reshape(1, -1)).astype(BF16)
    bc_all[me] = bc_send[...]
    bc_swaps = {k: swap(bc_send, bc_all.at[me], bs, br, k) for k in far}
    for k in far:
        bc_swaps[k].start()

    for k in far[:-1]:
        xc[k].wait()
        x += jnp.dot(feeds[k], xbuf[k], preferred_element_type=F32)
        zc[k].wait()
        z += jnp.dot(feeds[k], zbuf[k], preferred_element_type=F32)
    stream([owc[k] for k in far[:-1]])
    dt = softplus((dtp * inv).astype(BF16).astype(F32) + dt_bias[...].reshape(1, -1))
    decay = jnp.where(live, jnp.exp(-dt * jnp.exp(log_rate[...].reshape(1, -1))), 1.0)
    for h in range(heads):
        dec_out[h] = jnp.broadcast_to(decay[:, h : h + 1], (seqs, ns))
    spread = (
        lax.broadcasted_iota(jnp.int32, (heads, chans), 1) // hp
        == lax.broadcasted_iota(jnp.int32, (heads, chans), 0)
    ).astype(F32).astype(BF16)
    per_head = jnp.concatenate(
        [dt, decay, jnp.broadcast_to(skip[...].reshape(1, -1), (8, heads))], axis=0
    )
    high = per_head.astype(BF16)
    rest = per_head - high.astype(F32)
    mid = rest.astype(BF16)
    low = (rest - mid.astype(F32)).astype(BF16)
    wide = sum(jnp.dot(v, spread, preferred_element_type=F32) for v in (high, mid, low))
    dt_wide, decay_wide, skip_wide = wide[:seqs], wide[seqs : 2 * seqs], wide[2 * seqs : 2 * seqs + 1]

    x_new = (x * inv).astype(BF16)
    x_out[...] = x_new
    acc = x_new.astype(F32) * x_taps[3:4, :].astype(F32)
    for t in range(3):
        acc += x_state[t].astype(F32) * x_taps[t : t + 1, :].astype(F32)
    conv = silu(acc + x_bias[...].astype(F32).reshape(1, -1)).astype(BF16).astype(F32)
    u = jnp.where(live, dt_wide * conv, 0.0)
    high = u.astype(BF16).astype(F32)
    ut_out[...] = jnp.concatenate([high, u - high], axis=0).T.astype(BF16)
    gate = silu((z * inv).astype(BF16).astype(F32))

    for k in far:
        bc_swaps[k].wait_recv()
    stream([owc[far[-1]], owc[0]])
    both = jnp.concatenate([bc_all[j] for j in range(n)], axis=1).astype(F32)
    b_rows = both[:, :ns]
    c_rows = both[:, ns:]
    b_out[...] = b_rows
    along = jnp.sum(b_rows * c_rows, axis=1, keepdims=True)
    row_id = lax.broadcasted_iota(jnp.int32, (seqs, ns), 0)
    tile = ROWS if chans % ROWS == 0 else chans
    old_y = []
    for g, group in enumerate(GROUPS):
        rows = [q * span + i for q in group for i in range(span)]
        stationary = jnp.concatenate(
            [jnp.where(row_id == b, c_rows, 0.0).astype(BF16) for b in rows], axis=1
        )
        stationary = jnp.concatenate(
            [stationary, jnp.zeros((128 - seqs, len(rows) * ns), BF16)], axis=0
        )
        for q in group:
            stc[q].wait()
        for lo in range(0, chans, tile):
            moving = jnp.concatenate(
                [state_out[b, lo // hp : (lo + tile) // hp].reshape(tile, ns).astype(BF16) for b in rows],
                axis=1,
            )
            got = lax.dot_general(moving, stationary, NT, preferred_element_type=F32)
            if g == len(GROUPS) - 1:
                old_y.append((yt[lo : lo + tile, :] + got).T[:seqs])
            elif g:
                yt[lo : lo + tile, :] += got
            else:
                yt[lo : lo + tile, :] = got
    old_y = jnp.concatenate(old_y, axis=1)
    y = decay_wide * old_y + u * along + skip_wide * conv
    gated = y * gate
    scaled = (gated * norm_gain[...].reshape(1, -1)).astype(BF16)
    tails = []
    started = False
    for group in [[k] for k in far[:-1]] + [[far[-1], 0]]:
        for k in group:
            owc[k].wait()
        columns = jnp.concatenate([owbuf[k] for k in group], axis=1)
        got = jnp.dot(scaled, columns, preferred_element_type=F32)
        for i, k in enumerate(group):
            piece = got[:, i * feats : (i + 1) * feats]
            if k == 0:
                mine_out[...] = piece
            else:
                part_send[k] = piece.astype(BF16)
                tails.append(swap(part_send.at[k], parts.at[k - 1], ps, pr, k))
                tails[-1].start()
        if not started:
            started = True
            sq_out[...] = jnp.broadcast_to(jnp.sum(gated * gated, axis=1, keepdims=True), sq_out.shape)
            for k in far:
                tails.append(swap(sq_out, sqs.at[k - 1], qs, qr, k))
                tails[-1].start()
    for p in range(ready):
        update(p, dec_out, ut_out, b_out, state_out, state_out)
    for copies in (hid_swaps, bc_swaps):
        for k in far:
            copies[k].wait_send()
    for copy in tails:
        copy.wait()


def update(p, dec, ut, b_rows, state, out):
    seqs, heads, hp, ns = state.shape
    row_id = lax.broadcasted_iota(jnp.int32, (2 * seqs, ns), 0)
    b_twice = jnp.concatenate([b_rows[...], b_rows[...]], axis=0)
    stationary = jnp.concatenate(
        [
            jnp.where((row_id == 2 * p + i) | (row_id == 2 * p + i + seqs), b_twice, 0.0).astype(BF16)
            for i in range(2)
        ],
        axis=1,
    )
    pack = 128 // hp
    for lo in range(0, heads, pack):
        outer = jnp.dot(ut[lo * hp : (lo + pack) * hp, :], stationary, preferred_element_type=F32)
        for i in range(2):
            for h in range(pack):
                out[2 * p + i, lo + h] = (
                    dec[lo + h, pl.ds(2 * p + i, 1), :] * state[2 * p + i, lo + h]
                    + outer[h * hp : (h + 1) * hp, i * ns : (i + 1) * ns]
                )


def back_kernel(
    inner, ready,
    hidden, x_state, bc_state, slot, active, mine, sq, parts, sqs, x_new, bcp, ut, b_rows, dec, state,
    layer_h, x_next_h, bc_next_h, state_next,
    layer, x_next, bc_next, st, osem, lsem,
):
    seqs = state.shape[0]

    def write(source, p):
        both = pl.ds(2 * p, 2)
        return pltpu.make_async_copy(source.at[both], state_next.at[both], osem.at[p])

    for p in range(ready):
        write(state, p).start(priority=1)

    def step(p, carry):
        update(p, dec, ut, b_rows, state, st)
        write(st, p).start(priority=1)
        return carry

    lax.fori_loop(ready, seqs // 2, step, 0)
    onehot = slot_matrix(slot[...])
    live = jnp.sum(jnp.where(onehot, active[...], 0), axis=1, keepdims=True) > 0
    for old, new, nxt in ((x_state, x_new[...], x_next), (bc_state, bcp[...], bc_next)):
        nxt[0] = jnp.where(live, old[1], old[0])
        nxt[1] = jnp.where(live, old[2], old[1])
        nxt[2] = jnp.where(live, new, old[2])
    eye = lax.broadcasted_iota(jnp.int32, (seqs, seqs), 0) == lax.broadcasted_iota(
        jnp.int32, (seqs, seqs), 1
    )
    live = jnp.sum(jnp.where(eye, active[...], 0), axis=1, keepdims=True) > 0
    total = mine[...]
    squares = sq[:, :1]
    for k in range(parts.shape[0]):
        total += parts[k].astype(F32)
        squares += sqs[k][:, :1]
    inv = lax.rsqrt(squares / inner + 1e-05)
    delta = lax.dot_general(
        onehot.astype(F32), inv * total, TN,
        precision=lax.Precision.HIGHEST, preferred_element_type=F32,
    )
    old = hidden[...]
    layer[...] = jnp.where(live, (old.astype(F32) + delta).astype(BF16), old)
    outs = [
        pltpu.make_async_copy(s, d, lsem.at[i])
        for i, (s, d) in enumerate(((layer, layer_h), (x_next, x_next_h), (bc_next, bc_next_h)))
    ]
    for copy in outs:
        copy.start()

    def drain(p, carry):
        write(st, p).wait()
        return carry

    lax.fori_loop(0, seqs // 2, drain, 0)
    for copy in outs:
        copy.wait()


def shards(n, *args):
    hidden, z_weight, ssm_state = args[0], args[2], args[15]
    seqs, feats = hidden.shape
    chans = z_weight.shape[1]
    heads, hp, ns = ssm_state.shape[1:]
    aligned = feats % 128 == 0 and chans % 128 == 0 and ns == 128 and 128 % hp == 0
    if aligned and n > 1 and n & (n - 1) == 0 and seqs % 16 == 0 and seqs <= 128:
        return fast_shards(n, *args)
    return plain_shards(n, *args)


def fast_shards(
    n,
    hidden, in_gain, z_weight, x_weight, bc_weight, dt_weight,
    conv_x_weight, conv_x_bias, conv_bc_weight, conv_bc_bias, conv_x_state, conv_bc_state,
    dt_bias, log_rate, skip_gain, ssm_state, norm_gain, out_weight, pool_slot, active,
):
    seqs, feats = hidden.shape
    model, chans = z_weight.shape
    bc_own = bc_weight.shape[1]
    heads, hp, ns = ssm_state.shape[1:]
    steps = STEPS
    ready = READY
    in_hbm = lambda v: pltpu.with_memory_space_constraint(v, pltpu.HBM)
    active = active.reshape(1, -1)
    x_old = jnp.transpose(conv_x_state, (1, 0, 2))
    bc_old = jnp.transpose(conv_bc_state, (1, 0, 2))
    dma = pltpu.SemaphoreType.DMA
    shape = jax.ShapeDtypeStruct
    like = lambda v: pltpu.VMEM(v.shape, v.dtype)
    x_new, bcp, ut, b_rows, dec, mine, sq, parts, sqs, held, *kept = pl.pallas_call(
        functools.partial(front_kernel, n, steps, ready),
        out_shape=(
            pltpu.VMEM((seqs, chans), BF16),
            pltpu.VMEM((seqs, bc_own), BF16),
            pltpu.VMEM((chans, 2 * seqs), BF16),
            pltpu.VMEM((seqs, ns), F32),
            pltpu.VMEM((heads, seqs, ns), F32),
            pltpu.VMEM((seqs, feats), F32),
            pltpu.VMEM((seqs, 128), F32),
            pltpu.VMEM((n - 1, seqs, feats), BF16),
            pltpu.VMEM((n - 1, seqs, 128), F32),
            pltpu.VMEM(ssm_state.shape, F32),
            like(hidden), like(x_old), like(bc_old), like(pool_slot), like(active),
        ),
        in_specs=[HBM] * 20,
        out_specs=(VMEM,) * 15,
        scratch_shapes=[
            pltpu.VMEM((n, seqs, feats), BF16),
            pltpu.VMEM((n, feats, chans), BF16),
            pltpu.VMEM((n, feats, chans), BF16),
            pltpu.VMEM((bc_own, model), BF16),
            pltpu.VMEM((heads, model), BF16),
            pltpu.VMEM((n, chans, feats), BF16),
            pltpu.VMEM((seqs, bc_own), BF16),
            pltpu.VMEM((n, seqs, bc_own), BF16),
            pltpu.VMEM((chans, 128), F32),
            pltpu.VMEM((n, seqs, feats), BF16),
            like(in_gain), like(conv_x_weight), like(conv_x_bias), like(conv_bc_weight), like(conv_bc_bias),
            like(dt_bias), like(log_rate), like(skip_gain), like(norm_gain),
            dma((n - 1,)), dma((n - 1,)), dma((n - 1,)), dma((n - 1,)),
        ],
        compiler_params=pltpu.CompilerParams(
            collective_id=0, has_side_effects=True, vmem_limit_bytes=28 * 2**20
        ),
        name="front",
    )(*map(in_hbm, (
        hidden, in_gain, z_weight, x_weight, bc_weight.T, dt_weight.T, out_weight,
        conv_x_weight, conv_x_bias, x_old, conv_bc_weight, conv_bc_bias, bc_old,
        dt_bias, log_rate, skip_gain, norm_gain, pool_slot, active, ssm_state,
    )))
    layer_out, x_next, bc_next, state_next = pl.pallas_call(
        functools.partial(back_kernel, chans * n, ready),
        out_shape=(
            shape(hidden.shape, BF16),
            shape(x_old.shape, BF16),
            shape(bc_old.shape, BF16),
            shape(ssm_state.shape, F32),
        ),
        in_specs=[VMEM] * 15,
        out_specs=(HBM,) * 4,
        scratch_shapes=[
            like(hidden), like(x_old), like(bc_old), like(ssm_state),
            dma((seqs // 2,)), dma((3,)),
        ],
        compiler_params=pltpu.CompilerParams(vmem_limit_bytes=16 * 2**20),
        name="back",
    )(
        *kept, mine, sq, parts, sqs, x_new, bcp, ut, b_rows, dec, held,
    )
    return (
        layer_out,
        jnp.transpose(x_next, (1, 0, 2)),
        jnp.transpose(bc_next, (1, 0, 2)),
        state_next,
    )


def plain_shards(
    n,
    hidden, in_gain, z_weight, x_weight, bc_weight, dt_weight,
    conv_x_weight, conv_x_bias, conv_bc_weight, conv_bc_bias, conv_x_state, conv_bc_state,
    dt_bias, log_rate, skip_gain, ssm_state, norm_gain, out_weight, pool_slot, active,
):
    seqs, feats = hidden.shape
    model, chans = z_weight.shape
    bc_own = bc_weight.shape[1]
    heads, hp, ns = ssm_state.shape[1:]
    in_hbm = lambda v: pltpu.with_memory_space_constraint(v, pltpu.HBM)
    row = lambda v: v.reshape(1, -1)
    active = row(active)
    x_old = jnp.transpose(conv_x_state, (1, 0, 2))
    bc_old = jnp.transpose(conv_bc_state, (1, 0, 2))
    dma = pltpu.SemaphoreType.DMA
    shape = jax.ShapeDtypeStruct
    z, x, bcp, bc, dt, decay, held = pl.pallas_call(
        functools.partial(project_kernel, n),
        out_shape=(
            shape((seqs, chans), BF16),
            shape((seqs, chans), BF16),
            shape((seqs, bc_own), BF16),
            shape((seqs, bc_own * n), BF16),
            shape((seqs, heads), F32),
            shape((seqs, heads), F32),
            pltpu.VMEM(ssm_state.shape, F32),
        ),
        in_specs=[HBM] * 14,
        out_specs=(VMEM,) * 7,
        scratch_shapes=[
            pltpu.VMEM((n, seqs, feats), BF16),
            pltpu.VMEM((n, seqs, feats), BF16),
            pltpu.VMEM((n, feats, chans), BF16),
            pltpu.VMEM((n, feats, chans), BF16),
            pltpu.VMEM((seqs, bc_own), BF16),
            pltpu.VMEM((n, seqs, bc_own), BF16),
            pltpu.VMEM(in_gain.shape, F32),
            pltpu.VMEM((bc_own, model), BF16),
            pltpu.VMEM((heads, model), BF16),
            pltpu.VMEM(conv_bc_weight.shape, BF16),
            pltpu.VMEM(conv_bc_bias.shape, BF16),
            pltpu.VMEM(bc_old.shape, BF16),
            pltpu.VMEM(dt_bias.shape, F32),
            pltpu.VMEM(log_rate.shape, F32),
            pltpu.VMEM(pool_slot.shape, jnp.int32),
            pltpu.VMEM(active.shape, jnp.int32),
            dma((n,)), dma((n,)), dma((n,)), dma((n,)), dma((n,)), dma((n,)), dma(()), dma((10,)), dma(()),
        ],
        compiler_params=pltpu.CompilerParams(collective_id=0, has_side_effects=True, vmem_limit_bytes=20 * 2**20),
        name="project",
    )(*map(in_hbm, (
        hidden, in_gain, z_weight, x_weight, bc_weight.T, dt_weight.T,
        conv_bc_weight, conv_bc_bias, bc_old, dt_bias, log_rate, pool_slot, active, ssm_state,
    )))
    x_next, bc_next, state_next, branch, sq = pl.pallas_call(
        functools.partial(state_kernel, n, 4 if heads % 4 == 0 else heads),
        out_shape=(
            shape(x_old.shape, BF16),
            shape(bc_old.shape, BF16),
            shape(ssm_state.shape, F32),
            shape((n, seqs, feats), BF16),
            shape((seqs, 128), F32),
        ),
        in_specs=[SMEM] + [VMEM] * 15 + [HBM],
        out_specs=(VMEM, VMEM, HBM, VMEM, VMEM),
        scratch_shapes=[
            pltpu.VMEM(ssm_state.shape, F32),
            pltpu.VMEM(out_weight.shape, BF16),
            pltpu.VMEM((chans, 2 * seqs), BF16),
            pltpu.VMEM((seqs, chans), F32),
            pltpu.VMEM((seqs, ns), F32),
            dma((seqs,)), dma(()),
        ],
        compiler_params=pltpu.CompilerParams(vmem_limit_bytes=20 * 2**20),
        name="state",
    )(
        decay, decay, dt, z, x, bcp, bc, conv_x_weight, conv_x_bias, x_old, bc_old,
        row(skip_gain), norm_gain, pool_slot, active, held, in_hbm(out_weight),
    )
    layer_out = pl.pallas_call(
        functools.partial(reduce_kernel, n, chans * n),
        out_shape=shape((seqs, feats), BF16),
        in_specs=[VMEM] * 4,
        out_specs=VMEM,
        scratch_shapes=[
            pltpu.VMEM((n, seqs, feats), BF16),
            pltpu.VMEM((n, seqs, 128), F32),
            dma((n,)), dma((n,)), dma((n,)), dma((n,)),
        ],
        compiler_params=pltpu.CompilerParams(collective_id=1, has_side_effects=True, vmem_limit_bytes=2 * 2**20),
        name="reduce",
    )(branch, sq, hidden, active)
    return (
        layer_out,
        jnp.transpose(x_next, (1, 0, 2)),
        jnp.transpose(bc_next, (1, 0, 2)),
        state_next,
    )


def solution(mesh):
    rows = ("groups", "dp")
    placed = (
        P(rows, "tp"), P(), P(None, "tp"), P(None, "tp"), P(None, "tp"), P(None, "tp"),
        P(None, "tp"), P("tp"), P(None, "tp"), P("tp"),
        P(rows, None, "tp"), P(rows, None, "tp"),
        P("tp"), P("tp"), P("tp"), P(rows, "tp", None, None), P("tp"), P("tp", None),
        P(rows, None), P(rows),
    )
    return jax.shard_map(
        functools.partial(shards, mesh.shape["tp"]),
        mesh=mesh,
        in_specs=placed,
        out_specs=(
            P(rows, "tp"), P(rows, None, "tp"), P(rows, None, "tp"), P(rows, "tp", None, None),
        ),
        check_vma=False,
    )
```

```python
import functools

import jax
import jax.numpy as jnp
from jax import lax
from jax.experimental import pallas as pl
from jax.experimental.pallas import tpu as pltpu
from jax.sharding import PartitionSpec as P

F32 = jnp.float32
BF16 = jnp.bfloat16
VMEM = pl.BlockSpec(memory_space=pltpu.VMEM)
SMEM = pl.BlockSpec(memory_space=pltpu.SMEM)
ANY = pl.BlockSpec(memory_space=pl.ANY)
HBM = pl.BlockSpec(memory_space=pltpu.HBM)
NT = (((1,), (1,)), ((), ()))
TN = (((0,), (0,)), ((), ()))
STEPS = 8
ROWS = 128
READY = 3
GROUPS = ((0, 1, 2, 3), (4, 5), (6,), (7,))


def silu(v):
    return v / (1.0 + jnp.exp(-v))


def softplus(v):
    return jnp.maximum(v, 0.0) + jnp.log1p(jnp.exp(-jnp.abs(v)))


def slot_matrix(slot_row):
    rows = slot_row.shape[1]
    return slot_row == lax.broadcasted_iota(jnp.int32, (rows, rows), 0)


def greet(n):
    me = lax.axis_index("tp")
    barrier = pltpu.get_barrier_semaphore()
    for off in range(1, n):
        pl.semaphore_signal(
            barrier,
            inc=1,
            device_id={"tp": lax.rem(me + off, n)},
            device_id_type=pl.DeviceIdType.MESH,
        )
    pl.semaphore_wait(barrier, n - 1)


def push(src, dst, send, recv, off, n):
    copy = pltpu.make_async_remote_copy(
        src_ref=src,
        dst_ref=dst,
        send_sem=send.at[off],
        recv_sem=recv.at[off],
        device_id={"tp": lax.rem(lax.axis_index("tp") + off, n)},
        device_id_type=pl.DeviceIdType.MESH,
    )
    copy.start()
    return copy


def project_kernel(
    n,
    hidden, gain_h, zw, xw, bcw_h, dtw_h, bc_taps_h, bc_bias_h, bc_state_h, dt_bias_h, log_rate_h,
    slot_h, active_h, state_h,
    z_out, x_out, bcp_out, bc_out, dt_out, decay_out, state_out,
    hid_all, feed, zbuf, xbuf, bc_send, bc_all,
    gain, bcw, dtw, bc_taps, bc_bias, bc_state, dt_bias, log_rate, slot, active,
    zsem, xsem, hs, hr, bs, br, own_sem, small_sem, state_sem,
):
    me = lax.axis_index("tp")
    seqs, feats = hidden.shape
    own = pltpu.make_async_copy(hidden, hid_all.at[me], own_sem)
    own.start()
    smalls = []
    pairs = (
        (slot_h, slot), (active_h, active), (gain_h, gain), (bcw_h, bcw), (dtw_h, dtw),
        (bc_taps_h, bc_taps), (bc_bias_h, bc_bias), (bc_state_h, bc_state),
        (dt_bias_h, dt_bias), (log_rate_h, log_rate),
    )
    for k, (src, dst) in enumerate(pairs):
        copy = pltpu.make_async_copy(src, dst, small_sem.at[k])
        copy.start()
        smalls.append(copy)
    blocks = [lax.rem(me + n - off, n) for off in range(n)]
    loads = []
    for off, block in enumerate(blocks):
        rows = pl.ds(pl.multiple_of(block * feats, feats), feats)
        xc = pltpu.make_async_copy(xw.at[rows, :], xbuf.at[off], xsem.at[off])
        zc = pltpu.make_async_copy(zw.at[rows, :], zbuf.at[off], zsem.at[off])
        xc.start()
        zc.start()
        loads.append((xc, zc))
    state_copy = pltpu.make_async_copy(state_h, state_out, state_sem)
    state_copy.start()
    greet(n)
    own.wait()
    sends = [push(hid_all.at[me], hid_all.at[me], hs, hr, off, n) for off in range(1, n)]
    for copy in smalls:
        copy.wait()
    onehot = slot_matrix(slot[...])
    perm = onehot.astype(F32).astype(BF16)
    live = jnp.sum(jnp.where(onehot, active[...], 0), axis=1, keepdims=True) > 0
    gains = gain[...].reshape(1, -1)
    gains = [gains[:, j * feats : (j + 1) * feats] for j in range(n)]
    own_gain = gains[0]
    for j in range(1, n):
        own_gain = jnp.where(me == j, gains[j], own_gain)

    def fed(block, block_gain):
        return jnp.dot(
            perm, (block.astype(F32) * block_gain).astype(BF16), preferred_element_type=F32
        ).astype(BF16)

    part = fed(hid_all[me], own_gain)
    loads[0][0].wait()
    x = jnp.dot(part, xbuf[0], preferred_element_type=F32)
    loads[0][1].wait()
    z = jnp.dot(part, zbuf[0], preferred_element_type=F32)

    for copy in sends:
        copy.wait()
    squares = jnp.zeros((seqs, 1), F32)
    for j in range(n):
        block = hid_all[j]
        feed[j] = fed(block, gains[j])
        wide = block.astype(F32)
        squares += jnp.sum(wide * wide, axis=1, keepdims=True)
    inv = lax.rsqrt(squares / (n * feats) + 1e-05)
    inv = jnp.dot(
        onehot.astype(F32), jnp.broadcast_to(inv, (seqs, 128)),
        precision=lax.Precision.HIGHEST, preferred_element_type=F32,
    )[:, :1]
    whole = jnp.concatenate([feed[j] for j in range(n)], axis=1)
    bcp = lax.dot_general(whole, bcw[...], NT, preferred_element_type=F32)
    bcp = (bcp * inv).astype(BF16)
    bcp_out[...] = bcp
    acc = bcp.astype(F32) * bc_taps[3:4, :].astype(F32)
    for t in range(3):
        acc += bc_state[t].astype(F32) * bc_taps[t : t + 1, :].astype(F32)
    bc_send[...] = silu(acc + bc_bias[...].astype(F32).reshape(1, -1)).astype(BF16)
    bc_all[me] = bc_send[...]
    dtp = lax.dot_general(whole, dtw[...], NT, preferred_element_type=F32)
    sends = [push(bc_send, bc_all.at[me], bs, br, off, n) for off in range(1, n)]
    dt = softplus((dtp * inv).astype(BF16).astype(F32) + dt_bias[...].reshape(1, -1))
    dt_out[...] = dt
    decay_out[...] = jnp.where(live, jnp.exp(-dt * jnp.exp(log_rate[...].reshape(1, -1))), 1.0)

    for off in range(1, n):
        part = feed[blocks[off]]
        loads[off][0].wait()
        x += jnp.dot(part, xbuf[off], preferred_element_type=F32)
        loads[off][1].wait()
        z += jnp.dot(part, zbuf[off], preferred_element_type=F32)
    z_out[...] = (z * inv).astype(BF16)
    x_out[...] = (x * inv).astype(BF16)
    for copy in sends:
        copy.wait()
    bc_out[...] = jnp.concatenate([bc_all[j] for j in range(n)], axis=1)
    state_copy.wait()


def state_kernel(
    n, group,
    decay, decay_v, dt, z_proj, x_proj, bcp, bc, x_taps, x_bias, x_state, bc_state, skip, norm_gain,
    slot, active, state, out_w,
    x_next, bc_next, state_next, branch, sq,
    st, ow, ut, yb, c_rows, osem, wsem,
):
    seqs, heads, hp, ns = st.shape
    chans = heads * hp
    wcopy = pltpu.make_async_copy(out_w, ow, wsem)
    wcopy.start()

    onehot = slot_matrix(slot[...])
    live = jnp.sum(jnp.where(onehot, active[...], 0), axis=1, keepdims=True) > 0
    x_new = x_proj[...]
    acc = x_new.astype(F32) * x_taps[3:4, :].astype(F32)
    for t in range(3):
        acc += x_state[t].astype(F32) * x_taps[t : t + 1, :].astype(F32)
    xc = silu(acc + x_bias[...].astype(F32).reshape(1, -1)).astype(BF16).astype(F32)
    for old, new, nxt in ((x_state, x_new, x_next), (bc_state, bcp[...], bc_next)):
        nxt[0] = jnp.where(live, old[1], old[0])
        nxt[1] = jnp.where(live, old[2], old[1])
        nxt[2] = jnp.where(live, new, old[2])

    spread = (
        lax.broadcasted_iota(jnp.int32, (heads, chans), 1) // hp
        == lax.broadcasted_iota(jnp.int32, (heads, chans), 0)
    ).astype(F32)
    dt_wide = jnp.dot(dt[...], spread, precision=lax.Precision.HIGHEST, preferred_element_type=F32)
    skip_wide = jnp.dot(
        skip[...], spread, precision=lax.Precision.HIGHEST, preferred_element_type=F32
    )
    decay_wide = jnp.dot(
        decay_v[...], spread, precision=lax.Precision.HIGHEST, preferred_element_type=F32
    )
    u = jnp.where(live, dt_wide * xc, 0.0)
    high = u.astype(BF16).astype(F32)
    ut[...] = jnp.concatenate([high, u - high], axis=0).T.astype(BF16)
    b_rows = bc[:, :ns].astype(F32)
    b_twice = jnp.concatenate([b_rows, b_rows], axis=0)
    row_id = lax.broadcasted_iota(jnp.int32, (2 * seqs, ns), 0)
    c_rows[...] = bc[:, ns:].astype(F32)
    along = jnp.sum(b_rows * c_rows[...], axis=1, keepdims=True)

    def step(b, carry):
        b_one = jnp.where((row_id == b) | (row_id == b + seqs), b_twice, 0.0).astype(BF16)
        c_one = c_rows[pl.ds(b, 1), :].astype(BF16)
        for g in range(heads // group):
            lo = g * group * hp
            width = group * hp
            outer = jnp.dot(ut[lo : lo + width, :], b_one, preferred_element_type=F32)
            heads_here = pl.ds(g * group, group)
            old = state[b, heads_here].reshape(width, ns).astype(BF16)
            yb[pl.ds(b, 1), lo : lo + width] = lax.dot_general(
                c_one, old, NT, preferred_element_type=F32
            )
            for k in range(group):
                h = g * group + k
                st[b, h] = decay[b, h] * state[b, h] + outer[k * hp : (k + 1) * hp, :]
        pltpu.make_async_copy(st.at[b], state_next.at[b], osem.at[b]).start()
        return carry

    lax.fori_loop(0, seqs, step, 0, unroll=4)

    y = decay_wide * yb[...] + u * along + skip_wide * xc
    gated = y * silu(z_proj[...].astype(F32))
    perm = onehot.astype(F32)
    sq_slot = jnp.sum(gated * gated, axis=1, keepdims=True)
    sq_row = jnp.sum(perm * sq_slot, axis=0, keepdims=True)
    eye = lax.broadcasted_iota(jnp.int32, (seqs, seqs), 0) == lax.broadcasted_iota(
        jnp.int32, (seqs, seqs), 1
    )
    sq_col = jnp.sum(jnp.where(eye, sq_row, 0.0), axis=1, keepdims=True)
    sq[...] = jnp.broadcast_to(sq_col, sq.shape)
    scaled = (gated * norm_gain[...].reshape(1, -1)).astype(BF16)
    scaled = lax.dot_general(
        perm.astype(BF16), scaled, TN, preferred_element_type=F32
    ).astype(BF16)
    wcopy.wait()
    width = branch.shape[2]
    for j in range(n):
        branch[j] = jnp.dot(
            scaled, ow[:, j * width : (j + 1) * width], preferred_element_type=F32
        ).astype(BF16)

    def drain(b, carry):
        pltpu.make_async_copy(st.at[b], state_next.at[b], osem.at[b]).wait()
        return carry

    lax.fori_loop(0, seqs, drain, 0)


def reduce_kernel(n, inner, branch, sq, hidden, active, out, parts, sqs, ps, pr, qs, qr):
    me = lax.axis_index("tp")
    greet(n)
    copies = []
    for off in range(1, n):
        peer = lax.rem(me + off, n)
        copies.append(push(branch.at[peer], parts.at[off], ps, pr, off, n))
        copies.append(push(sq, sqs.at[off], qs, qr, off, n))
    rows = hidden.shape[0]
    eye = lax.broadcasted_iota(jnp.int32, (rows, rows), 0) == lax.broadcasted_iota(
        jnp.int32, (rows, rows), 1
    )
    live = jnp.sum(jnp.where(eye, active[...], 0), axis=1, keepdims=True) > 0
    old = hidden[...]
    total = branch[me].astype(F32)
    squares = sq[:, :1]
    for copy in copies:
        copy.wait()
    for off in range(1, n):
        total += parts[off].astype(F32)
        squares += sqs[off][:, :1]
    inv = lax.rsqrt(squares / inner + 1e-05)
    out[...] = jnp.where(live, (old.astype(F32) + inv * total).astype(BF16), old)


def flip(v, k):
    bit = 1
    while bit <= k:
        if k & bit:
            v = v + (1 - 2 * lax.rem(v // bit, 2)) * bit
        bit *= 2
    return v


def swap(src, dst, send, recv, k):
    return pltpu.make_async_remote_copy(
        src_ref=src,
        dst_ref=dst,
        send_sem=send.at[k],
        recv_sem=recv.at[k - 1],
        device_id={"tp": flip(lax.axis_index("tp"), k)},
        device_id_type=pl.DeviceIdType.MESH,
    )


def front_kernel(n, steps, ready, *refs):
    dma = pltpu.SemaphoreType.DMA
    pl.run_scoped(
        functools.partial(front_body, n, steps, ready, *refs),
        dma(()), dma((15,)), dma((n,)), dma((n,)), dma((steps,)), dma((n,)), dma((n,)), dma((n,)), dma((n,)), dma((n,)),
    )


def front_body(
    n, steps, ready,
    hidden, gain_h, zw, xw, bcw_h, dtw_h, ow_h, x_taps_h, x_bias_h, x_state_h,
    bc_taps_h, bc_bias_h, bc_state_h, dt_bias_h, log_rate_h, skip_h, norm_gain_h, slot_h, active_h, state_h,
    x_out, bcp_out, ut_out, b_out, dec_out, mine_out, sq_out, parts, sqs, state_out,
    own, x_state, bc_state, slot, active,
    hid, zbuf, xbuf, bcw, dtw, owbuf, bc_send, bc_all, yt, part_send,
    gain, x_taps, x_bias, bc_taps, bc_bias, dt_bias, log_rate, skip, norm_gain,
    hr, br, pr, qr,
    own_sem, small_sem, xsem, zsem, ssem, wsem, hs, bs, ps, qs,
):
    me = lax.axis_index("tp")
    seqs, feats = hidden.shape
    chans = x_out.shape[1]
    heads = dec_out.shape[0]
    ns = state_h.shape[3]
    hp = chans // heads
    far = list(range(2, n)) + list(range(1, min(n, 2)))
    blocks = [flip(me, k) for k in range(n)]
    spans = [pl.ds(pl.multiple_of(b * feats, feats), feats) for b in blocks]

    own_copy = pltpu.make_async_copy(hidden, own, own_sem)
    own_copy.start()
    pairs = (
        (slot_h, slot), (active_h, active), (gain_h, gain),
        (bc_taps_h, bc_taps), (bc_bias_h, bc_bias), (bc_state_h, bc_state),
        (dt_bias_h, dt_bias), (log_rate_h, log_rate), (skip_h, skip),
        (x_taps_h, x_taps), (x_bias_h, x_bias), (x_state_h, x_state), (norm_gain_h, norm_gain),
        (bcw_h, bcw), (dtw_h, dtw),
    )
    smalls = [pltpu.make_async_copy(s, d, small_sem.at[i]) for i, (s, d) in enumerate(pairs)]
    for copy in smalls[:-2]:
        copy.start()
    xc = [pltpu.make_async_copy(xw.at[spans[k], :], xbuf.at[k], xsem.at[k]) for k in range(n)]
    zc = [pltpu.make_async_copy(zw.at[spans[k], :], zbuf.at[k], zsem.at[k]) for k in range(n)]
    owc = [pltpu.make_async_copy(ow_h.at[:, spans[k]], owbuf.at[k], wsem.at[k]) for k in range(n)]
    span = seqs // steps
    stc = [
        pltpu.make_async_copy(
            state_h.at[pl.ds(q * span, span)], state_out.at[pl.ds(q * span, span)], ssem.at[q]
        )
        for q in range(steps)
    ]

    def stream(copies):
        for copy in copies:
            copy.start(priority=1)

    for k in range(n):
        stream([xc[k], zc[k]])
    stream(stc[:2])

    barrier = pltpu.get_barrier_semaphore()
    for k in range(1, n):
        pl.semaphore_signal(
            barrier, inc=1, device_id={"tp": blocks[k]}, device_id_type=pl.DeviceIdType.MESH
        )
    own_copy.wait()
    smalls[0].wait()
    for copy in smalls[-2:]:
        copy.start()
    onehot = slot_matrix(slot[...])
    perm = onehot.astype(F32).astype(BF16)
    hid[0] = jnp.dot(perm, own[...], preferred_element_type=F32).astype(BF16)
    pl.semaphore_wait(barrier, n - 1)
    hid_swaps = {k: swap(hid.at[0], hid.at[k], hs, hr, k) for k in far}
    for k in far:
        hid_swaps[k].start()

    for copy in smalls[1:-2]:
        copy.wait()
    live = jnp.sum(jnp.where(onehot, active[...], 0), axis=1, keepdims=True) > 0
    gains = gain[...].reshape(1, -1)
    gains = [gains[:, j * feats : (j + 1) * feats] for j in range(n)]

    def fed(k):
        block_gain = gains[0]
        for j in range(1, n):
            block_gain = jnp.where(blocks[k] == j, gains[j], block_gain)
        return (hid[k].astype(F32) * block_gain).astype(BF16)

    def squared(k):
        wide = hid[k].astype(F32)
        return jnp.sum(wide * wide, axis=1, keepdims=True)

    def narrow(k, part):
        return (
            lax.dot_general(part, bcw[:, spans[k]], NT, preferred_element_type=F32),
            lax.dot_general(part, dtw[:, spans[k]], NT, preferred_element_type=F32),
        )

    feed = fed(0)
    squares = squared(0)
    xc[0].wait()
    x = jnp.dot(feed, xbuf[0], preferred_element_type=F32)
    stream(stc[2:])
    zc[0].wait()
    z = jnp.dot(feed, zbuf[0], preferred_element_type=F32)
    for copy in smalls[-2:]:
        copy.wait()
    bcp, dtp = narrow(0, feed)
    feeds = {}
    for k in [1] + far[:-1]:
        hid_swaps[k].wait_recv()
        feeds[k] = fed(k)
        squares += squared(k)
        more = narrow(k, feeds[k])
        bcp += more[0]
        dtp += more[1]
        if k == 1:
            xc[1].wait()
            x += jnp.dot(feeds[1], xbuf[1], preferred_element_type=F32)
            zc[1].wait()
            z += jnp.dot(feeds[1], zbuf[1], preferred_element_type=F32)
    inv = lax.rsqrt(squares / (n * feats) + 1e-05)
    bcp = (bcp * inv).astype(BF16)
    bcp_out[...] = bcp
    acc = bcp.astype(F32) * bc_taps[3:4, :].astype(F32)
    for t in range(3):
        acc += bc_state[t].astype(F32) * bc_taps[t : t + 1, :].astype(F32)
    bc_send[...] = silu(acc + bc_bias[...].astype(F32).reshape(1, -1)).astype(BF16)
    bc_all[me] = bc_send[...]
    bc_swaps = {k: swap(bc_send, bc_all.at[me], bs, br, k) for k in far}
    for k in far:
        bc_swaps[k].start()

    for k in far[:-1]:
        xc[k].wait()
        x += jnp.dot(feeds[k], xbuf[k], preferred_element_type=F32)
        zc[k].wait()
        z += jnp.dot(feeds[k], zbuf[k], preferred_element_type=F32)
    stream([owc[k] for k in far[:-1]])
    dt = softplus((dtp * inv).astype(BF16).astype(F32) + dt_bias[...].reshape(1, -1))
    decay = jnp.where(live, jnp.exp(-dt * jnp.exp(log_rate[...].reshape(1, -1))), 1.0)
    for h in range(heads):
        dec_out[h] = jnp.broadcast_to(decay[:, h : h + 1], (seqs, ns))
    spread = (
        lax.broadcasted_iota(jnp.int32, (heads, chans), 1) // hp
        == lax.broadcasted_iota(jnp.int32, (heads, chans), 0)
    ).astype(F32).astype(BF16)
    per_head = jnp.concatenate(
        [dt, decay, jnp.broadcast_to(skip[...].reshape(1, -1), (8, heads))], axis=0
    )
    high = per_head.astype(BF16)
    rest = per_head - high.astype(F32)
    mid = rest.astype(BF16)
    low = (rest - mid.astype(F32)).astype(BF16)
    wide = sum(jnp.dot(v, spread, preferred_element_type=F32) for v in (high, mid, low))
    dt_wide, decay_wide, skip_wide = wide[:seqs], wide[seqs : 2 * seqs], wide[2 * seqs : 2 * seqs + 1]

    x_new = (x * inv).astype(BF16)
    x_out[...] = x_new
    acc = x_new.astype(F32) * x_taps[3:4, :].astype(F32)
    for t in range(3):
        acc += x_state[t].astype(F32) * x_taps[t : t + 1, :].astype(F32)
    conv = silu(acc + x_bias[...].astype(F32).reshape(1, -1)).astype(BF16).astype(F32)
    u = jnp.where(live, dt_wide * conv, 0.0)
    high = u.astype(BF16).astype(F32)
    ut_out[...] = jnp.concatenate([high, u - high], axis=0).T.astype(BF16)
    gate = silu((z * inv).astype(BF16).astype(F32))

    for k in far:
        bc_swaps[k].wait_recv()
    stream([owc[far[-1]], owc[0]])
    both = jnp.concatenate([bc_all[j] for j in range(n)], axis=1).astype(F32)
    b_rows = both[:, :ns]
    c_rows = both[:, ns:]
    b_out[...] = b_rows
    along = jnp.sum(b_rows * c_rows, axis=1, keepdims=True)
    row_id = lax.broadcasted_iota(jnp.int32, (seqs, ns), 0)
    tile = ROWS if chans % ROWS == 0 else chans
    old_y = []
    for g, group in enumerate(GROUPS):
        rows = [q * span + i for q in group for i in range(span)]
        stationary = jnp.concatenate(
            [jnp.where(row_id == b, c_rows, 0.0).astype(BF16) for b in rows], axis=1
        )
        stationary = jnp.concatenate(
            [stationary, jnp.zeros((128 - seqs, len(rows) * ns), BF16)], axis=0
        )
        for q in group:
            stc[q].wait()
        for lo in range(0, chans, tile):
            moving = jnp.concatenate(
                [state_out[b, lo // hp : (lo + tile) // hp].reshape(tile, ns).astype(BF16) for b in rows],
                axis=1,
            )
            got = lax.dot_general(moving, stationary, NT, preferred_element_type=F32)
            if g == len(GROUPS) - 1:
                old_y.append((yt[lo : lo + tile, :] + got).T[:seqs])
            elif g:
                yt[lo : lo + tile, :] += got
            else:
                yt[lo : lo + tile, :] = got
    old_y = jnp.concatenate(old_y, axis=1)
    y = decay_wide * old_y + u * along + skip_wide * conv
    gated = y * gate
    scaled = (gated * norm_gain[...].reshape(1, -1)).astype(BF16)
    tails = []
    started = False
    for group in [[k] for k in far[:-1]] + [[far[-1], 0]]:
        for k in group:
            owc[k].wait()
        columns = jnp.concatenate([owbuf[k] for k in group], axis=1)
        got = jnp.dot(scaled, columns, preferred_element_type=F32)
        for i, k in enumerate(group):
            piece = got[:, i * feats : (i + 1) * feats]
            if k == 0:
                mine_out[...] = piece
            else:
                part_send[k] = piece.astype(BF16)
                tails.append(swap(part_send.at[k], parts.at[k - 1], ps, pr, k))
                tails[-1].start()
        if not started:
            started = True
            sq_out[...] = jnp.broadcast_to(jnp.sum(gated * gated, axis=1, keepdims=True), sq_out.shape)
            for k in far:
                tails.append(swap(sq_out, sqs.at[k - 1], qs, qr, k))
                tails[-1].start()
    for p in range(ready):
        update(p, dec_out, ut_out, b_out, state_out, state_out)
    for copies in (hid_swaps, bc_swaps):
        for k in far:
            copies[k].wait_send()
    for copy in tails:
        copy.wait()


def update(p, dec, ut, b_rows, state, out):
    seqs, heads, hp, ns = state.shape
    row_id = lax.broadcasted_iota(jnp.int32, (2 * seqs, ns), 0)
    b_twice = jnp.concatenate([b_rows[...], b_rows[...]], axis=0)
    stationary = jnp.concatenate(
        [
            jnp.where((row_id == 2 * p + i) | (row_id == 2 * p + i + seqs), b_twice, 0.0).astype(BF16)
            for i in range(2)
        ],
        axis=1,
    )
    pack = 128 // hp
    for lo in range(0, heads, pack):
        outer = jnp.dot(ut[lo * hp : (lo + pack) * hp, :], stationary, preferred_element_type=F32)
        for i in range(2):
            for h in range(pack):
                out[2 * p + i, lo + h] = (
                    dec[lo + h, pl.ds(2 * p + i, 1), :] * state[2 * p + i, lo + h]
                    + outer[h * hp : (h + 1) * hp, i * ns : (i + 1) * ns]
                )


def back_kernel(
    inner, ready,
    hidden, x_state, bc_state, slot, active, mine, sq, parts, sqs, x_new, bcp, ut, b_rows, dec, state,
    layer_h, x_next_h, bc_next_h, state_next,
    layer, x_next, bc_next, st, osem, lsem,
):
    seqs = state.shape[0]

    def write(source, p):
        both = pl.ds(2 * p, 2)
        return pltpu.make_async_copy(source.at[both], state_next.at[both], osem.at[p])

    for p in range(ready):
        write(state, p).start(priority=1)

    def step(p, carry):
        update(p, dec, ut, b_rows, state, st)
        write(st, p).start(priority=1)
        return carry

    lax.fori_loop(ready, seqs // 2, step, 0)
    onehot = slot_matrix(slot[...])
    live = jnp.sum(jnp.where(onehot, active[...], 0), axis=1, keepdims=True) > 0
    for old, new, nxt in ((x_state, x_new[...], x_next), (bc_state, bcp[...], bc_next)):
        nxt[0] = jnp.where(live, old[1], old[0])
        nxt[1] = jnp.where(live, old[2], old[1])
        nxt[2] = jnp.where(live, new, old[2])
    eye = lax.broadcasted_iota(jnp.int32, (seqs, seqs), 0) == lax.broadcasted_iota(
        jnp.int32, (seqs, seqs), 1
    )
    live = jnp.sum(jnp.where(eye, active[...], 0), axis=1, keepdims=True) > 0
    total = mine[...]
    squares = sq[:, :1]
    for k in range(parts.shape[0]):
        total += parts[k].astype(F32)
        squares += sqs[k][:, :1]
    inv = lax.rsqrt(squares / inner + 1e-05)
    delta = lax.dot_general(
        onehot.astype(F32), inv * total, TN,
        precision=lax.Precision.HIGHEST, preferred_element_type=F32,
    )
    old = hidden[...]
    layer[...] = jnp.where(live, (old.astype(F32) + delta).astype(BF16), old)
    outs = [
        pltpu.make_async_copy(s, d, lsem.at[i])
        for i, (s, d) in enumerate(((layer, layer_h), (x_next, x_next_h), (bc_next, bc_next_h)))
    ]
    for copy in outs:
        copy.start()

    def drain(p, carry):
        write(st, p).wait()
        return carry

    lax.fori_loop(0, seqs // 2, drain, 0)
    for copy in outs:
        copy.wait()


def shards(n, *args):
    hidden, z_weight, ssm_state = args[0], args[2], args[15]
    seqs, feats = hidden.shape
    chans = z_weight.shape[1]
    heads, hp, ns = ssm_state.shape[1:]
    aligned = feats % 128 == 0 and chans % 128 == 0 and ns == 128 and 128 % hp == 0
    if aligned and n > 1 and n & (n - 1) == 0 and seqs % 16 == 0 and seqs <= 128:
        return fast_shards(n, *args)
    return plain_shards(n, *args)


def fast_shards(
    n,
    hidden, in_gain, z_weight, x_weight, bc_weight, dt_weight,
    conv_x_weight, conv_x_bias, conv_bc_weight, conv_bc_bias, conv_x_state, conv_bc_state,
    dt_bias, log_rate, skip_gain, ssm_state, norm_gain, out_weight, pool_slot, active,
):
    seqs, feats = hidden.shape
    model, chans = z_weight.shape
    bc_own = bc_weight.shape[1]
    heads, hp, ns = ssm_state.shape[1:]
    steps = STEPS
    ready = READY
    in_hbm = lambda v: pltpu.with_memory_space_constraint(v, pltpu.HBM)
    active = active.reshape(1, -1)
    x_old = jnp.transpose(conv_x_state, (1, 0, 2))
    bc_old = jnp.transpose(conv_bc_state, (1, 0, 2))
    dma = pltpu.SemaphoreType.DMA
    shape = jax.ShapeDtypeStruct
    like = lambda v: pltpu.VMEM(v.shape, v.dtype)
    x_new, bcp, ut, b_rows, dec, mine, sq, parts, sqs, held, *kept = pl.pallas_call(
        functools.partial(front_kernel, n, steps, ready),
        out_shape=(
            pltpu.VMEM((seqs, chans), BF16),
            pltpu.VMEM((seqs, bc_own), BF16),
            pltpu.VMEM((chans, 2 * seqs), BF16),
            pltpu.VMEM((seqs, ns), F32),
            pltpu.VMEM((heads, seqs, ns), F32),
            pltpu.VMEM((seqs, feats), F32),
            pltpu.VMEM((seqs, 128), F32),
            pltpu.VMEM((n - 1, seqs, feats), BF16),
            pltpu.VMEM((n - 1, seqs, 128), F32),
            pltpu.VMEM(ssm_state.shape, F32),
            like(hidden), like(x_old), like(bc_old), like(pool_slot), like(active),
        ),
        in_specs=[HBM] * 20,
        out_specs=(VMEM,) * 15,
        scratch_shapes=[
            pltpu.VMEM((n, seqs, feats), BF16),
            pltpu.VMEM((n, feats, chans), BF16),
            pltpu.VMEM((n, feats, chans), BF16),
            pltpu.VMEM((bc_own, model), BF16),
            pltpu.VMEM((heads, model), BF16),
            pltpu.VMEM((n, chans, feats), BF16),
            pltpu.VMEM((seqs, bc_own), BF16),
            pltpu.VMEM((n, seqs, bc_own), BF16),
            pltpu.VMEM((chans, 128), F32),
            pltpu.VMEM((n, seqs, feats), BF16),
            like(in_gain), like(conv_x_weight), like(conv_x_bias), like(conv_bc_weight), like(conv_bc_bias),
            like(dt_bias), like(log_rate), like(skip_gain), like(norm_gain),
            dma((n - 1,)), dma((n - 1,)), dma((n - 1,)), dma((n - 1,)),
        ],
        compiler_params=pltpu.CompilerParams(
            collective_id=0, has_side_effects=True, vmem_limit_bytes=28 * 2**20
        ),
        name="front",
    )(*map(in_hbm, (
        hidden, in_gain, z_weight, x_weight, bc_weight.T, dt_weight.T, out_weight,
        conv_x_weight, conv_x_bias, x_old, conv_bc_weight, conv_bc_bias, bc_old,
        dt_bias, log_rate, skip_gain, norm_gain, pool_slot, active, ssm_state,
    )))
    layer_out, x_next, bc_next, state_next = pl.pallas_call(
        functools.partial(back_kernel, chans * n, ready),
        out_shape=(
            shape(hidden.shape, BF16),
            shape(x_old.shape, BF16),
            shape(bc_old.shape, BF16),
            shape(ssm_state.shape, F32),
        ),
        in_specs=[VMEM] * 15,
        out_specs=(HBM,) * 4,
        scratch_shapes=[
            like(hidden), like(x_old), like(bc_old), like(ssm_state),
            dma((seqs // 2,)), dma((3,)),
        ],
        compiler_params=pltpu.CompilerParams(vmem_limit_bytes=16 * 2**20),
        name="back",
    )(
        *kept, mine, sq, parts, sqs, x_new, bcp, ut, b_rows, dec, held,
    )
    return (
        layer_out,
        jnp.transpose(x_next, (1, 0, 2)),
        jnp.transpose(bc_next, (1, 0, 2)),
        state_next,
    )


def plain_shards(
    n,
    hidden, in_gain, z_weight, x_weight, bc_weight, dt_weight,
    conv_x_weight, conv_x_bias, conv_bc_weight, conv_bc_bias, conv_x_state, conv_bc_state,
    dt_bias, log_rate, skip_gain, ssm_state, norm_gain, out_weight, pool_slot, active,
):
    seqs, feats = hidden.shape
    model, chans = z_weight.shape
    bc_own = bc_weight.shape[1]
    heads, hp, ns = ssm_state.shape[1:]
    in_hbm = lambda v: pltpu.with_memory_space_constraint(v, pltpu.HBM)
    row = lambda v: v.reshape(1, -1)
    active = row(active)
    x_old = jnp.transpose(conv_x_state, (1, 0, 2))
    bc_old = jnp.transpose(conv_bc_state, (1, 0, 2))
    dma = pltpu.SemaphoreType.DMA
    shape = jax.ShapeDtypeStruct
    z, x, bcp, bc, dt, decay, held = pl.pallas_call(
        functools.partial(project_kernel, n),
        out_shape=(
            shape((seqs, chans), BF16),
            shape((seqs, chans), BF16),
            shape((seqs, bc_own), BF16),
            shape((seqs, bc_own * n), BF16),
            shape((seqs, heads), F32),
            shape((seqs, heads), F32),
            pltpu.VMEM(ssm_state.shape, F32),
        ),
        in_specs=[HBM] * 14,
        out_specs=(VMEM,) * 7,
        scratch_shapes=[
            pltpu.VMEM((n, seqs, feats), BF16),
            pltpu.VMEM((n, seqs, feats), BF16),
            pltpu.VMEM((n, feats, chans), BF16),
            pltpu.VMEM((n, feats, chans), BF16),
            pltpu.VMEM((seqs, bc_own), BF16),
            pltpu.VMEM((n, seqs, bc_own), BF16),
            pltpu.VMEM(in_gain.shape, F32),
            pltpu.VMEM((bc_own, model), BF16),
            pltpu.VMEM((heads, model), BF16),
            pltpu.VMEM(conv_bc_weight.shape, BF16),
            pltpu.VMEM(conv_bc_bias.shape, BF16),
            pltpu.VMEM(bc_old.shape, BF16),
            pltpu.VMEM(dt_bias.shape, F32),
            pltpu.VMEM(log_rate.shape, F32),
            pltpu.VMEM(pool_slot.shape, jnp.int32),
            pltpu.VMEM(active.shape, jnp.int32),
            dma((n,)), dma((n,)), dma((n,)), dma((n,)), dma((n,)), dma((n,)), dma(()), dma((10,)), dma(()),
        ],
        compiler_params=pltpu.CompilerParams(collective_id=0, has_side_effects=True, vmem_limit_bytes=20 * 2**20),
        name="project",
    )(*map(in_hbm, (
        hidden, in_gain, z_weight, x_weight, bc_weight.T, dt_weight.T,
        conv_bc_weight, conv_bc_bias, bc_old, dt_bias, log_rate, pool_slot, active, ssm_state,
    )))
    x_next, bc_next, state_next, branch, sq = pl.pallas_call(
        functools.partial(state_kernel, n, 4 if heads % 4 == 0 else heads),
        out_shape=(
            shape(x_old.shape, BF16),
            shape(bc_old.shape, BF16),
            shape(ssm_state.shape, F32),
            shape((n, seqs, feats), BF16),
            shape((seqs, 128), F32),
        ),
        in_specs=[SMEM] + [VMEM] * 15 + [HBM],
        out_specs=(VMEM, VMEM, HBM, VMEM, VMEM),
        scratch_shapes=[
            pltpu.VMEM(ssm_state.shape, F32),
            pltpu.VMEM(out_weight.shape, BF16),
            pltpu.VMEM((chans, 2 * seqs), BF16),
            pltpu.VMEM((seqs, chans), F32),
            pltpu.VMEM((seqs, ns), F32),
            dma((seqs,)), dma(()),
        ],
        compiler_params=pltpu.CompilerParams(vmem_limit_bytes=20 * 2**20),
        name="state",
    )(
        decay, decay, dt, z, x, bcp, bc, conv_x_weight, conv_x_bias, x_old, bc_old,
        row(skip_gain), norm_gain, pool_slot, active, held, in_hbm(out_weight),
    )
    layer_out = pl.pallas_call(
        functools.partial(reduce_kernel, n, chans * n),
        out_shape=shape((seqs, feats), BF16),
        in_specs=[VMEM] * 4,
        out_specs=VMEM,
        scratch_shapes=[
            pltpu.VMEM((n, seqs, feats), BF16),
            pltpu.VMEM((n, seqs, 128), F32),
            dma((n,)), dma((n,)), dma((n,)), dma((n,)),
        ],
        compiler_params=pltpu.CompilerParams(collective_id=1, has_side_effects=True, vmem_limit_bytes=2 * 2**20),
        name="reduce",
    )(branch, sq, hidden, active)
    return (
        layer_out,
        jnp.transpose(x_next, (1, 0, 2)),
        jnp.transpose(bc_next, (1, 0, 2)),
        state_next,
    )


def solution(mesh):
    rows = ("groups", "dp")
    placed = (
        P(rows, "tp"), P(), P(None, "tp"), P(None, "tp"), P(None, "tp"), P(None, "tp"),
        P(None, "tp"), P("tp"), P(None, "tp"), P("tp"),
        P(rows, None, "tp"), P(rows, None, "tp"),
        P("tp"), P("tp"), P("tp"), P(rows, "tp", None, None), P("tp"), P("tp", None),
        P(rows, None), P(rows),
    )
    return jax.shard_map(
        functools.partial(shards, mesh.shape["tp"]),
        mesh=mesh,
        in_specs=placed,
        out_specs=(
            P(rows, "tp"), P(rows, None, "tp"), P(rows, None, "tp"), P(rows, "tp", None, None),
        ),
        check_vma=False,
    )
```
